32 devices in a mesh: expert: 8 (over z, x), shard: 4 (over y, core).
Axes of the slice: x: 2, y: 2, z: 4, core: 2. Of those that a mesh axis runs over, the one named last changes fastest.
Arguments:
- tokens: bfloat16 [64, 384, 768], P(('expert', 'shard')), may hold values from -6 to 6
- cotangent: bfloat16 [64, 384, 768], P(('expert', 'shard')), may hold values from -6 to 6
- lengths: int32 [64], replicated, may hold values from 1 to 384, 18432 in all
- dealing: int32 [64], P(('expert', 'shard')), may hold values from 0 to 63, each once
- routes: int32 [64, 384, 2], P(('expert', 'shard')), may hold values from 0 to 7, all different within a row; in each aligned block of 384 rows (0 to 383, 384 to 767, ..., all dimensions but the last counted through in order) at most 192 rows name the same one
- query_weight: bfloat16 [768, 768], P('shard'), may hold values from -0.21875 to 0.21875
- key_weight: bfloat16 [768, 768], P('shard'), may hold values from -0.21875 to 0.21875
- value_weight: bfloat16 [768, 768], P('shard'), may hold values from -0.21875 to 0.21875
- output_weight: bfloat16 [768, 768], P('shard'), may hold values from -0.875 to 0.875
- router_weight: bfloat16 [768, 8], P('shard'), may hold values from -0.3125 to 0.3125
- first_gain: bfloat16 [768], P('shard'), may hold values from 0.5 to 1.5
- second_gain: bfloat16 [768], P('shard'), may hold values from 0.5 to 1.5
- position_bias: bfloat16 [12, 32], P('shard'), may hold values from -3 to 3
- inner_weight: bfloat16 [8, 768, 3072], P('expert', None, 'shard'), may hold values from -0.21875 to 0.21875
- outer_weight: bfloat16 [8, 3072, 768], P('expert', 'shard'), may hold values from -0.109375 to 0.109375
Outputs:
- result: bfloat16 [64, 384, 768], P(('expert', 'shard'))
- input_gradient: bfloat16 [64, 384, 768], P(('expert', 'shard'))
- query_gradient: float32 [768, 768], P('shard')
- key_gradient: float32 [768, 768], P('shard')
- value_gradient: float32 [768, 768], P('shard')
- output_gradient: float32 [768, 768], P('shard')
- router_gradient: float32 [768, 8], P('shard')
- first_gain_gradient: float32 [768], P('shard')
- second_gain_gradient: float32 [768], P('shard')
- bias_gradient: float32 [12, 32], P('shard')
- inner_gradient: float32 [8, 768, 3072], P('expert', None, 'shard')
- outer_gradient: float32 [8, 3072, 768], P('expert', 'shard')
The draws below stay inside these ranges and needn't reach their ends.
Inputs may be any that keep to these rules, and one draw needn't show every extreme that they name: The lengths of all sequences; some sequence fills all 384 slots. `dealing`: each sequence number appears once. `routes`: A token's two experts differ; within one sequence no expert is chosen by more than 192 tokens, and in every draw some expert is chosen by exactly 192 tokens of some sequence.
All inputs are finite; a program needn't handle non-finite values.
Results may differ from the reference program's by a relative error of at most 0.017.
Values may be sent and summed in bfloat16 or wider, within the bound.
A program may use at most 256 MiB of HBM per device.

```python
import math
import jax
import jax.numpy as jnp
import numpy as np
from jax import lax

D = 768
H = 12
HD = 64
FF = 3072
NBUCK = 32
SEQ = 384
E = 8
CAP = 192
NSEQ = 64


def level_of(key, extent, shards, low, high):
    level = 1.0
    for dim, parts in shards:
        heights = jax.random.uniform(jax.random.fold_in(jax.random.fold_in(key, 6), dim), (parts,), jnp.float32, low / len(shards), high / len(shards))
        level = level * jnp.repeat(jnp.exp(heights), extent[dim] // parts).reshape((-1,) + (1,) * (len(extent) - 1 - dim))
    return level


def profile(amount, total, reach, skew):
    weights = [(1 << 20) // math.isqrt(grade ** skew) + 1 for grade in range(2, amount + 1)]
    surplus, counts = total - reach - (amount - 1), [1] * (amount - 1)
    while surplus > 0:
        free = [i for i in range(amount - 1) if counts[i] < reach]
        pool, budget = sum([weights[i] for i in free]), surplus
        for i in free:
            extra = min(reach - counts[i], max(1, budget * weights[i] // pool), surplus)
            counts[i] = counts[i] + extra
            surplus = surplus - extra
    return np.array([reach] + counts)


def uneven_parts(rng, amount, total, most, skew):
    if amount == 2:
        one = jax.random.randint(rng, (), max(1, total - most), min(most, total - 1) + 1)
        return jnp.stack([one, total - one])
    sizes = jnp.asarray(profile(amount, total, most, skew), jnp.int32)
    pairs = (amount - 1) // 2
    source_of, taker = sizes[1:1 + 2 * pairs:2], sizes[2:2 + 2 * pairs:2]
    slack = jnp.minimum(source_of - 1, most - taker)
    moved = jax.random.randint(jax.random.fold_in(rng, 1), (pairs,), 0, 1 << 20) % (slack + 1)
    sizes = sizes.at[1:1 + 2 * pairs:2].set(source_of - moved).at[2:2 + 2 * pairs:2].set(taker + moved)
    return sizes[jax.random.permutation(jax.random.fold_in(rng, 2), amount)]


def assign_block(rng, own, number, rows, count, top, most, skew):
    ranking = jax.random.permutation(rng, count)
    heavy_load, common = portions_of(count, rows * top, most, skew, True), portions_of(count, rows * top, most, skew, False)
    places = jnp.arange(count)

    def named(tallies, offset_by):
        used = int((tallies > 0).sum())
        fixed = max(1, used // 4)
        passed = fixed + (places - fixed + offset_by * (used - fixed)) % max(1, count - fixed)
        return jnp.zeros((count,), jnp.int32).at[ranking[jnp.where(places < fixed, places, passed)]].set(jnp.asarray(tallies, jnp.int32))

    tallies = jnp.where(number % 4 == 0, named(heavy_load, number // 4), named(common, number - number // 4 - 1))
    mixed = jax.random.permutation(jax.random.fold_in(own, 3), count)
    donor, receiver = mixed[0:count // 2 * 2:2], mixed[1:count // 2 * 2:2]
    room = jnp.minimum(tallies[donor] - 1, most - tallies[receiver]) // 2
    room = jnp.where((donor == ranking[0]) | (receiver == ranking[0]) | (tallies[receiver] == 0), 0, jnp.maximum(room, 0))
    passed = jax.random.randint(jax.random.fold_in(own, 4), (count // 2,), 0, 1 << 20) % (room + 1)
    tallies = tallies.at[donor].add(-passed).at[receiver].add(passed)
    items = jnp.searchsorted(jnp.cumsum(tallies), jnp.arange(rows * top), side="right").astype(jnp.int32)
    grid = items.reshape(top, rows).T
    grid = grid[jax.random.permutation(jax.random.fold_in(own, 1), rows)]
    offset_by = jax.random.randint(jax.random.fold_in(own, 2), (rows, 1), 0, top)
    return jnp.take_along_axis(grid, (jnp.arange(top)[None, :] + offset_by) % top, axis=1)


def portions_of(number_of, total, limit, slope, full):
    weights = [(1 << 20) // math.isqrt(rank ** slope) + 1 for rank in range(1, number_of + 1)]
    largest = limit if full else min(limit, max(-(-total // number_of), total * weights[0] // sum(weights)))
    least = 1 if total - largest >= number_of - 1 else 0
    given, rest = [largest] + [least] * (number_of - 1), total - largest - least * (number_of - 1)
    while rest > 0:
        free = [i for i in range(1, number_of) if given[i] < largest] or [i for i in range(1, number_of) if given[i] < limit]
        whole, left = sum([weights[i] for i in free]), rest
        for i in free:
            addition = min(limit - given[i], max(1, left * weights[i] // whole), rest)
            given[i] = given[i] + addition
            rest = rest - addition
    return np.array(given)


def gaussian(key, dims, scale, bound, pieces=(), kind=jnp.bfloat16):
    entries = scale * jax.random.normal(key, dims, jnp.float32)
    if pieces:
        entries = entries * level_of(key, dims, pieces, -0.22, 0.18)
    return jnp.clip(entries, -bound, bound).astype(kind)


def setup_inputs(seed: int = 0) -> dict:
    seeds = jax.random.split(jax.random.key(seed), 16)
    tokens = gaussian(seeds[0], (NSEQ, SEQ, D), 1.0, 6.0, ((0, 32),))
    cotangent = gaussian(seeds[1], (NSEQ, SEQ, D), 1.0, 6.0, ((0, 32),))
    lengths = uneven_parts(seeds[2], NSEQ, NSEQ * SEQ * 3 // 4, SEQ, 1).astype(jnp.int32)
    dealing = jax.random.permutation(seeds[3], NSEQ).astype(jnp.int32)
    routes_keys = jax.random.split(jax.random.fold_in(seeds[4], 1), NSEQ * SEQ // SEQ)
    routes_turns = jax.random.permutation(jax.random.fold_in(seeds[4], 3), NSEQ * SEQ // SEQ)
    routes = jax.vmap(lambda own, number: assign_block(jax.random.fold_in(seeds[4], 2), own, number, SEQ, E, 2, CAP, 1))(routes_keys, routes_turns).reshape((NSEQ, SEQ, 2))
    query_weight = gaussian(seeds[5], (D, D), D ** -0.5, 0.21875, ((0, 4),))
    key_weight = gaussian(seeds[6], (D, D), D ** -0.5, 0.21875, ((0, 4),))
    value_weight = gaussian(seeds[7], (D, D), D ** -0.5, 0.21875, ((0, 4),))
    output_weight = gaussian(seeds[8], (D, D), (D // 16) ** -0.5, 0.875, ((0, 4),))
    router_weight = gaussian(seeds[9], (D, E), (D // 2) ** -0.5, 0.3125, ((0, 4),))
    first_gain = jnp.clip(1.0 + 0.1 * jax.random.normal(seeds[10], (D,), jnp.float32), 0.5, 1.5).astype(jnp.bfloat16)
    second_gain = jnp.clip(1.0 + 0.1 * jax.random.normal(seeds[11], (D,), jnp.float32), 0.5, 1.5).astype(jnp.bfloat16)
    position_bias = gaussian(seeds[12], (H, NBUCK), 1.0, 3.0, ((0, 4),))
    inner_weight = gaussian(seeds[13], (E, D, FF), D ** -0.5, 0.21875, ((0, 8), (2, 4)))
    outer_weight = gaussian(seeds[14], (E, FF, D), FF ** -0.5, 0.109375, ((0, 8), (1, 4)))
    return {"tokens": tokens, "cotangent": cotangent, "lengths": lengths, "dealing": dealing, "routes": routes, "query_weight": query_weight, "key_weight": key_weight, "value_weight": value_weight, "output_weight": output_weight, "router_weight": router_weight, "first_gain": first_gain, "second_gain": second_gain, "position_bias": position_bias, "inner_weight": inner_weight, "outer_weight": outer_weight}


@jax.custom_vjp
def low(v):
    return lax.optimization_barrier(v.astype(jnp.bfloat16)).astype(jnp.float32)

@jax.custom_vjp
def low_back(v):
    return v

def low_keep(v):
    return (low(v), None)

def low_pass(kept, grad):
    return (grad,)

def back_keep(v):
    return (v, None)

def back_low(kept, grad):
    return (low(grad),)
low.defvjp(low_keep, low_pass)
low_back.defvjp(back_keep, back_low)
EPSILON = 1e-06
HIGH = lax.Precision.HIGHEST
NEGATIVE = -1000000000.0

def rounded(value):
    return low(low_back(value))

def bucket_table(length):
    distance = np.arange(length)
    scaled = 16 + np.floor(np.log(np.maximum(distance, 1) / 16.0) / np.log(8.0) * 16.0)
    return np.where(distance < 16, distance, np.minimum(scaled, 31)).astype(np.int32)

def rms_norm(value, gain):
    return value * lax.rsqrt(lax.optimization_barrier(jnp.mean(value * value, -1, keepdims=True)) + EPSILON) * gain

def reference(tokens, cotangent, lengths, dealing, routes, query_weight, key_weight, value_weight, output_weight, router_weight, first_gain, second_gain, position_bias, inner_weight, outer_weight):
    experts = inner_weight.shape[0]
    capacity = 4 * SEQ // experts
    seq_count = tokens.shape[0]
    pick_total = seq_count * 2 * SEQ
    pick_ids = routes.reshape(seq_count, 2 * SEQ)
    onehot = (pick_ids[:, :, None] == jnp.arange(experts, dtype=jnp.int32)[None, None, :]).astype(jnp.int32)
    ranks = lax.optimization_barrier(jnp.sum((jnp.cumsum(onehot, 1) - onehot) * onehot, 2))
    slot_place = pick_ids * (seq_count * capacity) + jnp.arange(seq_count, dtype=jnp.int32)[:, None] * capacity + ranks
    slot_place = slot_place.reshape(-1).astype(jnp.int32)
    total_slots = experts * seq_count * capacity
    source = jnp.full((total_slots,), pick_total, jnp.int32).at[slot_place].set(jnp.arange(pick_total, dtype=jnp.int32))
    token_source = jnp.where(source == pick_total, seq_count * SEQ, source // 2).astype(jnp.int32)
    seq_length = jnp.take(lengths, dealing)
    table = jnp.asarray(bucket_table(SEQ))
    bucket_hot = (table[None, :] == jnp.arange(NBUCK, dtype=jnp.int32)[:, None]).astype(jnp.float32)
    places = np.arange(SEQ)
    distance = jnp.asarray(np.maximum(places[:, None] - places[None, :], 0).astype(np.int32))
    positions = jnp.arange(SEQ, dtype=jnp.int32)
    causal = positions[None, :] <= positions[:, None]
    pick_hot = (routes.reshape(-1, 2)[:, :, None] == jnp.arange(experts, dtype=jnp.int32)[None, None, :]).astype(jnp.float32)
    score_scale = HD ** (-0.5)

    def forward(inputs, query_mat, key_mat, value_mat, output_mat, router_mat, gain_one, gain_two, bias_table, inner_mats, outer_mats):
        normed_one = low(rms_norm(inputs, gain_one))
        bias_dist = jnp.dot(bias_table, bucket_hot, precision=HIGH)
        bias_full = jnp.take(bias_dist, distance, axis=1)

        def attend(pair):
            normed, length = pair
            queries = rounded(jnp.dot(normed, query_mat, precision=HIGH)).reshape(SEQ, H, HD)
            key_rows = rounded(jnp.dot(normed, key_mat, precision=HIGH)).reshape(SEQ, H, HD)
            value_rows = rounded(jnp.dot(normed, value_mat, precision=HIGH)).reshape(SEQ, H, HD)
            logits = jnp.einsum('qhd,khd->hqk', queries, key_rows, precision=HIGH) * score_scale + bias_full
            logits = low_back(logits)
            valid = causal & (positions[None, :] < length)
            masked = jnp.where(valid[None], logits, NEGATIVE)
            top_value = lax.optimization_barrier(jnp.max(masked, 2, keepdims=True))
            exponent = jnp.exp(masked - top_value)
            soft = low(exponent / lax.optimization_barrier(jnp.sum(exponent, 2, keepdims=True)))
            mixture = jnp.einsum('hqk,khd->qhd', soft, value_rows, precision=HIGH).reshape(SEQ, H * HD)
            return rounded(mixture)
        mixture = lax.map(jax.checkpoint(attend), (normed_one, seq_length))
        branch = low_back(jnp.dot(mixture.reshape(-1, H * HD), output_mat, precision=HIGH))
        residual = inputs.reshape(-1, H * HD) + branch
        normed_two = low(rms_norm(residual, gain_two))
        router = jnp.dot(normed_two, router_mat, precision=HIGH)
        chosen = lax.optimization_barrier(jnp.sum(router[:, None, :] * pick_hot, 2))
        chosen_top = lax.optimization_barrier(jnp.max(chosen, 1, keepdims=True))
        chosen_exp = jnp.exp(chosen - chosen_top)
        gates = chosen_exp / lax.optimization_barrier(jnp.sum(chosen_exp, 1, keepdims=True))
        padded = jnp.concatenate([normed_two, jnp.zeros((1, H * HD), jnp.float32)], 0)
        expert_rows = low_back(jnp.take(padded, token_source, axis=0)).reshape(experts, seq_count * capacity, H * HD)

        def expert_apply(triple):
            rows_one, inner_one, outer_one = triple
            pre_act = low_back(jnp.dot(rows_one, inner_one, precision=HIGH))
            hidden = low(jax.nn.gelu(pre_act, approximate=False))
            return rounded(jnp.dot(hidden, outer_one, precision=HIGH))
        outputs = lax.map(jax.checkpoint(expert_apply), (expert_rows, inner_mats, outer_mats)).reshape(total_slots, H * HD)
        picked = jnp.take(outputs, slot_place, axis=0).reshape(-1, 2, H * HD)
        combined = residual + lax.optimization_barrier(jnp.sum(gates[:, :, None] * picked, 1))
        return combined.reshape(seq_count, SEQ, H * HD)
    primals = (tokens.astype(jnp.float32), query_weight.astype(jnp.float32), key_weight.astype(jnp.float32), value_weight.astype(jnp.float32), output_weight.astype(jnp.float32), router_weight.astype(jnp.float32), first_gain.astype(jnp.float32), second_gain.astype(jnp.float32), position_bias.astype(jnp.float32), inner_weight.astype(jnp.float32), outer_weight.astype(jnp.float32))
    result, pullback = jax.vjp(forward, *primals)
    grads = pullback(cotangent.astype(jnp.float32))
    return (result.astype(jnp.bfloat16), grads[0].astype(jnp.bfloat16), grads[1], grads[2], grads[3], grads[4], grads[5], grads[6], grads[7], grads[8], grads[9], grads[10])
```

```python
import functools
import math

import jax
import jax.numpy as jnp
import numpy as np
from jax import lax
from jax.sharding import PartitionSpec as P

EPSILON = 1e-06
HIGH = lax.Precision.HIGHEST
NEGATIVE = -1000000000.0
INV_ROOT_TWO = 1.0 / math.sqrt(2.0)
INV_ROOT_TAU = 1.0 / math.sqrt(2.0 * math.pi)


def bucket_table(length):
    distance = np.arange(length)
    scaled = 16 + np.floor(np.log(np.maximum(distance, 1) / 16.0) / np.log(8.0) * 16.0)
    return np.where(distance < 16, distance, np.minimum(scaled, 31)).astype(np.int32)


def bucket_matrix(length):
    table = bucket_table(length)
    places = np.arange(length)
    distance = np.maximum(places[:, None] - places[None, :], 0)
    return jnp.asarray(table[distance].astype(np.int32))


def normalize(value, gain):
    inverse = lax.rsqrt(jnp.mean(value * value, -1, keepdims=True) + EPSILON)
    return (value * inverse * gain, inverse)


def normalize_back(value, inverse, gain, grad_result):
    unit_rows = value * inverse
    grad_unit = grad_result * gain
    grad_gain = jnp.sum(grad_result * unit_rows, 0)
    grad_value = inverse * (
        grad_unit - unit_rows * jnp.mean(grad_unit * unit_rows, -1, keepdims=True)
    )
    return (grad_value, grad_gain)


def gelu_parts(pre_act):
    normal_cdf = 0.5 * (1.0 + lax.erf(pre_act * INV_ROOT_TWO))
    return (
        pre_act * normal_cdf,
        normal_cdf + pre_act * jnp.exp(-0.5 * pre_act * pre_act) * INV_ROOT_TAU,
    )


def slot_tables(pick_ids, experts, capacity, seq_len):
    pick_total = pick_ids.shape[0]
    onehot = (pick_ids[:, None] == jnp.arange(experts, dtype=jnp.int32)[None, :]).astype(
        jnp.bfloat16
    )
    order = jnp.arange(pick_total, dtype=jnp.int32)
    earlier = (order[None, :] < order[:, None]).astype(jnp.bfloat16)
    before = jnp.dot(earlier, onehot, preferred_element_type=jnp.float32)
    ranks = jnp.sum(before * onehot.astype(jnp.float32), 1).astype(jnp.int32)
    places = pick_ids * capacity + ranks
    slot_numbers = jnp.arange(experts * capacity, dtype=jnp.int32)
    slot_hot = (places[None, :] == slot_numbers[:, None]).astype(jnp.bfloat16)
    token_hot = jnp.sum(
        slot_hot.reshape(experts * capacity, seq_len, 2).astype(jnp.float32), 2
    ).astype(jnp.bfloat16)
    return (slot_hot, token_hot)


def attention_scores(queries, key_rows, bias_full, valid, score_scale):
    logits = (
        jnp.einsum("qhd,khd->hqk", queries, key_rows, preferred_element_type=jnp.float32)
        * score_scale
        + bias_full
    )
    return jnp.where(valid[None], logits, NEGATIVE)


def attention_forward(normed, query_full, key_full, value_full, bias_full, valid):
    seq_len, model_width = normed.shape
    head_count = bias_full.shape[0]
    head_dim = model_width // head_count
    score_scale = head_dim ** (-0.5)

    def project(matrix):
        return (
            jnp.dot(normed, matrix, preferred_element_type=jnp.float32)
            .astype(jnp.bfloat16)
            .reshape(seq_len, head_count, head_dim)
        )

    queries = project(query_full)
    key_rows = project(key_full)
    value_rows = project(value_full)
    masked = attention_scores(queries, key_rows, bias_full, valid, score_scale)
    top_value = jnp.max(masked, 2, keepdims=True)
    exponent = jnp.exp(masked - top_value)
    totals = jnp.sum(exponent, 2, keepdims=True)
    soft = (exponent / totals).astype(jnp.bfloat16)
    mixture = jnp.einsum("hqk,khd->qhd", soft, value_rows, preferred_element_type=jnp.float32)
    mixture = mixture.astype(jnp.bfloat16).reshape(seq_len, model_width)
    return (mixture, (queries, key_rows, value_rows, top_value + jnp.log(totals)))


def attention_backward(saved, bias_full, valid, grad_mixture):
    queries, key_rows, value_rows, log_total = saved
    seq_len, head_count, head_dim = queries.shape
    score_scale = head_dim ** (-0.5)
    masked = attention_scores(queries, key_rows, bias_full, valid, score_scale)
    soft = jnp.exp(masked - log_total)
    grad_heads = grad_mixture.reshape(seq_len, head_count, head_dim)
    grad_soft = jnp.einsum(
        "qhd,khd->hqk", grad_heads, value_rows, preferred_element_type=jnp.float32
    )
    grad_logits = (soft * (grad_soft - jnp.sum(soft * grad_soft, 2, keepdims=True))).astype(
        jnp.bfloat16
    )
    grad_values = jnp.einsum(
        "hqk,qhd->khd", soft.astype(jnp.bfloat16), grad_heads, preferred_element_type=jnp.float32
    )
    grad_queries = (
        jnp.einsum("hqk,khd->qhd", grad_logits, key_rows, preferred_element_type=jnp.float32)
        * score_scale
    )
    grad_keys = (
        jnp.einsum("hqk,qhd->khd", grad_logits, queries, preferred_element_type=jnp.float32)
        * score_scale
    )
    flat_width = head_count * head_dim
    return (
        grad_queries.astype(jnp.bfloat16).reshape(seq_len, flat_width),
        grad_keys.astype(jnp.bfloat16).reshape(seq_len, flat_width),
        grad_values.astype(jnp.bfloat16).reshape(seq_len, flat_width),
        grad_logits,
    )


def flip(value, axis):
    return lax.ppermute(value, axis, [(0, 1), (1, 0)])


class Grouped:
    shard_axes = "shard"
    swap_axes = "expert"
    data_axes = ("expert", "shard")

    def gather_experts(self, inner, outer):
        return (
            lax.all_gather(inner, "shard", axis=1, tiled=True),
            lax.all_gather(outer, "shard", axis=0, tiled=True),
        )

    def shard_index(self):
        return lax.axis_index("shard")

    def reduce_mixer(self, grad):
        share = lax.psum_scatter(
            grad.astype(jnp.bfloat16), "shard", scatter_dimension=0, tiled=True
        )
        return lax.psum(share.astype(jnp.float32), "expert")

    def reduce_experts(self, grad_inner, grad_outer):
        return (
            lax.psum_scatter(
                grad_inner.astype(jnp.bfloat16), "shard", scatter_dimension=1, tiled=True
            ).astype(jnp.float32),
            lax.psum_scatter(
                grad_outer.astype(jnp.bfloat16), "shard", scatter_dimension=0, tiled=True
            ).astype(jnp.float32),
        )


class Halved:
    shard_axes = ("y", "core")
    swap_axes = ("y", "zl", "x")
    data_axes = ("zh", "zl", "x", "y", "core")

    def gather_one(self, quarter, axis):
        at_home = lax.axis_index("zh") == lax.axis_index("y")
        other = flip(quarter, "zh")
        kept = jnp.where(at_home, quarter, other)
        given = jnp.where(at_home, other, quarter)
        pair = jnp.concatenate([kept, flip(given, "y")], axis)
        return jnp.concatenate([pair, flip(pair, "core")], axis)

    def gather_experts(self, inner, outer):
        return (self.gather_one(inner, 1), self.gather_one(outer, 0))

    def shard_index(self):
        return lax.axis_index("y") * 2 + lax.axis_index("core")

    def reduce_one(self, grad, axis):
        quarter = grad.shape[axis] // 4
        parts = [lax.slice_in_dim(grad, i * quarter, (i + 1) * quarter, axis=axis) for i in range(4)]
        sent = jnp.concatenate([parts[2], parts[3]], axis).astype(jnp.bfloat16)
        got = flip(sent, "core").astype(jnp.float32)
        kept = parts[0] + lax.slice_in_dim(got, 0, quarter, axis=axis)
        given = parts[1] + lax.slice_in_dim(got, quarter, 2 * quarter, axis=axis)
        kept = kept.astype(jnp.bfloat16)
        got = flip(given.astype(jnp.bfloat16), "y")
        at_home = lax.axis_index("zh") == lax.axis_index("y")
        mine = jnp.where(at_home, kept, got)
        sent = jnp.where(at_home, got, kept)
        return mine.astype(jnp.float32) + flip(sent, "zh").astype(jnp.float32)

    def reduce_experts(self, grad_inner, grad_outer):
        return (self.reduce_one(grad_inner, 1), self.reduce_one(grad_outer, 0))

    def halve(self, grad, axis):
        rows = grad.shape[0] // 2
        pos = lax.axis_index(axis)
        sent = lax.dynamic_slice_in_dim(grad, (1 - pos) * rows, rows, 0).astype(jnp.bfloat16)
        kept = lax.dynamic_slice_in_dim(grad, pos * rows, rows, 0)
        return kept + flip(sent, axis).astype(jnp.float32)

    def join(self, part, axis):
        other = flip(part, axis)
        first = lax.axis_index(axis) == 0
        return jnp.concatenate(
            [jnp.where(first, part, other), jnp.where(first, other, part)], 0
        )

    def reduce_mixer(self, grad):
        for axis in ("y", "core", "x", "zl", "zh"):
            grad = self.halve(grad, axis)
        grad = grad.astype(jnp.bfloat16)
        for axis in ("zh", "zl", "x"):
            grad = self.join(grad, axis)
        return grad.astype(jnp.float32)


def accumulate(running, grads):
    if running is None:
        return grads
    return jax.tree.map(jnp.add, running, grads)


def body(
    plan,
    tokens,
    cotangent,
    lengths,
    dealing,
    routes,
    query_weight,
    key_weight,
    value_weight,
    output_weight,
    router_weight,
    first_gain,
    second_gain,
    position_bias,
    inner_weight,
    outer_weight,
):
    micro_count, seq_len, model_width = tokens.shape
    experts = lax.axis_size(plan.swap_axes)
    capacity = 4 * seq_len // experts
    pick_total = 2 * seq_len
    bucket_count = position_bias.shape[1]
    bucket_mat = bucket_matrix(seq_len)
    positions = jnp.arange(seq_len, dtype=jnp.int32)
    causal = positions[None, :] <= positions[:, None]
    seq_numbers = jnp.arange(lengths.shape[0], dtype=jnp.int32)
    expert_numbers = jnp.arange(experts, dtype=jnp.int32)
    inner_local, outer_local = plan.gather_experts(inner_weight[0], outer_weight[0])
    (
        query_full,
        key_full,
        value_full,
        output_full,
        router_full,
        gain_one,
        gain_two,
        bias_part,
    ) = (
        lax.all_gather(weight, plan.shard_axes, axis=0, tiled=True)
        for weight in (
            query_weight,
            key_weight,
            value_weight,
            output_weight,
            router_weight,
            first_gain,
            second_gain,
            position_bias,
        )
    )
    gain_one = gain_one.astype(jnp.float32)
    gain_two = gain_two.astype(jnp.float32)

    def expand(bias_value):
        total = jnp.zeros((bias_value.shape[0], seq_len, seq_len), jnp.float32)
        for bucket in range(bucket_count):
            total = (
                total
                + bias_value[:, bucket, None, None]
                * (bucket_mat == bucket).astype(jnp.float32)[None]
            )
        return total

    mixer_running = None
    expert_running = None
    results = []
    input_grads = []
    for batch_index in range(micro_count):
        seq_length = jnp.sum(jnp.where(seq_numbers == dealing[batch_index], lengths, 0))
        valid = causal & (positions[None, :] < seq_length)
        bias_full, expand_back = jax.vjp(expand, bias_part.astype(jnp.float32))
        inputs = tokens[batch_index].astype(jnp.float32)
        normed_one, inverse_one = normalize(inputs, gain_one)
        normed_one = normed_one.astype(jnp.bfloat16)
        mixture, saved = attention_forward(
            normed_one, query_full, key_full, value_full, bias_full, valid
        )
        residual = inputs + jnp.dot(mixture, output_full, preferred_element_type=jnp.float32)
        normed_two, inverse_two = normalize(residual, gain_two)
        normed_two = normed_two.astype(jnp.bfloat16)
        router = jnp.dot(normed_two, router_full, preferred_element_type=jnp.float32)
        pick_ids = routes[batch_index]
        pick_hot = (pick_ids[:, :, None] == expert_numbers[None, None, :]).astype(jnp.float32)
        chosen = jnp.sum(router[:, None, :] * pick_hot, 2)
        chosen_exp = jnp.exp(chosen - jnp.max(chosen, 1, keepdims=True))
        gates = chosen_exp / jnp.sum(chosen_exp, 1, keepdims=True)
        slot_hot, token_hot = slot_tables(pick_ids.reshape(-1), experts, capacity, seq_len)
        send_rows = (
            jnp.dot(token_hot, normed_two, preferred_element_type=jnp.float32)
            .astype(jnp.bfloat16)
            .reshape(experts, capacity, model_width)
        )
        arrived = lax.all_to_all(send_rows, plan.swap_axes, split_axis=0, concat_axis=0, tiled=True)
        expert_rows = arrived.reshape(-1, model_width)
        pre_act = jnp.dot(expert_rows, inner_local, preferred_element_type=jnp.float32)
        activated, slope = gelu_parts(pre_act)
        hidden = activated.astype(jnp.bfloat16)
        partial_out = jnp.dot(hidden, outer_local, preferred_element_type=jnp.float32)
        expert_out = partial_out.astype(jnp.bfloat16).reshape(experts, capacity, model_width)
        returned = lax.all_to_all(
            expert_out, plan.swap_axes, split_axis=0, concat_axis=0, tiled=True
        ).reshape(-1, model_width)
        picked = jnp.einsum(
            "sp,sd->pd", slot_hot, returned, preferred_element_type=jnp.float32
        ).reshape(seq_len, 2, model_width)
        results.append((residual + jnp.sum(gates[:, :, None] * picked, 1)).astype(jnp.bfloat16))
        grad_result = cotangent[batch_index].astype(jnp.float32)
        grad_gates = jnp.sum(grad_result[:, None, :] * picked, 2)
        grad_chosen = gates * (grad_gates - jnp.sum(gates * grad_gates, 1, keepdims=True))
        grad_router = jnp.sum(grad_chosen[:, :, None] * pick_hot, 1)
        grad_picked = (
            (gates[:, :, None] * grad_result[:, None, :])
            .astype(jnp.bfloat16)
            .reshape(pick_total, model_width)
        )
        send_grads = (
            jnp.dot(slot_hot, grad_picked, preferred_element_type=jnp.float32)
            .astype(jnp.bfloat16)
            .reshape(experts, capacity, model_width)
        )
        arrived_grads = lax.all_to_all(
            send_grads, plan.swap_axes, split_axis=0, concat_axis=0, tiled=True
        )
        grad_rows = arrived_grads.reshape(-1, model_width)
        grad_hidden = jnp.dot(grad_rows, outer_local.T, preferred_element_type=jnp.float32)
        grad_pre = (grad_hidden * slope).astype(jnp.bfloat16)
        grad_outer = jnp.dot(hidden.T, grad_rows, preferred_element_type=jnp.float32)
        grad_inner = jnp.dot(expert_rows.T, grad_pre, preferred_element_type=jnp.float32)
        grad_expert_in = jnp.dot(grad_pre, inner_local.T, preferred_element_type=jnp.float32)
        grad_back = grad_expert_in.astype(jnp.bfloat16).reshape(experts, capacity, model_width)
        returned_grads = lax.all_to_all(
            grad_back, plan.swap_axes, split_axis=0, concat_axis=0, tiled=True
        ).reshape(-1, model_width)
        grad_normed_two = jnp.einsum(
            "st,sd->td", token_hot, returned_grads, preferred_element_type=jnp.float32
        )
        router_float = router_full.astype(jnp.float32)
        grad_normed_two = grad_normed_two + jnp.dot(grad_router, router_float.T, precision=HIGH)
        grad_router_weight = jnp.dot(normed_two.astype(jnp.float32).T, grad_router, precision=HIGH)
        grad_from_norm, grad_gain_two = normalize_back(
            residual, inverse_two, gain_two, grad_normed_two
        )
        grad_residual = grad_result + grad_from_norm
        grad_branch = grad_residual.astype(jnp.bfloat16)
        grad_output_weight = jnp.dot(mixture.T, grad_branch, preferred_element_type=jnp.float32)
        grad_mixture = jnp.dot(
            grad_branch, output_full.T, preferred_element_type=jnp.float32
        ).astype(jnp.bfloat16)
        grad_queries, grad_keys, grad_values, grad_logits = attention_backward(
            saved, bias_full, valid, grad_mixture
        )
        grad_bias = expand_back(grad_logits.astype(jnp.float32))[0]
        grad_query_weight = jnp.dot(normed_one.T, grad_queries, preferred_element_type=jnp.float32)
        grad_key_weight = jnp.dot(normed_one.T, grad_keys, preferred_element_type=jnp.float32)
        grad_value_weight = jnp.dot(normed_one.T, grad_values, preferred_element_type=jnp.float32)
        grad_normed_one = jnp.dot(grad_queries, query_full.T, preferred_element_type=jnp.float32)
        grad_normed_one = grad_normed_one + jnp.dot(
            grad_keys, key_full.T, preferred_element_type=jnp.float32
        )
        grad_normed_one = grad_normed_one + jnp.dot(
            grad_values, value_full.T, preferred_element_type=jnp.float32
        )
        grad_from_first, grad_gain_one = normalize_back(
            inputs, inverse_one, gain_one, grad_normed_one
        )
        input_grads.append((grad_residual + grad_from_first).astype(jnp.bfloat16))
        mixer_grads = (
            grad_query_weight,
            grad_key_weight,
            grad_value_weight,
            grad_output_weight,
            grad_router_weight,
            grad_gain_one,
            grad_gain_two,
            grad_bias,
        )
        expert_grads = (grad_inner, grad_outer)
        mixer_running = accumulate(mixer_running, mixer_grads)
        expert_running = accumulate(expert_running, expert_grads)
    grad_inner, grad_outer = plan.reduce_experts(*expert_running)
    big = plan.reduce_mixer(jnp.concatenate(mixer_running[:4], 1))
    shards = model_width // query_weight.shape[0]
    small = jnp.concatenate([part.reshape(shards, -1) for part in mixer_running[4:]], 1)
    small = lax.psum(small, plan.data_axes)
    small = lax.dynamic_index_in_dim(small, plan.shard_index(), 0, keepdims=False)
    pieces = []
    start = 0
    for like in (router_weight, first_gain, second_gain, position_bias):
        pieces.append(small[start : start + like.size].reshape(like.shape))
        start += like.size
    return (
        jnp.stack(results, 0),
        jnp.stack(input_grads, 0),
        big[:, :model_width],
        big[:, model_width : 2 * model_width],
        big[:, 2 * model_width : 3 * model_width],
        big[:, 3 * model_width :],
        *pieces,
        grad_inner[None],
        grad_outer[None],
    )


def solution(mesh):
    experts, shards = mesh.shape["expert"], mesh.shape["shard"]
    if (experts, shards) == (8, 4):
        plan = Halved()
        mesh = jax.sharding.Mesh(
            mesh.devices.reshape(2, 2, 2, 2, 2), ("zh", "zl", "x", "y", "core")
        )
        expert_axes, shard_axes = ("zh", "zl", "x"), ("y", "core")
    else:
        plan = Grouped()
        expert_axes, shard_axes = ("expert",), ("shard",)
    both = (*expert_axes, *shard_axes)
    rows = P(both, None, None)
    weight = P(shard_axes, None)
    in_specs = (rows, rows, P(), P(both), rows, *([weight] * 5))
    in_specs += (P(shard_axes), P(shard_axes), weight)
    in_specs += (P(expert_axes, None, shard_axes), P(expert_axes, shard_axes, None))
    out_specs = (rows, rows, *([weight] * 5), P(shard_axes), P(shard_axes), weight)
    out_specs += (P(expert_axes, None, shard_axes), P(expert_axes, shard_axes, None))
    return jax.shard_map(
        functools.partial(body, plan),
        mesh=mesh,
        in_specs=in_specs,
        out_specs=out_specs,
        check_vma=False,
    )
```

```python
import functools
import math

import jax
import jax.numpy as jnp
import numpy as np
from jax import lax
from jax.experimental import pallas as pl
from jax.experimental.pallas import tpu as pltpu
from jax.sharding import PartitionSpec as P

EPSILON = 1e-06
HIGH = lax.Precision.HIGHEST
NEGATIVE = -1000000000.0
INV_ROOT_TWO = 1.0 / math.sqrt(2.0)
INV_ROOT_TAU = 1.0 / math.sqrt(2.0 * math.pi)
LANES = 128


def bucket_table(length):
    distance = np.arange(length)
    scaled = 16 + np.floor(np.log(np.maximum(distance, 1) / 16.0) / np.log(8.0) * 16.0)
    return np.where(distance < 16, distance, np.minimum(scaled, 31)).astype(np.int32)


def gelu_parts(pre_act):
    normal_cdf = 0.5 * (1.0 + lax.erf(pre_act * INV_ROOT_TWO))
    return (
        pre_act * normal_cdf,
        normal_cdf + pre_act * jnp.exp(-0.5 * pre_act * pre_act) * INV_ROOT_TAU,
    )


def distance_table(length):
    offsets = np.arange(length // LANES)[:, None] * LANES
    return offsets, np.arange(2 * LANES)[None, :]


def spread_hot(length, bucket_count):
    offsets, lanes = distance_table(length)
    signed = np.where(lanes < LANES, lanes, lanes - 2 * LANES)
    distance = np.clip(offsets - signed, 0, length - 1).reshape(-1)
    return (bucket_table(length)[distance][None, :] == np.arange(bucket_count)[:, None]).astype(
        np.float32
    )


def collect_hot(length, bucket_count):
    offsets, lanes = distance_table(length)
    distance = (offsets + LANES - 1 - lanes).reshape(-1)
    inside = (distance >= 0) & (distance < length)
    table = bucket_table(length)[np.clip(distance, 0, length - 1)]
    return ((table[:, None] == np.arange(bucket_count)[None, :]) & inside[:, None]).astype(
        np.float32
    )


def half_mask(head):
    lane = lax.broadcasted_iota(jnp.int32, (1, LANES), 1)
    return (lane < LANES // 2) if head == 0 else (lane >= LANES // 2)


def only(value, head):
    return jnp.where(half_mask(head), value, jnp.zeros_like(value))


def nt_dot(left, right):
    return lax.dot_general(
        left, right, (((1,), (1,)), ((), ())), preferred_element_type=jnp.float32
    )


def tn_dot(left, right):
    return lax.dot_general(
        left, right, (((0,), (0,)), ((), ())), preferred_element_type=jnp.float32
    )


def toeplitz_block(row):
    spread = pltpu.roll(
        jnp.broadcast_to(row, (LANES, 2 * LANES)), 0, 1, stride=1, stride_axis=0
    )
    return spread[:, :LANES]


def fill_bias(bias_ref, table_ref, blocks):
    for head in range(2):
        for offset in range(blocks):
            table_ref[head, offset] = toeplitz_block(bias_ref[0, head, offset, :][None, :])


def masked_logits(query, keys, table_ref, head, block, length):
    width = (block + 1) * LANES
    bias = jnp.concatenate([table_ref[head, block - j] for j in range(block + 1)], 1)
    logits = nt_dot(query, keys) * ((LANES // 2) ** (-0.5)) + bias
    row = lax.broadcasted_iota(jnp.int32, (LANES, width), 0) + block * LANES
    column = lax.broadcasted_iota(jnp.int32, (LANES, width), 1)
    return jnp.where((column <= row) & (column < length), logits, NEGATIVE)


SLOTS = 192


def unit(value):
    return lax.rsqrt(jnp.mean(value * value, -1, keepdims=True) + EPSILON)


def column_iota(rows, columns):
    return lax.broadcasted_iota(jnp.int32, (rows, columns), 1)


def row_iota(rows, columns):
    return lax.broadcasted_iota(jnp.int32, (rows, columns), 0)


def row_places(routes_t_ref, experts, capacity):
    tokens = routes_t_ref.shape[1]
    padded = -(-experts // 16) * 16
    expert = row_iota(padded, tokens)
    hot = [expert == routes_t_ref[pick : pick + 1, :] for pick in range(2)]
    both = jnp.where(hot[0] | hot[1], 1.0, 0.0).astype(jnp.bfloat16)
    before = (row_iota(tokens, tokens) < column_iota(tokens, tokens)).astype(jnp.float32)
    rank = jnp.dot(both, before.astype(jnp.bfloat16), preferred_element_type=jnp.float32)
    slot = rank + (expert * capacity).astype(jnp.float32)
    return [jnp.sum(jnp.where(chosen, slot, 0.0), 0, keepdims=True) for chosen in hot]


def column_places(routes_ref, experts, capacity):
    tokens = routes_ref.shape[0]
    expert = column_iota(tokens, LANES)
    hot = [expert == routes_ref[:, pick : pick + 1] for pick in range(2)]
    both = jnp.where(hot[0] | hot[1], 1.0, 0.0).astype(jnp.bfloat16)
    before = (column_iota(tokens, tokens) < row_iota(tokens, tokens)).astype(jnp.float32)
    rank = jnp.dot(before.astype(jnp.bfloat16), both, preferred_element_type=jnp.float32)
    slot = rank + (expert * capacity).astype(jnp.float32)
    return [jnp.sum(jnp.where(chosen, slot, 0.0), 1, keepdims=True) for chosen in hot], hot


def one_hot(condition):
    return jnp.where(condition, 1.0, 0.0).astype(jnp.bfloat16)


def forward_math(
    experts,
    capacity,
    length,
    x_ref,
    g_ref,
    routes_ref,
    routes_t_ref,
    query_ref,
    key_ref,
    value_ref,
    output_ref,
    router_ref,
    gain_ref,
    bias_ref,
    sent_ref,
    normed_ref,
    q_ref,
    k_ref,
    v_ref,
    mix_ref,
    residual_ref,
    gates_ref,
    table_ref,
):
    tokens, width = x_ref.shape
    blocks = tokens // LANES
    inputs = x_ref[...].astype(jnp.float32)
    normed = (inputs * unit(inputs) * gain_ref[0:1, :]).astype(jnp.bfloat16)
    normed_ref[...] = normed
    for weight, out in ((query_ref, q_ref), (key_ref, k_ref), (value_ref, v_ref)):
        out[...] = jnp.dot(normed, weight[...], preferred_element_type=jnp.float32).astype(
            jnp.bfloat16
        )

    def attend(pair, carry):
        lanes = pl.ds(pl.multiple_of(pair * LANES, LANES), LANES)
        fill_bias(bias_ref.at[pl.ds(pair, 1)], table_ref, blocks)
        for block in range(blocks):
            rows = pl.ds(block * LANES, LANES)
            reach = (block + 1) * LANES
            mixed = jnp.zeros((LANES, LANES), jnp.float32)
            for head in range(2):
                logits = masked_logits(
                    only(q_ref[rows, lanes], head),
                    k_ref[:reach, lanes],
                    table_ref,
                    head,
                    block,
                    length,
                )
                exponent = jnp.exp(logits - jnp.max(logits, 1, keepdims=True))
                soft = exponent / jnp.sum(exponent, 1, keepdims=True)
                mixed = mixed + jnp.dot(
                    soft.astype(jnp.bfloat16),
                    only(v_ref[:reach, lanes], head),
                    preferred_element_type=jnp.float32,
                )
            mix_ref[rows, lanes] = mixed.astype(jnp.bfloat16)
        return carry

    lax.fori_loop(0, width // LANES, attend, 0)
    residual = inputs + jnp.dot(
        mix_ref[...], output_ref[...], preferred_element_type=jnp.float32
    )
    residual_ref[...] = residual
    normed = (residual * unit(residual) * gain_ref[1:2, :]).astype(jnp.bfloat16)
    router = jnp.dot(normed, router_ref[...], preferred_element_type=jnp.float32)
    lane = column_iota(tokens, LANES)
    chosen = [
        jnp.sum(jnp.where(lane == routes_ref[:, pick : pick + 1], router, 0.0), 1, keepdims=True)
        for pick in range(2)
    ]
    top = jnp.maximum(chosen[0], chosen[1])
    gates = [jnp.exp(value - top) for value in chosen]
    total = gates[0] + gates[1]
    gates = [value / total for value in gates]
    gates_ref[...] = jnp.where(lane == 0, gates[0], jnp.where(lane == 1, gates[1], 0.0))
    grads = [(g_ref[...].astype(jnp.float32) * gate).astype(jnp.bfloat16) for gate in gates]
    places = row_places(routes_t_ref, experts, capacity)
    slots = sent_ref.shape[2]
    for index in range(sent_ref.shape[0]):
        slot = (row_iota(slots, tokens) + index * slots).astype(jnp.float32)
        hot = [jnp.where(slot == place, 1.0, 0.0) for place in places]
        sent_ref[index, 0] = jnp.dot(
            (hot[0] + hot[1]).astype(jnp.bfloat16), normed, preferred_element_type=jnp.float32
        ).astype(jnp.bfloat16)
        sent_ref[index, 1] = (
            jnp.dot(hot[0].astype(jnp.bfloat16), grads[0], preferred_element_type=jnp.float32)
            + jnp.dot(hot[1].astype(jnp.bfloat16), grads[1], preferred_element_type=jnp.float32)
        ).astype(jnp.bfloat16)


def forward_kernel(experts, capacity, length_ref, *refs):
    forward_math(experts, capacity, length_ref[0], *refs)


def split(value):
    high = value.astype(jnp.bfloat16)
    return high, (value - high.astype(jnp.float32)).astype(jnp.bfloat16)


def norm_back(value, gain, grad):
    scale = unit(value)
    rows = value * scale
    grad_unit = grad * gain
    grad_gain = jnp.sum(grad * rows, 0, keepdims=True)
    mean = jnp.mean(grad_unit * rows, -1, keepdims=True)
    return scale * (grad_unit - rows * mean), grad_gain


def backward_math(
    experts,
    capacity,
    tick,
    length,
    x_ref,
    g_ref,
    routes_ref,
    query_ref,
    key_ref,
    value_ref,
    output_ref,
    router_ref,
    gain_ref,
    bias_ref,
    q_ref,
    k_ref,
    v_ref,
    residual_ref,
    gates_ref,
    out_rows_ref,
    back_rows_ref,
    result_ref,
    input_grad_ref,
    branch_ref,
    dq_ref,
    dk_ref,
    dv_ref,
    router_grad_ref,
    gain_grad_ref,
    diag_ref,
    grad_mix_ref,
    grad_residual_ref,
    table_ref,
    dk_sum,
    dv_sum,
    skew_ref,
):
    tokens, width = x_ref.shape
    blocks = tokens // LANES
    scale = (LANES // 2) ** (-0.5)
    grad_result = g_ref[...].astype(jnp.float32)
    residual = residual_ref[...]
    places, picks = column_places(routes_ref, experts, capacity)
    gates = [gates_ref[:, pick : pick + 1] for pick in range(2)]
    slots = out_rows_ref.shape[1]
    picked = [jnp.zeros((tokens, width), jnp.float32) for _ in range(2)]
    grad_normed = jnp.zeros((tokens, width), jnp.float32)
    for index in range(0, out_rows_ref.shape[0], 2):
        slot = (column_iota(tokens, 2 * slots) + index * slots).astype(jnp.float32)
        hot = [jnp.where(slot == place, 1.0, 0.0) for place in places]
        out_rows = out_rows_ref[index : index + 2].reshape(2 * slots, width)
        back_rows = back_rows_ref[index : index + 2].reshape(2 * slots, width)
        for pick in range(2):
            picked[pick] = picked[pick] + jnp.dot(
                hot[pick].astype(jnp.bfloat16), out_rows, preferred_element_type=jnp.float32
            )
        grad_normed = grad_normed + jnp.dot(
            (hot[0] + hot[1]).astype(jnp.bfloat16), back_rows, preferred_element_type=jnp.float32
        )
    result_ref[...] = (residual + (gates[0] * picked[0] + gates[1] * picked[1])).astype(
        jnp.bfloat16
    )
    grad_gates = [jnp.sum(grad_result * rows, 1, keepdims=True) for rows in picked]
    common = gates[0] * grad_gates[0] + gates[1] * grad_gates[1]
    grad_router = jnp.zeros((tokens, LANES), jnp.float32)
    for pick in range(2):
        grad_router = grad_router + jnp.where(
            picks[pick], gates[pick] * (grad_gates[pick] - common), 0.0
        )
    normed = (residual * unit(residual) * gain_ref[1:2, :]).astype(jnp.bfloat16)
    router_grad = jnp.zeros((width, LANES), jnp.float32)
    for part in split(grad_router):
        grad_normed = grad_normed + nt_dot(part, router_ref[...])
        router_grad = router_grad + tn_dot(normed, part)
    router_grad_ref[...] = router_grad
    from_norm, grad_gain = norm_back(residual, gain_ref[1:2, :], grad_normed)
    gain_grad_ref[1:2, :] = grad_gain
    grad_residual = grad_result + from_norm
    grad_residual_ref[...] = grad_residual
    branch = grad_residual.astype(jnp.bfloat16)
    branch_ref[...] = branch
    grad_mix_ref[...] = nt_dot(branch, output_ref[...]).astype(jnp.bfloat16)
    tick()

    row, column = row_iota(LANES, LANES), column_iota(LANES, LANES)
    upside = (row + column == LANES - 1).astype(jnp.float32)

    def attend_back(pair, carry):
        lanes = pl.ds(pl.multiple_of(pair * LANES, LANES), LANES)
        fill_bias(bias_ref.at[pl.ds(pair, 1)], table_ref, blocks)
        dk_sum[...] = jnp.zeros_like(dk_sum)
        dv_sum[...] = jnp.zeros_like(dv_sum)
        skew_ref[...] = jnp.zeros_like(skew_ref)
        for block in range(blocks):
            rows = pl.ds(block * LANES, LANES)
            reach = (block + 1) * LANES
            dq = jnp.zeros((LANES, LANES), jnp.float32)
            for head in range(2):
                query = only(q_ref[rows, lanes], head)
                grad = only(grad_mix_ref[rows, lanes], head)
                keys = k_ref[:reach, lanes]
                logits = masked_logits(query, keys, table_ref, head, block, length)
                exponent = jnp.exp(logits - jnp.max(logits, 1, keepdims=True))
                soft = exponent / jnp.sum(exponent, 1, keepdims=True)
                grad_soft = nt_dot(grad, v_ref[:reach, lanes])
                inner = jnp.sum(soft * grad_soft, 1, keepdims=True)
                grad_logits = (soft * (grad_soft - inner)).astype(jnp.bfloat16)
                dv_sum[:reach, :] += tn_dot(soft.astype(jnp.bfloat16), grad)
                dk_sum[:reach, :] += tn_dot(grad_logits, query)
                dq = dq + jnp.dot(
                    grad_logits, only(keys, head), preferred_element_type=jnp.float32
                )
                wide = grad_logits.astype(jnp.float32)
                for j in range(block + 1):
                    skew_ref[head, block - j] += wide[:, j * LANES : (j + 1) * LANES]
            dq_ref[rows, lanes] = (dq * scale).astype(jnp.bfloat16)
        dk_ref[:, lanes] = (dk_sum[...] * scale).astype(jnp.bfloat16)
        dv_ref[:, lanes] = dv_sum[...].astype(jnp.bfloat16)
        for head in range(2):
            for offset in range(blocks):
                flipped = jnp.dot(
                    upside,
                    skew_ref[head, offset],
                    precision=HIGH,
                    preferred_element_type=jnp.float32,
                )
                padded = jnp.concatenate([flipped, jnp.zeros_like(flipped)], 1)
                lined = pltpu.roll(padded, 0, 1, stride=1, stride_axis=0)
                diag_ref[pair, head, offset, :] = jnp.sum(lined, 0)
        return carry

    pairs = width // LANES
    lax.fori_loop(0, pairs // 2, attend_back, 0)
    tick()
    lax.fori_loop(pairs // 2, pairs, attend_back, 0)
    tick()
    grad_normed = nt_dot(dq_ref[...], query_ref[...])
    grad_normed = grad_normed + nt_dot(dk_ref[...], key_ref[...])
    grad_normed = grad_normed + nt_dot(dv_ref[...], value_ref[...])
    inputs = x_ref[...].astype(jnp.float32)
    from_norm, grad_gain = norm_back(inputs, gain_ref[0:1, :], grad_normed)
    gain_grad_ref[0:1, :] = grad_gain
    input_grad_ref[...] = (grad_residual_ref[...] + from_norm).astype(jnp.bfloat16)


def backward_kernel(experts, capacity, length_ref, *refs):
    backward_math(experts, capacity, lambda: None, length_ref[0], *refs)


VMEM = pl.BlockSpec(memory_space=pltpu.VMEM)
SMEM = pl.BlockSpec(memory_space=pltpu.SMEM)


def layer_forward(index, experts, capacity, length, x, g, routes, routes_t, weights, router, gains, bias):
    _, tokens, width = x.shape
    blocks = tokens // LANES
    flat = jax.ShapeDtypeStruct((tokens, width), jnp.bfloat16)
    rows = pl.BlockSpec((None, tokens, width), lambda i: (index, 0, 0))
    return pl.pallas_call(
        functools.partial(forward_kernel, experts, capacity),
        grid=(1,),
        out_shape=(
            jax.ShapeDtypeStruct((experts * capacity // SLOTS, 2, SLOTS, width), jnp.bfloat16),
            flat,
            flat,
            flat,
            flat,
            flat,
            jax.ShapeDtypeStruct((tokens, width), jnp.float32),
            jax.ShapeDtypeStruct((tokens, LANES), jnp.float32),
        ),
        in_specs=[SMEM, rows, rows, *([VMEM] * 9)],
        out_specs=[VMEM] * 8,
        scratch_shapes=[pltpu.VMEM((2, blocks, LANES, LANES), jnp.float32)],
        compiler_params=pltpu.CompilerParams(vmem_limit_bytes=56 * 2**20),
        cost_estimate=pl.CostEstimate(
            flops=2 * tokens * width * (4 * width + 4 * tokens + 6 * tokens),
            bytes_accessed=40 * tokens * width,
            transcendentals=tokens * tokens * 12,
        ),
        name="layer_forward",
    )(length, x, g, routes, routes_t, *weights, router, gains, bias)


def layer_backward(
    index, experts, capacity, length, x, g, routes, weights, router, gains, bias, saved, returned
):
    _, tokens, width = x.shape
    blocks = tokens // LANES
    flat = jax.ShapeDtypeStruct((tokens, width), jnp.bfloat16)
    _, count, _, slots, _ = returned.shape

    def one(array):
        return pl.BlockSpec((None, *array.shape[1:]), lambda i: (index, 0, 0))

    rows = one(x)

    def side(which):
        return pl.BlockSpec(
            (None, count, None, slots, width), lambda i: (index, 0, which, 0, 0)
        )

    return pl.pallas_call(
        functools.partial(backward_kernel, experts, capacity),
        grid=(1,),
        out_shape=(
            *([flat] * 6),
            jax.ShapeDtypeStruct((width, LANES), jnp.float32),
            jax.ShapeDtypeStruct((2, width), jnp.float32),
            jax.ShapeDtypeStruct(bias.shape, jnp.float32),
        ),
        in_specs=[
            SMEM,
            rows,
            rows,
            one(routes),
            *([VMEM] * 7),
            *map(one, saved),
            side(0),
            side(1),
        ],
        out_specs=[VMEM] * 9,
        scratch_shapes=[
            pltpu.VMEM((tokens, width), jnp.bfloat16),
            pltpu.VMEM((tokens, width), jnp.float32),
            pltpu.VMEM((2, blocks, LANES, LANES), jnp.float32),
            pltpu.VMEM((tokens, LANES), jnp.float32),
            pltpu.VMEM((tokens, LANES), jnp.float32),
            pltpu.VMEM((2, blocks, LANES, LANES), jnp.float32),
        ],
        compiler_params=pltpu.CompilerParams(vmem_limit_bytes=56 * 2**20),
        cost_estimate=pl.CostEstimate(
            flops=2 * tokens * width * (4 * width + 12 * tokens + 10 * tokens),
            bytes_accessed=40 * tokens * width,
            transcendentals=tokens * tokens * 12,
        ),
        name="layer_backward",
    )(length, x, g, routes, *weights, router, gains, bias, *saved, returned, returned)


def expert_kernel(count, x_ref, g_ref, *refs):
    inner_refs, outer_refs = refs[:count], refs[count : 2 * count]
    back_ref, hidden_ref, grad_ref = refs[2 * count :]
    shape = x_ref.shape
    inputs = x_ref[...].reshape(-1, shape[-1])
    grads = g_ref[...].reshape(-1, shape[-1])
    out = jnp.zeros(inputs.shape, jnp.float32)
    back = jnp.zeros(inputs.shape, jnp.float32)
    start = 0
    for inner_ref, outer_ref in zip(inner_refs, outer_refs):
        part = pl.ds(start, inner_ref.shape[1])
        start += inner_ref.shape[1]
        pre_act = jnp.dot(inputs, inner_ref[...], preferred_element_type=jnp.float32)
        activated, slope = gelu_parts(pre_act)
        hidden = activated.astype(jnp.bfloat16)
        grad_pre = (nt_dot(grads, outer_ref[...]) * slope).astype(jnp.bfloat16)
        hidden_ref[:, part] = hidden
        grad_ref[:, part] = grad_pre
        out = out + jnp.dot(hidden, outer_ref[...], preferred_element_type=jnp.float32)
        back = back + nt_dot(grad_pre, inner_ref[...])
    back_ref[:, 0] = out.astype(jnp.bfloat16).reshape(shape)
    back_ref[:, 1] = back.astype(jnp.bfloat16).reshape(shape)


def expert_pass(arrived, inner, outer):
    sources, _, capacity, width = arrived.shape
    total = sources * capacity
    units = sum(part.shape[1] for part in inner)
    group = sources // 4

    def side(which):
        return pl.BlockSpec((group, None, capacity, width), lambda i: (i, which, 0, 0))

    def whole(shape):
        return pl.BlockSpec(shape, lambda i: (0, 0), pipeline_mode=pl.Buffered(1))

    unit_spec = pl.BlockSpec((group * capacity, units), lambda i: (i, 0))
    deep = jax.ShapeDtypeStruct((total, units), jnp.bfloat16)
    return pl.pallas_call(
        functools.partial(expert_kernel, len(inner)),
        grid=(sources // group,),
        out_shape=(jax.ShapeDtypeStruct(arrived.shape, jnp.bfloat16), deep, deep),
        in_specs=[side(0), side(1), *(whole(part.shape) for part in (*inner, *outer))],
        out_specs=(
            pl.BlockSpec((group, 2, capacity, width), lambda i: (i, 0, 0, 0)),
            unit_spec,
            unit_spec,
        ),
        compiler_params=pltpu.CompilerParams(vmem_limit_bytes=60 * 2**20),
        cost_estimate=pl.CostEstimate(
            flops=8 * total * width * units,
            bytes_accessed=4 * (2 * width + units) * total + 4 * width * units,
            transcendentals=2 * total * units,
        ),
        name="expert_pass",
    )(arrived, arrived, *inner, *outer)


def weight_kernel(x0_ref, x1_ref, g0_ref, g1_ref, p0_ref, p1_ref, h0_ref, h1_ref, *out_refs):
    inner_ref, outer_ref = out_refs

    def flat(ref):
        return ref[...].reshape(-1, ref.shape[-1])

    inner = tn_dot(flat(x0_ref), p0_ref[...]) + tn_dot(flat(x1_ref), p1_ref[...])
    inner_ref[...] = inner.astype(jnp.bfloat16)
    outer = tn_dot(h0_ref[...], flat(g0_ref)) + tn_dot(h1_ref[...], flat(g1_ref))
    outer_ref[...] = outer.astype(jnp.bfloat16)


def weight_pass(first, count, chunks, arrived, pres, hiddens):
    sources, _, capacity, width = arrived[0].shape
    total = sources * capacity
    size = hiddens[0].shape[1] // chunks
    step = math.gcd(size, 256)
    steps = size // step

    def side(which):
        return pl.BlockSpec(
            (sources, None, capacity, width),
            lambda i: (0, which, 0, 0),
            pipeline_mode=pl.Buffered(1),
        )

    units = pl.BlockSpec((total, step), lambda i: (0, first * steps + i))
    inner, outer = pl.pallas_call(
        weight_kernel,
        grid=(count * steps,),
        out_shape=(
            jax.ShapeDtypeStruct((count, width, size), jnp.bfloat16),
            jax.ShapeDtypeStruct((count * size, width), jnp.bfloat16),
        ),
        in_specs=[side(0)] * 2 + [side(1)] * 2 + [units] * 4,
        out_specs=(
            pl.BlockSpec((None, width, step), lambda i: (i // steps, 0, i % steps)),
            pl.BlockSpec((step, width), lambda i: (i, 0)),
        ),
        compiler_params=pltpu.CompilerParams(vmem_limit_bytes=60 * 2**20),
        cost_estimate=pl.CostEstimate(
            flops=8 * total * width * count * size,
            bytes_accessed=8 * total * (width + count * size) + 4 * width * count * size,
            transcendentals=0,
        ),
        name="weight_pass",
    )(*arrived, *arrived, *pres, *hiddens)
    return list(inner), list(outer.reshape(count, size, width))


FOLD_ORDERS = (("y", "x", "zl", "zh"), ("x", "zl", "y", "zh"), ("zl", "y", "x", "zh"))


def greet(axes):
    barrier = pltpu.get_barrier_semaphore()
    for axis in axes:
        pl.semaphore_signal(
            barrier,
            inc=1,
            device_id={axis: 1 - lax.axis_index(axis)},
            device_id_type=pl.DeviceIdType.MESH,
        )
    pl.semaphore_wait(barrier, len(axes))


def push(source, target, send_sem, recv_sem, axis):
    copy = pltpu.make_async_remote_copy(
        src_ref=source,
        dst_ref=target,
        send_sem=send_sem,
        recv_sem=recv_sem,
        device_id={axis: 1 - lax.axis_index(axis)},
        device_id_type=pl.DeviceIdType.MESH,
    )
    copy.start()
    return copy


def fold_math(operands, ready_ref, outs, grads, sums, inboxes, send_sem, recv_sem):
    count = len(outs)
    grads = [*grads, ready_ref]
    mine = {axis: lax.axis_index(axis) for axis in ("core", "y", "x", "zl", "zh")}
    core = mine["core"]
    orders = [FOLD_ORDERS[i % len(FOLD_ORDERS)] for i in range(count)]

    def cut(ref, i, depth, axes, partner=None):
        done = orders[i][:depth]
        place = dict(mine)
        if partner is not None:
            place[partner] = 1 - place[partner]
        index = [place[axis] if axis in done else slice(None) for axis in axes]
        columns = slice(None)
        if "zh" in done:
            width = ref.shape[-1] // 2
            columns = pl.ds(pl.multiple_of(place["zh"] * width, LANES), width)
        return ref.at[(*index, slice(None), columns)]

    spread, joined = ("y", "x", "zl"), ("x", "zl")
    started = []
    flying = []
    for i in range(count):
        if i < count - 1:
            left_0, right_0, left_1, right_1 = operands[i]
            total = tn_dot(left_0[...], right_0[...]) + tn_dot(left_1[...], right_1[...])
            grads[i][...] = total.astype(jnp.bfloat16).reshape(grads[i].shape)
        flying.append(
            push(
                grads[i].at[:, 1 - core],
                inboxes[0][i],
                send_sem.at[i, 0],
                recv_sem.at[i, 0],
                "core",
            )
        )
    for step in range(5):
        for i in range(count):
            flying[i].wait_recv()
            if step == 0:
                sums[i][...] = (
                    grads[i][:, core].astype(jnp.float32)
                    + inboxes[0][i][...].astype(jnp.float32)
                ).astype(jnp.bfloat16)
            else:
                kept = cut(sums[i], i, step, spread)
                total = kept[...].astype(jnp.float32) + inboxes[step][i][...].astype(jnp.float32)
                kept[...] = total.astype(jnp.bfloat16)
            started.append(flying[i])
            if step < 4:
                axis = orders[i][step]
                flying[i] = push(
                    cut(sums[i], i, step + 1, spread, axis),
                    inboxes[step + 1][i],
                    send_sem.at[i, step + 1],
                    recv_sem.at[i, step + 1],
                    axis,
                )
    for i in range(count):
        cut(outs[i], i, 4, joined)[...] = cut(sums[i], i, 4, spread)[...]
    left = [[axis for axis in reversed(order)] for order in orders]
    for step in range(4):
        for i in range(count):
            if step:
                if flying[i] is not None:
                    flying[i].wait_recv()
                    started.append(flying[i])
            axis = left[i][step]
            flying[i] = None
            if axis != "y":
                place = cut(outs[i], i, 4 - step, joined)
                flying[i] = push(
                    place, place, send_sem.at[i, 5 + step], recv_sem.at[i, 5 + step], axis
                )
    for i in range(count):
        if flying[i] is not None:
            flying[i].wait_recv()
            started.append(flying[i])
    for copy in started:
        copy.wait_send()


PEER_AXES = ("y", "zl", "x")
CHUNKS = 4


def peer_of(step):
    target, block = {}, 0
    for bit, axis in enumerate(reversed(PEER_AXES)):
        place = lax.axis_index(axis)
        if step >> bit & 1:
            place = 1 - place
            target[axis] = place
        block = block + place * (1 << bit)
    return target, block


def send(source, target, send_sem, recv_sem, device):
    copy = pltpu.make_async_remote_copy(
        src_ref=source,
        dst_ref=target,
        send_sem=send_sem,
        recv_sem=recv_sem,
        device_id=device,
        device_id_type=pl.DeviceIdType.MESH,
    )
    copy.start()
    return copy


def meet(devices):
    barrier = pltpu.get_barrier_semaphore()
    for device in devices:
        pl.semaphore_signal(
            barrier, inc=1, device_id=device, device_id_type=pl.DeviceIdType.MESH
        )
    pl.semaphore_wait(barrier, len(devices))


def across(axis):
    return {axis: 1 - lax.axis_index(axis)}


def head_kernel(
    experts,
    capacity,
    lengths_ref,
    x_ref,
    g_ref,
    routes_ref,
    routes_t_ref,
    inner_ref,
    outer_ref,
    *refs,
):
    count = 6
    parts, refs = refs[:count], refs[count:]
    wholes, refs = refs[:count], refs[count:]
    inner_outs, outer_outs, refs = refs[:4], refs[4:8], refs[8:]
    arrived_ref, refs = refs[0], refs[1:]
    normed_ref, q_ref, k_ref, v_ref, mix_ref, residual_ref, gates_ref, gain_ref, bias_ref = refs[:9]
    refs = refs[9:]
    sent_refs, relays = refs[:2], refs[2:4]
    table_ref = refs[4]
    mixer_send, mixer_recv, move_send, move_recv, row_send, row_recv, local_sem = refs[5:]
    core, y, x, zh = (lax.axis_index(axis) for axis in ("core", "y", "x", "zh"))
    at_home = zh == y
    away = zh != y
    batch, tokens, width = x_ref.shape

    meet([across("core"), across("zh"), *(peer_of(step)[0] for step in range(1, 8))])

    sources = (inner_ref, outer_ref)
    outs = (inner_outs, outer_outs)
    rows = inner_ref.shape[0] // CHUNKS

    def piece(ref, chunk):
        return ref.at[pl.ds(chunk * rows, rows)]

    class Moves:
        @staticmethod
        def copy(which, chunk, kind, source, target, axis):
            return pltpu.make_async_remote_copy(
                src_ref=piece(source, chunk),
                dst_ref=piece(target, chunk),
                send_sem=move_send.at[which, chunk, kind],
                recv_sem=move_recv.at[which, chunk, kind],
                device_id=across(axis),
                device_id_type=pl.DeviceIdType.MESH,
            )

    def move_z(which, chunk):
        source = sources[which]

        @pl.when(at_home)
        def _():
            Moves.copy(which, chunk, 0, source, outs[which][0], "zh").start()

        @pl.when(away)
        def _():
            Moves.copy(which, chunk, 0, source, relays[which], "zh").start()

    def move_first(which, chunk):
        source = sources[which]

        @pl.when(away)
        def _():
            Moves.copy(which, chunk, 1, source, outs[which][2], "y").start()

        @pl.when(at_home)
        def _():
            Moves.copy(which, chunk, 2, source, outs[which][1], "core").start()

    def relay_z(which, chunk):
        @pl.when(at_home)
        def _():
            Moves.copy(which, chunk, 0, sources[which], relays[which], "zh").wait_recv()
            Moves.copy(which, chunk, 1, relays[which], outs[which][2], "y").start()

        @pl.when(away)
        def _():
            Moves.copy(which, chunk, 0, sources[which], outs[which][0], "zh").wait_recv()
            Moves.copy(which, chunk, 2, outs[which][0], outs[which][1], "core").start()

    def relay_y(which, chunk):
        Moves.copy(which, chunk, 1, sources[which], outs[which][2], "y").wait_recv()
        Moves.copy(which, chunk, 3, outs[which][2], outs[which][3], "core").start()

    def finish(which, chunk):
        for kind, axis in ((2, "core"), (3, "core")):
            Moves.copy(which, chunk, kind, sources[which], outs[which][1], axis).wait_recv()
        for kind, axis in ((0, "zh"), (1, "y"), (2, "core"), (3, "core")):
            Moves.copy(which, chunk, kind, sources[which], outs[which][1], axis).wait_send()

    def half(part, which):
        size = part.shape[0] // 2
        return pl.ds(pl.multiple_of(which * size, size), size)

    def spot(part, whole, y_at, core_at, half_at=None):
        size = part.shape[0]
        start = (y_at * 2 + core_at) * size
        if half_at is not None:
            size = size // 2
            start = start + half_at * size
        return whole.at[pl.ds(pl.multiple_of(start, size), size)]

    mixers = []
    for i, (part, whole) in enumerate(zip(parts, wholes)):
        for j, axis in enumerate(("y", "core")):
            source = part if axis == "core" else part.at[half(part, x)]
            place = spot(part, whole, y, core, x if axis == "y" else None)
            mixers.append(push(source, place, mixer_send.at[i, j], mixer_recv.at[i, j], axis))
    for chunk in range(CHUNKS):
        move_z(0, chunk)
    for i, (part, whole) in enumerate(zip(parts, wholes)):
        spot(part, whole, y, core)[...] = part[...]
    for i, whole in enumerate(wholes):
        mixers[2 * i].wait_recv()
        place = spot(parts[i], whole, 1 - y, core, x)
        for j, axis in ((2, "x"), (3, "core")):
            mixers.append(push(place, place, mixer_send.at[i, j], mixer_recv.at[i, j], axis))
    for i, whole in enumerate(wholes):
        mixers[2 * count + 2 * i].wait_recv()
        place = spot(parts[i], whole, 1 - y, core, 1 - x)
        mixers.append(push(place, place, mixer_send.at[i, 4], mixer_recv.at[i, 4], "core"))
    for which in range(2):
        for chunk in range(CHUNKS):
            move_first(which, chunk)

    @pl.when(at_home)
    def _():
        for which in range(2):
            pltpu.make_async_copy(sources[which], outs[which][0], local_sem.at[which]).start()

    for i in range(count):
        mixers[2 * i + 1].wait_recv()
        mixers[2 * count + 2 * i + 1].wait_recv()
        mixers[4 * count + i].wait_recv()

    misc = wholes[5][...].astype(jnp.float32)
    per_shard = misc.shape[0] // 4
    for i in range(2):
        line = sum(misc[s * per_shard + 3 + i : s * per_shard + 4 + i, :] for s in range(4))
        gain_ref[i : i + 1, :] = line
    for head in range(4 * 3):
        row = (head // 3) * per_shard + head % 3
        for offset in range(bias_ref.shape[2]):
            bias_ref[head // 2, head % 2, offset : offset + 1, :] = misc[
                row : row + 1, offset * 2 * LANES : (offset + 1) * 2 * LANES
            ]

    rows_flying = []
    for b in range(batch):
        forward_math(
            experts,
            capacity,
            lengths_ref[b],
            x_ref.at[b],
            g_ref.at[b],
            routes_ref.at[b],
            routes_t_ref.at[b],
            *wholes[:5],
            gain_ref,
            bias_ref,
            sent_refs[b],
            normed_ref.at[b],
            q_ref.at[b],
            k_ref.at[b],
            v_ref.at[b],
            mix_ref.at[b],
            residual_ref.at[b],
            gates_ref.at[b],
            table_ref,
        )
        _, mine = peer_of(0)
        local = pltpu.make_async_copy(
            sent_refs[b].at[mine], arrived_ref.at[b, mine], local_sem.at[2 + b]
        )
        local.start()
        rows_flying.append(local)
        for turn, step in enumerate((7, 1, 6, 2, 5, 3, 4)):
            target, block = peer_of(step)
            copy = send(
                sent_refs[b].at[block],
                arrived_ref.at[b, mine],
                row_send.at[b, step - 1],
                row_recv.at[b, step - 1],
                target,
            )
            rows_flying.append(copy)
            if b == 0 and turn % 2 == 0:
                move_z(1, turn // 2)
        if b == 0:
            for chunk in range(CHUNKS):
                relay_z(0, chunk)
    for chunk in range(CHUNKS):
        relay_y(0, chunk)
    for chunk in range(CHUNKS):
        relay_z(1, chunk)
    for chunk in range(CHUNKS):
        relay_y(1, chunk)
    for which in range(2):
        for chunk in range(CHUNKS):
            finish(which, chunk)

    @pl.when(at_home)
    def _():
        for which in range(2):
            pltpu.make_async_copy(sources[which], outs[which][0], local_sem.at[which]).wait()

    for copy in mixers:
        copy.wait_send()
    for copy in rows_flying:
        copy.wait()


def layer_head(experts, capacity, lengths, x, g, routes, routes_t, inner, outer, parts, bias_shape):
    batch, tokens, width = x.shape
    blocks = tokens // LANES
    count = len(parts)
    shape = jax.ShapeDtypeStruct
    wholes = [shape((4 * part.shape[0], part.shape[1]), part.dtype) for part in parts]
    moved = shape(inner.shape, inner.dtype)
    exchange = (experts * capacity // SLOTS, 2, SLOTS, width)
    flat = shape(x.shape, jnp.bfloat16)
    anywhere = pl.BlockSpec(memory_space=pl.ANY)
    dma = pltpu.SemaphoreType.DMA
    results = pl.pallas_call(
        functools.partial(head_kernel, experts, capacity),
        out_shape=(
            *wholes,
            *([moved] * 8),
            shape((batch, *exchange), jnp.bfloat16),
            *([flat] * 5),
            shape(x.shape, jnp.float32),
            shape((batch, tokens, LANES), jnp.float32),
            shape((2, width), jnp.float32),
            shape(bias_shape, jnp.float32),
        ),
        in_specs=[SMEM, *([VMEM] * (6 + count))],
        out_specs=[*([VMEM] * count), *([anywhere] * 9), *([VMEM] * 9)],
        scratch_shapes=[
            pltpu.VMEM(exchange, jnp.bfloat16),
            pltpu.VMEM(exchange, jnp.bfloat16),
            pltpu.VMEM(inner.shape, jnp.bfloat16),
            pltpu.VMEM(outer.shape, jnp.bfloat16),
            pltpu.VMEM((2, blocks, LANES, LANES), jnp.float32),
            dma((count, 5)),
            dma((count, 5)),
            dma((2, CHUNKS, 4)),
            dma((2, CHUNKS, 4)),
            dma((batch, 7)),
            dma((batch, 7)),
            dma((4,)),
        ],
        compiler_params=pltpu.CompilerParams(
            collective_id=1, has_side_effects=True, vmem_limit_bytes=60 * 2**20
        ),
        name="layer_head",
    )(lengths, x, g, routes, routes_t, inner, outer, *parts)
    wholes, rest = results[:count], results[count:]
    return wholes, rest[:4], rest[4:8], rest[8], rest[9:16], rest[16], rest[17]


def middle_kernel(arrived_ref, *refs):
    inner_refs, outer_refs, refs = refs[:4], refs[4:8], refs[8:]
    returned_ref, outs, refs = refs[0], refs[1:5], refs[5:]
    taken, going, inner_sums, outer_sums, refs = refs[0], refs[1], refs[2:6], refs[6:10], refs[10:]
    stage, inbox, take_sem, send_sem, recv_sem, local_sem, core_send, core_recv = refs
    y, zl, x = (lax.axis_index(axis) for axis in PEER_AXES)
    mine = y * 4 + zl * 2 + x
    batch, sources, _, slots, width = arrived_ref.shape
    groups = sources // 2
    total = batch * groups

    meet([across("core"), *(peer_of(step)[0] for step in range(1, 8))])
    for ref in (*inner_sums, *outer_sums):
        ref[...] = jnp.zeros_like(ref)

    def partner(i, side):
        turn = lax.rem(i, groups)
        step = turn if side == 0 else 2 * groups - 1 - turn
        places = {}
        for axis, place, flipped in (
            ("y", y, step // 4),
            ("zl", zl, lax.rem(step // 2, 2)),
            ("x", x, lax.rem(step, 2)),
        ):
            places[axis] = place + flipped - 2 * place * flipped
        return lax.div(i, groups), places, (places["y"] * 2 + places["zl"]) * 2 + places["x"]

    def take(i, side):
        b, _, block = partner(i, side)
        slot = lax.rem(i, 2)
        return pltpu.make_async_copy(
            arrived_ref.at[b, block], taken.at[slot, side], take_sem.at[slot, side]
        )

    def back(i, side, action):
        b, target, block = partner(i, side)
        slot = lax.rem(i, 2)

        def far():
            action(
                pltpu.make_async_remote_copy(
                    src_ref=going.at[slot, side],
                    dst_ref=returned_ref.at[b, mine],
                    send_sem=send_sem.at[b, block],
                    recv_sem=recv_sem.at[b, mine],
                    device_id=target,
                    device_id_type=pl.DeviceIdType.MESH,
                ),
                True,
            )

        if side:
            far()
            return
        pl.when(block != mine)(far)

        @pl.when(block == mine)
        def _():
            action(
                pltpu.make_async_copy(
                    going.at[slot, side], returned_ref.at[b, mine], local_sem.at[b]
                ),
                False,
            )

    def begin(copy, remote):
        copy.start()

    def sent(copy, remote):
        if remote:
            copy.wait_send()
        else:
            copy.wait()

    for side in range(2):
        take(0, side).start()

    def work(i, carry):
        slot = lax.rem(i, 2)

        @pl.when(i + 1 < total)
        def _():
            for side in range(2):
                take(i + 1, side).start()

        for side in range(2):
            take(i, side).wait()
        rows = taken[slot, :, 0].reshape(2 * slots, width)
        grads = taken[slot, :, 1].reshape(2 * slots, width)
        out = jnp.zeros((2 * slots, width), jnp.float32)
        result = jnp.zeros((2 * slots, width), jnp.float32)
        for part in range(4):
            inner, outer = inner_refs[part][...], outer_refs[part][...]
            pre_act = jnp.dot(rows, inner, preferred_element_type=jnp.float32)
            activated, slope = gelu_parts(pre_act)
            hidden = activated.astype(jnp.bfloat16)
            grad_pre = (nt_dot(grads, outer) * slope).astype(jnp.bfloat16)
            out = out + jnp.dot(hidden, outer, preferred_element_type=jnp.float32)
            result = result + nt_dot(grad_pre, inner)
            inner_sums[part][...] += tn_dot(rows, grad_pre)
            outer_sums[part][...] += tn_dot(hidden, grads)

        @pl.when(i >= 2)
        def _():
            for side in range(2):
                back(i - 2, side, sent)

        going[slot, :, 0] = out.astype(jnp.bfloat16).reshape(2, slots, width)
        going[slot, :, 1] = result.astype(jnp.bfloat16).reshape(2, slots, width)
        for side in range(2):
            back(i, side, begin)
        return carry

    lax.fori_loop(0, total, work, 0)
    crossing = []
    for index in range(4):
        sums = (inner_sums, outer_sums)[index % 2]
        stage[index] = sums[3 - 2 * (index // 2)][...].astype(jnp.bfloat16)
        crossing.append(
            send(
                stage.at[index],
                inbox.at[index],
                core_send.at[index],
                core_recv.at[index],
                across("core"),
            )
        )
    for index in range(4):
        sums = (inner_sums, outer_sums)[index % 2]
        crossing[index].wait()
        met = sums[2 - 2 * (index // 2)][...] + inbox[index].astype(jnp.float32)
        outs[index][...] = met.astype(jnp.bfloat16)
    for i in (total - 2, total - 1):
        for side in range(2):
            back(i, side, sent)
    for b in range(batch):
        for step in range(1, 8):
            target, block = peer_of(step)
            pltpu.make_async_remote_copy(
                src_ref=going.at[0, 0],
                dst_ref=returned_ref.at[b, block],
                send_sem=send_sem.at[b, block],
                recv_sem=recv_sem.at[b, block],
                device_id=target,
                device_id_type=pl.DeviceIdType.MESH,
            ).wait_recv()


def layer_middle(arrived, inner, outer):
    batch, sources, _, slots, width = arrived.shape
    quarter = inner[0].shape
    anywhere = pl.BlockSpec(memory_space=pl.ANY)
    dma = pltpu.SemaphoreType.DMA
    results = pl.pallas_call(
        middle_kernel,
        out_shape=(
            jax.ShapeDtypeStruct(arrived.shape, jnp.bfloat16),
            *([jax.ShapeDtypeStruct(quarter, jnp.bfloat16)] * 4),
        ),
        in_specs=[anywhere, *([VMEM] * 8)],
        out_specs=[anywhere, *([VMEM] * 4)],
        scratch_shapes=[
            pltpu.VMEM((2, 2, 2, slots, width), jnp.bfloat16),
            pltpu.VMEM((2, 2, 2, slots, width), jnp.bfloat16),
            *([pltpu.VMEM(quarter, jnp.float32)] * 8),
            pltpu.VMEM((4, *quarter), jnp.bfloat16),
            pltpu.VMEM((4, *quarter), jnp.bfloat16),
            dma((2, 2)),
            dma((batch, sources)),
            dma((batch, sources)),
            dma((batch,)),
            dma((4,)),
            dma((4,)),
        ],
        compiler_params=pltpu.CompilerParams(
            collective_id=3, has_side_effects=True, vmem_limit_bytes=63 * 2**20
        ),
        name="layer_middle",
    )(arrived, *inner, *outer)
    return results[0], results[1:]


def bias_columns(diagonals, shards, bucket_count):
    lines = diagonals.shape[1]
    width = lines
    row = row_iota(lines, 1)
    distance = (row // (2 * LANES)) * LANES + LANES - 1 - row % (2 * LANES)
    table = bucket_table(lines // (2 * LANES) * LANES)
    bucket = jnp.minimum(distance, 16)
    for value in range(17, bucket_count):
        bucket = bucket + (distance >= int(np.argmax(table >= value))).astype(jnp.int32)
    lane = column_iota(1, width)
    place = lane % (width // shards)
    heads = 3
    hot = one_hot((bucket == place % bucket_count) & (place < heads * bucket_count))
    sums = sum(jnp.dot(part, hot, preferred_element_type=jnp.float32) for part in split(diagonals))
    head = lane // (width // shards) * heads + place // bucket_count
    return jnp.sum(jnp.where(row_iota(sums.shape[0], width) == head, sums, 0.0), 0, keepdims=True)


def tail_kernel(experts, capacity, bucket_count, lengths_ref, *refs):
    x_ref, g_ref, routes_ref, refs = refs[0], refs[1], refs[2], refs[3:]
    weights, gain_ref, bias_ref, refs = refs[:5], refs[5], refs[6], refs[7:]
    normed_ref, q_ref, k_ref, v_ref, mix_ref, residual_ref, gates_ref, returned_ref = refs[:8]
    partials, refs = refs[8:12], refs[12:]
    result_ref, input_grad_ref, home_refs, outs, refs = refs[0], refs[1], refs[2:4], refs[4:9], refs[9:]
    out_rows, back_rows, branch, dq, dk, dv, router_grad, gain_grad, diag, refs = *refs[:9], refs[9:]
    scratch, ready, grads, sums, refs = refs[:6], refs[6], refs[7:11], refs[11:16], refs[16:]
    inboxes, refs = [refs[5 * i : 5 * i + 5] for i in range(5)], refs[25:]
    fetched, landed, fold_send, fold_recv, move_send, move_recv, local_sem, own_sem = refs
    y, zh = lax.axis_index("y"), lax.axis_index("zh")
    at_home, away = zh == y, zh != y
    batch, tokens, width = x_ref.shape
    far, near = partials[:2], partials[2:]
    rows = far[0].shape[0] // CHUNKS

    greet(("core", "y", "x", "zl", "zh"))

    def load(b):
        return [
            pltpu.make_async_copy(returned_ref.at[b, :, which], target, local_sem.at[which])
            for which, target in enumerate((out_rows, back_rows))
        ]

    def piece(ref, chunk):
        return ref.at[pl.ds(chunk * rows, rows)]

    def own(which, chunk):
        return pltpu.make_async_copy(
            piece(near[which], chunk),
            (out_rows, back_rows)[which].at[chunk],
            own_sem.at[which, chunk],
        )

    def copy(which, chunk, kind, source, target, axis):
        return pltpu.make_async_remote_copy(
            src_ref=piece(source, chunk),
            dst_ref=piece(target, chunk),
            send_sem=move_send.at[which, chunk, kind],
            recv_sem=move_recv.at[which, chunk, kind],
            device_id=across(axis),
            device_id_type=pl.DeviceIdType.MESH,
        )

    order = [(which, chunk) for which in range(2) for chunk in range(CHUNKS)]
    for which, chunk in order:
        copy(which, chunk, 0, far[which], fetched.at[which], "y").start()

        @pl.when(away)
        def _():
            copy(which, chunk, 1, near[which], landed.at[which], "zh").start()

    waiting = list(order)

    def tick(amount=2):
        for which, chunk in waiting[:amount]:
            copy(which, chunk, 0, far[which], fetched.at[which], "y").wait_recv()

            @pl.when(at_home)
            def _():
                copy(which, chunk, 1, fetched.at[which], landed.at[which], "zh").start()

        del waiting[:amount]

    for part in load(0):
        part.start()
    for b in range(batch):
        for part in load(b):
            part.wait()

        def combined():
            if b + 1 < batch:
                for part in load(b + 1):
                    part.start()
            else:
                for which, chunk in order:
                    own(which, chunk).start()
            tick(1)

        backward_math(
            experts,
            capacity,
            Ticks([combined, tick, tick]),
            lengths_ref[b],
            x_ref.at[b],
            g_ref.at[b],
            routes_ref.at[b],
            *weights,
            gain_ref,
            bias_ref,
            q_ref.at[b],
            k_ref.at[b],
            v_ref.at[b],
            residual_ref.at[b],
            gates_ref.at[b],
            out_rows,
            back_rows,
            result_ref.at[b],
            input_grad_ref.at[b],
            branch.at[b],
            dq.at[b],
            dk.at[b],
            dv.at[b],
            router_grad.at[b],
            gain_grad.at[b],
            diag.at[b],
            *scratch,
        )
    tick(len(order))

    lines = [
        jnp.concatenate(
            [
                jnp.concatenate(
                    [
                        diag[0, head // 2, head % 2, offset : offset + 1, :]
                        + diag[1, head // 2, head % 2, offset : offset + 1, :]
                        for offset in range(diag.shape[3])
                    ],
                    1,
                )
                for head in range(2 * diag.shape[1])
            ],
            0,
        )
    ]
    lines.append(jnp.zeros((16 - lines[0].shape[0], lines[0].shape[1]), jnp.float32))
    bias_line = bias_columns(jnp.concatenate(lines, 0), 4, bucket_count)
    gain_lines = gain_grad[0] + gain_grad[1]
    row = row_iota(LANES, width)
    stacked = jnp.where(
        row == 0,
        gain_lines[0:1, :],
        jnp.where(row == 1, gain_lines[1:2, :], jnp.where(row == 2, bias_line, 0.0)),
    )
    packed = jnp.concatenate([router_grad[0] + router_grad[1], stacked.T], 1)
    ready[...] = packed.astype(jnp.bfloat16).reshape(ready.shape)
    fold_math(
        [
            (normed_ref.at[0], dq.at[0], normed_ref.at[1], dq.at[1]),
            (normed_ref.at[0], dk.at[0], normed_ref.at[1], dk.at[1]),
            (normed_ref.at[0], dv.at[0], normed_ref.at[1], dv.at[1]),
            (mix_ref.at[0], branch.at[0], mix_ref.at[1], branch.at[1]),
        ],
        ready,
        outs,
        grads,
        sums,
        inboxes,
        fold_send,
        fold_recv,
    )

    for which, chunk in order:
        own(which, chunk).wait()
        copy(which, chunk, 1, near[which], landed.at[which], "zh").wait()
        copy(which, chunk, 0, far[which], fetched.at[which], "y").wait_send()
        place = pl.ds(chunk * rows, rows)

        def settle(kept):
            total = kept.astype(jnp.float32) + landed[which, place].astype(jnp.float32)
            home_refs[which][place] = total.astype(jnp.bfloat16)

        pl.when(at_home)(lambda: settle((out_rows, back_rows)[which][chunk]))
        pl.when(away)(lambda: settle(fetched[which, place]))


class Ticks:
    def __init__(self, actions):
        self.actions = list(actions)

    def __call__(self):
        self.actions.pop(0)()


def layer_tail(experts, capacity, bucket_count, lengths, x, g, routes, weights, gains, bias, saved, returned, partials):
    batch, tokens, width = x.shape
    blocks = tokens // LANES
    shape, dma = jax.ShapeDtypeStruct, pltpu.SemaphoreType.DMA
    anywhere = pl.BlockSpec(memory_space=pl.ANY)
    flat = shape(x.shape, jnp.bfloat16)
    quarter = partials[0].shape
    sizes = [(width // 16, width)] * 4 + [(width // 16, 2 * LANES)]
    boxes = []
    for depth in range(5):
        for i, (part, columns) in enumerate(sizes):
            done = FOLD_ORDERS[i % len(FOLD_ORDERS)][:depth]
            lead = [2] * (3 - sum(axis != "zh" for axis in done))
            boxes.append(
                pltpu.VMEM(
                    (*lead, part, columns // 2 if "zh" in done else columns), jnp.bfloat16
                )
            )
    side = returned.shape[1:2] + returned.shape[3:]
    results = pl.pallas_call(
        functools.partial(tail_kernel, experts, capacity, bucket_count),
        out_shape=(
            flat,
            flat,
            *([shape(quarter, jnp.bfloat16)] * 2),
            *(shape((2, 2, *size), jnp.bfloat16) for size in sizes),
        ),
        in_specs=[SMEM, *([VMEM] * (3 + 5 + 2 + 7)), *([anywhere] * 5)],
        out_specs=[VMEM] * 9,
        scratch_shapes=[
            pltpu.VMEM(side, jnp.bfloat16),
            pltpu.VMEM(side, jnp.bfloat16),
            *([pltpu.VMEM(x.shape, jnp.bfloat16)] * 4),
            pltpu.VMEM((batch, width, LANES), jnp.float32),
            pltpu.VMEM((batch, 2, width), jnp.float32),
            pltpu.VMEM((batch, *bias.shape), jnp.float32),
            pltpu.VMEM((tokens, width), jnp.bfloat16),
            pltpu.VMEM((tokens, width), jnp.float32),
            pltpu.VMEM((2, blocks, LANES, LANES), jnp.float32),
            pltpu.VMEM((tokens, LANES), jnp.float32),
            pltpu.VMEM((tokens, LANES), jnp.float32),
            pltpu.VMEM((2, blocks, LANES, LANES), jnp.float32),
            pltpu.VMEM((2, 2, 2, 2, *sizes[-1]), jnp.bfloat16),
            *(pltpu.VMEM((2, 2, 2, 2, *size), jnp.bfloat16) for size in sizes[:-1]),
            *(pltpu.VMEM((2, 2, 2, *size), jnp.bfloat16) for size in sizes),
            *boxes,
            pltpu.VMEM((2, *quarter), jnp.bfloat16),
            pltpu.VMEM((2, *quarter), jnp.bfloat16),
            dma((5, 9)),
            dma((5, 9)),
            dma((2, CHUNKS, 2)),
            dma((2, CHUNKS, 2)),
            dma((2,)),
            dma((2, CHUNKS)),
        ],
        compiler_params=pltpu.CompilerParams(
            collective_id=2, has_side_effects=True, vmem_limit_bytes=63 * 2**20
        ),
        name="layer_tail",
    )(lengths, x, g, routes, *weights, gains, bias, *saved, returned, *partials)
    folded = [out.reshape(-1, out.shape[-1]).astype(jnp.float32) for out in results[4:]]
    homes = [home.astype(jnp.float32) for home in results[2:4]]
    return results[0], results[1], folded, homes


class Grouped:
    swap_axes = "expert"

    def begin(self, sizes, lengths, x, g, routes, routes_t, inner, outer, parts, bias_shape):
        wholes = [lax.all_gather(part, "shard", axis=0, tiled=True) for part in parts]
        misc = wholes[5].reshape(-1, *parts[5].shape).astype(jnp.float32)
        gains = jnp.sum(misc[:, -2:], 0)
        bias_rows = misc[:, :-2].reshape(bias_shape)
        inner, outer = (list(lax.all_gather(part, "shard", axis=0)) for part in (inner, outer))
        arrived, saved = [], []
        for index in range(x.shape[0]):
            sent, *kept = layer_forward(
                index,
                *sizes,
                lengths[index : index + 1],
                x,
                g,
                routes[index],
                routes_t[index],
                wholes[:4],
                wholes[4],
                gains,
                bias_rows,
            )
            saved.append(kept)
            arrived.append(self.swap(sent))
        saved = [jnp.stack(pair) for pair in zip(*saved)]
        return wholes, inner, outer, arrived, saved, gains, bias_rows

    def swap(self, blocks):
        experts = lax.axis_size("expert")
        count, _, slots, width = blocks.shape
        merged = blocks.swapaxes(0, 1).reshape(2, experts, -1, width).swapaxes(0, 1)
        merged = lax.all_to_all(merged, "expert", split_axis=0, concat_axis=0, tiled=True)
        return merged.swapaxes(0, 1).reshape(2, count, slots, width).swapaxes(0, 1)

    def finish(
        self,
        sizes,
        bucket_count,
        lengths,
        x,
        g,
        routes,
        wholes,
        gains,
        bias_rows,
        saved,
        arrived,
        inner,
        outer,
        likes,
    ):
        returned, units = [], []
        for rows in arrived:
            going, *unit_pair = expert_pass(rows, inner, outer)
            units.append(unit_pair)
            returned.append(self.swap(going))
        returned = jnp.stack(returned)
        hiddens, pres = zip(*units)
        chunks = len(inner)
        passes = weight_pass(0, chunks, chunks, arrived, pres, hiddens)
        homes = [
            lax.psum_scatter(jnp.stack(grads), "shard", scatter_dimension=0).astype(jnp.float32)
            for grads in passes
        ]
        normed, queries, key_rows, value_rows, mixture, residual, gates = saved
        results, input_grads, grads, small = [], [], [], []
        for index in range(x.shape[0]):
            result, input_grad, branch, dq, dk, dv, *rest = layer_backward(
                index,
                *sizes,
                lengths[index : index + 1],
                x,
                g,
                routes,
                wholes[:4],
                wholes[4],
                gains,
                bias_rows,
                (queries, key_rows, value_rows, residual, gates),
                returned,
            )
            results.append(result)
            input_grads.append(input_grad)
            lefts = (normed[index],) * 3 + (mixture[index],)
            grads.append([tn_dot(*pair) for pair in zip(lefts, (dq, dk, dv, branch))])
            small.append(rest)
        router_grad, gain_grad, diagonals = (sum(parts) for parts in zip(*small))
        bias_grad = jnp.dot(
            diagonals.reshape(bias_rows.shape[0] * 2, -1),
            jnp.asarray(collect_hot(x.shape[1], bucket_count)),
            precision=HIGH,
        )
        small = (router_grad[:, : sizes[0]], gain_grad[0], gain_grad[1], bias_grad)
        shares = [
            lax.psum_scatter(
                sum(pair).astype(jnp.bfloat16), "shard", scatter_dimension=0, tiled=True
            ).astype(jnp.float32)
            for pair in (*zip(*grads), *((part,) for part in small))
        ]
        return jnp.stack(results), jnp.stack(input_grads), lax.psum(shares, "expert"), homes

    def shard_index(self):
        return lax.axis_index("shard")


class Halved:
    swap_axes = ("y", "zl", "x")

    def begin(self, sizes, lengths, x, g, routes, routes_t, inner, outer, parts, bias_shape):
        misc = jnp.pad(parts[5], ((0, 32 - parts[5].shape[0]), (0, 0)))
        return layer_head(
            *sizes, lengths, x, g, routes, routes_t, inner, outer, [*parts[:5], misc], bias_shape
        )

    def shard_index(self):
        return lax.axis_index("y") * 2 + lax.axis_index("core")

    def finish(
        self,
        sizes,
        bucket_count,
        lengths,
        x,
        g,
        routes,
        wholes,
        gains,
        bias_rows,
        saved,
        arrived,
        inner,
        outer,
        likes,
    ):
        returned, partials = layer_middle(arrived, inner, outer)
        result, input_grad, folded, homes = layer_tail(
            *sizes,
            bucket_count,
            lengths,
            x,
            g,
            routes,
            wholes[:5],
            gains,
            bias_rows,
            saved,
            returned,
            partials,
        )
        *large, packed = folded
        router, gain_one, gain_two, bias = likes
        small = [
            packed[:, : router.shape[1]],
            packed[:, LANES],
            packed[:, LANES + 1],
            packed[: bias.size, LANES + 2].reshape(bias.shape),
        ]
        return result, input_grad, [*large, *small], homes


def body(
    plan,
    tokens,
    cotangent,
    lengths,
    dealing,
    routes,
    query_weight,
    key_weight,
    value_weight,
    output_weight,
    router_weight,
    first_gain,
    second_gain,
    position_bias,
    inner_weight,
    outer_weight,
):
    batch, seq_len, model_width = tokens.shape
    experts = lax.axis_size(plan.swap_axes)
    capacity = 4 * seq_len // experts
    bucket_count = position_bias.shape[1]
    shard_rows = query_weight.shape[0]
    shards = model_width // shard_rows
    small_shard = (router_weight, first_gain, second_gain, position_bias)
    lane_shard = jnp.arange(model_width) // shard_rows
    bias_shard = jnp.dot(
        position_bias.astype(jnp.float32),
        jnp.asarray(spread_hot(seq_len, bucket_count)),
        precision=HIGH,
    ).astype(jnp.bfloat16)
    gain_shard = jnp.where(
        lane_shard == plan.shard_index(),
        jnp.tile(jnp.stack([first_gain, second_gain]), (1, shards)),
        0,
    )
    parts = [
        query_weight,
        key_weight,
        value_weight,
        output_weight,
        jnp.pad(router_weight, ((0, 0), (0, LANES - experts))),
        jnp.concatenate([bias_shard, gain_shard], 0),
    ]
    heads = shards * position_bias.shape[0]
    bias_shape = (heads // 2, 2, seq_len // LANES, 2 * LANES)
    seq_numbers = jnp.arange(lengths.shape[0], dtype=jnp.int32)
    seq_lengths = jnp.sum(jnp.where(seq_numbers == dealing[:, None], lengths, 0), 1)
    sizes = (experts, capacity)
    wholes, inner_parts, outer_parts, arrived, saved, gains, bias_rows = plan.begin(
        sizes,
        seq_lengths,
        tokens,
        cotangent,
        routes,
        routes.swapaxes(1, 2),
        inner_weight[0],
        outer_weight[0],
        parts,
        bias_shape,
    )
    results, input_grads, large_and_small, homes = plan.finish(
        sizes,
        bucket_count,
        seq_lengths,
        tokens,
        cotangent,
        routes,
        wholes,
        gains,
        bias_rows,
        saved,
        arrived,
        inner_parts,
        outer_parts,
        small_shard,
    )
    return (results, input_grads, *large_and_small, homes[0][None], homes[1][None])


def solution(mesh):
    experts, shards = mesh.shape["expert"], mesh.shape["shard"]
    if (experts, shards) == (8, 4):
        plan = Halved()
        mesh = jax.sharding.Mesh(
            mesh.devices.reshape(2, 2, 2, 2, 2), ("zh", "zl", "x", "y", "core")
        )
        expert_axes, shard_axes = ("zh", "zl", "x"), ("y", "core")
    else:
        plan = Grouped()
        expert_axes, shard_axes = ("expert",), ("shard",)
    both = (*expert_axes, *shard_axes)
    rows = P(both, None, None)
    weight = P(shard_axes, None)
    in_specs = (rows, rows, P(), P(both), rows, *([weight] * 5))
    in_specs += (P(shard_axes), P(shard_axes), weight)
    in_specs += (P(expert_axes, None, shard_axes), P(expert_axes, shard_axes, None))
    out_specs = (rows, rows, *([weight] * 5), P(shard_axes), P(shard_axes), weight)
    out_specs += (P(expert_axes, None, shard_axes), P(expert_axes, shard_axes, None))
    return jax.shard_map(
        functools.partial(body, plan),
        mesh=mesh,
        in_specs=in_specs,
        out_specs=out_specs,
        check_vma=False,
    )
```

```python
import functools
import math

import jax
import jax.numpy as jnp
import numpy as np
from jax import lax
from jax.experimental import pallas as pl
from jax.experimental.pallas import tpu as pltpu
from jax.sharding import PartitionSpec as P

EPSILON = 1e-06
HIGH = lax.Precision.HIGHEST
NEGATIVE = -1000000000.0
INV_ROOT_TWO = 1.0 / math.sqrt(2.0)
INV_ROOT_TAU = 1.0 / math.sqrt(2.0 * math.pi)
LANES = 128


def bucket_table(length):
    distance = np.arange(length)
    scaled = 16 + np.floor(np.log(np.maximum(distance, 1) / 16.0) / np.log(8.0) * 16.0)
    return np.where(distance < 16, distance, np.minimum(scaled, 31)).astype(np.int32)


def gelu_parts(pre_act):
    normal_cdf = 0.5 * (1.0 + lax.erf(pre_act * INV_ROOT_TWO))
    return (
        pre_act * normal_cdf,
        normal_cdf + pre_act * jnp.exp(-0.5 * pre_act * pre_act) * INV_ROOT_TAU,
    )


def distance_table(length):
    offsets = np.arange(length // LANES)[:, None] * LANES
    return offsets, np.arange(2 * LANES)[None, :]


def spread_hot(length, bucket_count):
    offsets, lanes = distance_table(length)
    signed = np.where(lanes < LANES, lanes, lanes - 2 * LANES)
    distance = np.clip(offsets - signed, 0, length - 1).reshape(-1)
    return (bucket_table(length)[distance][None, :] == np.arange(bucket_count)[:, None]).astype(
        np.float32
    )


def collect_hot(length, bucket_count):
    offsets, lanes = distance_table(length)
    distance = (offsets + LANES - 1 - lanes).reshape(-1)
    inside = (distance >= 0) & (distance < length)
    table = bucket_table(length)[np.clip(distance, 0, length - 1)]
    return ((table[:, None] == np.arange(bucket_count)[None, :]) & inside[:, None]).astype(
        np.float32
    )


def half_mask(head):
    lane = lax.broadcasted_iota(jnp.int32, (1, LANES), 1)
    return (lane < LANES // 2) if head == 0 else (lane >= LANES // 2)


def only(value, head):
    return jnp.where(half_mask(head), value, jnp.zeros_like(value))


def nt_dot(left, right):
    return lax.dot_general(
        left, right, (((1,), (1,)), ((), ())), preferred_element_type=jnp.float32
    )


def tn_dot(left, right):
    return lax.dot_general(
        left, right, (((0,), (0,)), ((), ())), preferred_element_type=jnp.float32
    )


def toeplitz_block(row):
    spread = pltpu.roll(
        jnp.broadcast_to(row, (LANES, 2 * LANES)), 0, 1, stride=1, stride_axis=0
    )
    return spread[:, :LANES]


def fill_bias(bias_ref, table_ref, blocks):
    for head in range(2):
        for offset in range(blocks):
            table_ref[head, offset] = toeplitz_block(bias_ref[0, head, offset, :][None, :])


def masked_logits(query, keys, table_ref, head, block, length):
    width = (block + 1) * LANES
    bias = jnp.concatenate([table_ref[head, block - j] for j in range(block + 1)], 1)
    logits = nt_dot(query, keys) * ((LANES // 2) ** (-0.5)) + bias
    row = lax.broadcasted_iota(jnp.int32, (LANES, width), 0) + block * LANES
    column = lax.broadcasted_iota(jnp.int32, (LANES, width), 1)
    return jnp.where((column <= row) & (column < length), logits, NEGATIVE)


SLOTS = 192


def unit(value):
    return lax.rsqrt(jnp.mean(value * value, -1, keepdims=True) + EPSILON)


def column_iota(rows, columns):
    return lax.broadcasted_iota(jnp.int32, (rows, columns), 1)


def row_iota(rows, columns):
    return lax.broadcasted_iota(jnp.int32, (rows, columns), 0)


def row_places(routes_t_ref, experts, capacity):
    tokens = routes_t_ref.shape[1]
    padded = -(-experts // 16) * 16
    expert = row_iota(padded, tokens)
    hot = [expert == routes_t_ref[pick : pick + 1, :] for pick in range(2)]
    both = jnp.where(hot[0] | hot[1], 1.0, 0.0).astype(jnp.bfloat16)
    before = (row_iota(tokens, tokens) < column_iota(tokens, tokens)).astype(jnp.float32)
    rank = jnp.dot(both, before.astype(jnp.bfloat16), preferred_element_type=jnp.float32)
    slot = rank + (expert * capacity).astype(jnp.float32)
    return [jnp.sum(jnp.where(chosen, slot, 0.0), 0, keepdims=True) for chosen in hot]


def column_places(routes_ref, experts, capacity):
    tokens = routes_ref.shape[0]
    expert = column_iota(tokens, LANES)
    hot = [expert == routes_ref[:, pick : pick + 1] for pick in range(2)]
    both = jnp.where(hot[0] | hot[1], 1.0, 0.0).astype(jnp.bfloat16)
    before = (column_iota(tokens, tokens) < row_iota(tokens, tokens)).astype(jnp.float32)
    rank = jnp.dot(before.astype(jnp.bfloat16), both, preferred_element_type=jnp.float32)
    slot = rank + (expert * capacity).astype(jnp.float32)
    return [jnp.sum(jnp.where(chosen, slot, 0.0), 1, keepdims=True) for chosen in hot], hot


def one_hot(condition):
    return jnp.where(condition, 1.0, 0.0).astype(jnp.bfloat16)


def forward_math(
    length,
    x_ref,
    routes_ref,
    query_ref,
    key_ref,
    value_ref,
    output_ref,
    router_ref,
    gain_ref,
    bias_ref,
    tokens_ref,
    normed_ref,
    q_ref,
    k_ref,
    v_ref,
    mix_ref,
    residual_ref,
    gates_ref,
    table_ref,
):
    tokens, width = x_ref.shape
    blocks = tokens // LANES
    inputs = x_ref[...].astype(jnp.float32)
    normed = (inputs * unit(inputs) * gain_ref[0:1, :]).astype(jnp.bfloat16)
    normed_ref[...] = normed
    for weight, out in ((query_ref, q_ref), (key_ref, k_ref), (value_ref, v_ref)):
        out[...] = jnp.dot(normed, weight[...], preferred_element_type=jnp.float32).astype(
            jnp.bfloat16
        )

    def attend(pair, carry):
        lanes = pl.ds(pl.multiple_of(pair * LANES, LANES), LANES)
        fill_bias(bias_ref.at[pl.ds(pair, 1)], table_ref, blocks)
        for block in range(blocks):
            rows = pl.ds(block * LANES, LANES)
            reach = (block + 1) * LANES
            mixed = jnp.zeros((LANES, LANES), jnp.float32)
            for head in range(2):
                logits = masked_logits(
                    only(q_ref[rows, lanes], head),
                    k_ref[:reach, lanes],
                    table_ref,
                    head,
                    block,
                    length,
                )
                exponent = jnp.exp(logits - jnp.max(logits, 1, keepdims=True))
                soft = exponent / jnp.sum(exponent, 1, keepdims=True)
                mixed = mixed + jnp.dot(
                    soft.astype(jnp.bfloat16),
                    only(v_ref[:reach, lanes], head),
                    preferred_element_type=jnp.float32,
                )
            mix_ref[rows, lanes] = mixed.astype(jnp.bfloat16)
        return carry

    lax.fori_loop(0, width // LANES, attend, 0)
    residual = inputs + jnp.dot(
        mix_ref[...], output_ref[...], preferred_element_type=jnp.float32
    )
    residual_ref[...] = residual
    normed = (residual * unit(residual) * gain_ref[1:2, :]).astype(jnp.bfloat16)
    tokens_ref[...] = normed
    router = jnp.dot(normed, router_ref[...], preferred_element_type=jnp.float32)
    lane = column_iota(tokens, LANES)
    chosen = [
        jnp.sum(jnp.where(lane == routes_ref[:, pick : pick + 1], router, 0.0), 1, keepdims=True)
        for pick in range(2)
    ]
    top = jnp.maximum(chosen[0], chosen[1])
    gates = [jnp.exp(value - top) for value in chosen]
    total = gates[0] + gates[1]
    gates = [value / total for value in gates]
    gates_ref[...] = jnp.where(lane == 0, gates[0], jnp.where(lane == 1, gates[1], 0.0))


def dispatcher(experts, capacity, tokens_ref, g_ref, gates_ref, routes_t_ref):
    tokens = tokens_ref.shape[0]
    places = row_places(routes_t_ref, experts, capacity)
    grads = [
        (g_ref[...].astype(jnp.float32) * gates_ref[:, pick : pick + 1]).astype(jnp.bfloat16)
        for pick in range(2)
    ]

    def fill(index, block_ref):
        slots = block_ref.shape[1]
        slot = (row_iota(slots, tokens) + index * slots).astype(jnp.float32)
        hot = [jnp.where(slot == place, 1.0, 0.0) for place in places]
        block_ref[0] = jnp.dot(
            (hot[0] + hot[1]).astype(jnp.bfloat16),
            tokens_ref[...],
            preferred_element_type=jnp.float32,
        ).astype(jnp.bfloat16)
        block_ref[1] = (
            jnp.dot(hot[0].astype(jnp.bfloat16), grads[0], preferred_element_type=jnp.float32)
            + jnp.dot(hot[1].astype(jnp.bfloat16), grads[1], preferred_element_type=jnp.float32)
        ).astype(jnp.bfloat16)

    return fill


def forward_kernel(experts, capacity, length_ref, x_ref, g_ref, routes_ref, routes_t_ref, *refs):
    refs, (sent_ref, *outs, gates_ref, tokens_ref, table_ref) = refs[:7], refs[7:]
    forward_math(
        length_ref[0], x_ref, routes_ref, *refs, tokens_ref, *outs, gates_ref, table_ref
    )
    fill = dispatcher(experts, capacity, tokens_ref, g_ref, gates_ref, routes_t_ref)
    for index in range(sent_ref.shape[0]):
        fill(index, sent_ref.at[index])


def split(value):
    high = value.astype(jnp.bfloat16)
    return high, (value - high.astype(jnp.float32)).astype(jnp.bfloat16)


def norm_back(value, gain, grad):
    scale = unit(value)
    rows = value * scale
    grad_unit = grad * gain
    grad_gain = jnp.sum(grad * rows, 0, keepdims=True)
    mean = jnp.mean(grad_unit * rows, -1, keepdims=True)
    return scale * (grad_unit - rows * mean), grad_gain


def combine_math(
    experts,
    capacity,
    g_ref,
    routes_ref,
    output_ref,
    router_ref,
    gain_ref,
    residual_ref,
    gates_ref,
    out_rows_ref,
    back_rows_ref,
    result_ref,
    branch_ref,
    router_grad_ref,
    gain_grad_ref,
    grad_mix_ref,
    grad_residual_ref,
):
    tokens, width = g_ref.shape
    grad_result = g_ref[...].astype(jnp.float32)
    residual = residual_ref[...]
    places, picks = column_places(routes_ref, experts, capacity)
    gates = [gates_ref[:, pick : pick + 1] for pick in range(2)]
    slots = out_rows_ref.shape[1]
    picked = [jnp.zeros((tokens, width), jnp.float32) for _ in range(2)]
    grad_normed = jnp.zeros((tokens, width), jnp.float32)
    for index in range(0, out_rows_ref.shape[0], 2):
        slot = (column_iota(tokens, 2 * slots) + index * slots).astype(jnp.float32)
        hot = [jnp.where(slot == place, 1.0, 0.0) for place in places]
        out_rows = out_rows_ref[index : index + 2].reshape(2 * slots, width)
        back_rows = back_rows_ref[index : index + 2].reshape(2 * slots, width)
        for pick in range(2):
            picked[pick] = picked[pick] + jnp.dot(
                hot[pick].astype(jnp.bfloat16), out_rows, preferred_element_type=jnp.float32
            )
        grad_normed = grad_normed + jnp.dot(
            (hot[0] + hot[1]).astype(jnp.bfloat16), back_rows, preferred_element_type=jnp.float32
        )
    result_ref[...] = (residual + (gates[0] * picked[0] + gates[1] * picked[1])).astype(
        jnp.bfloat16
    )
    grad_gates = [jnp.sum(grad_result * rows, 1, keepdims=True) for rows in picked]
    common = gates[0] * grad_gates[0] + gates[1] * grad_gates[1]
    grad_router = jnp.zeros((tokens, LANES), jnp.float32)
    for pick in range(2):
        grad_router = grad_router + jnp.where(
            picks[pick], gates[pick] * (grad_gates[pick] - common), 0.0
        )
    normed = (residual * unit(residual) * gain_ref[1:2, :]).astype(jnp.bfloat16)
    router_grad = jnp.zeros((width, LANES), jnp.float32)
    for part in split(grad_router):
        grad_normed = grad_normed + nt_dot(part, router_ref[...])
        router_grad = router_grad + tn_dot(normed, part)
    router_grad_ref[...] = router_grad
    from_norm, grad_gain = norm_back(residual, gain_ref[1:2, :], grad_normed)
    gain_grad_ref[1:2, :] = grad_gain
    grad_residual = grad_result + from_norm
    grad_residual_ref[...] = grad_residual
    branch = grad_residual.astype(jnp.bfloat16)
    branch_ref[...] = branch
    grad_mix_ref[...] = nt_dot(branch, output_ref[...]).astype(jnp.bfloat16)


def attend_back_math(
    pair,
    length,
    q_ref,
    k_ref,
    v_ref,
    grad_mix_ref,
    bias_ref,
    dq_ref,
    dk_ref,
    dv_ref,
    diag_ref,
    table_ref,
    dk_sum,
    dv_sum,
    skew_ref,
):
    blocks = q_ref.shape[0] // LANES
    scale = (LANES // 2) ** (-0.5)
    upside = (row_iota(LANES, LANES) + column_iota(LANES, LANES) == LANES - 1).astype(jnp.float32)
    lanes = pl.ds(pl.multiple_of(pair * LANES, LANES), LANES)
    fill_bias(bias_ref.at[pl.ds(pair, 1)], table_ref, blocks)
    dk_sum[...] = jnp.zeros_like(dk_sum)
    dv_sum[...] = jnp.zeros_like(dv_sum)
    skew_ref[...] = jnp.zeros_like(skew_ref)
    for block in range(blocks):
        rows = pl.ds(block * LANES, LANES)
        reach = (block + 1) * LANES
        dq = jnp.zeros((LANES, LANES), jnp.float32)
        for head in range(2):
            query = only(q_ref[rows, lanes], head)
            grad = only(grad_mix_ref[rows, lanes], head)
            keys = k_ref[:reach, lanes]
            logits = masked_logits(query, keys, table_ref, head, block, length)
            exponent = jnp.exp(logits - jnp.max(logits, 1, keepdims=True))
            soft = exponent / jnp.sum(exponent, 1, keepdims=True)
            grad_soft = nt_dot(grad, v_ref[:reach, lanes])
            inner = jnp.sum(soft * grad_soft, 1, keepdims=True)
            grad_logits = (soft * (grad_soft - inner)).astype(jnp.bfloat16)
            dv_sum[:reach, :] += tn_dot(soft.astype(jnp.bfloat16), grad)
            dk_sum[:reach, :] += tn_dot(grad_logits, query)
            dq = dq + jnp.dot(
                grad_logits, only(keys, head), preferred_element_type=jnp.float32
            )
            wide = grad_logits.astype(jnp.float32)
            for j in range(block + 1):
                skew_ref[head, block - j] += wide[:, j * LANES : (j + 1) * LANES]
        dq_ref[rows, lanes] = (dq * scale).astype(jnp.bfloat16)
    dk_ref[:, lanes] = (dk_sum[...] * scale).astype(jnp.bfloat16)
    dv_ref[:, lanes] = dv_sum[...].astype(jnp.bfloat16)
    for head in range(2):
        for offset in range(blocks):
            flipped = jnp.dot(
                upside,
                skew_ref[head, offset],
                precision=HIGH,
                preferred_element_type=jnp.float32,
            )
            padded = jnp.concatenate([flipped, jnp.zeros_like(flipped)], 1)
            lined = pltpu.roll(padded, 0, 1, stride=1, stride_axis=0)
            diag_ref[pair, head, offset, :] = jnp.sum(lined, 0)


def finish_math(
    x_ref,
    query_ref,
    key_ref,
    value_ref,
    gain_ref,
    dq_ref,
    dk_ref,
    dv_ref,
    grad_residual_ref,
    gain_grad_ref,
    input_grad_ref,
):
    grad_normed = nt_dot(dq_ref[...], query_ref[...])
    grad_normed = grad_normed + nt_dot(dk_ref[...], key_ref[...])
    grad_normed = grad_normed + nt_dot(dv_ref[...], value_ref[...])
    inputs = x_ref[...].astype(jnp.float32)
    from_norm, grad_gain = norm_back(inputs, gain_ref[0:1, :], grad_normed)
    gain_grad_ref[0:1, :] = grad_gain
    input_grad_ref[...] = (grad_residual_ref[...] + from_norm).astype(jnp.bfloat16)


def backward_kernel(
    experts,
    capacity,
    length_ref,
    x_ref,
    g_ref,
    routes_ref,
    query_ref,
    key_ref,
    value_ref,
    output_ref,
    router_ref,
    gain_ref,
    bias_ref,
    q_ref,
    k_ref,
    v_ref,
    residual_ref,
    gates_ref,
    out_rows_ref,
    back_rows_ref,
    result_ref,
    input_grad_ref,
    branch_ref,
    dq_ref,
    dk_ref,
    dv_ref,
    router_grad_ref,
    gain_grad_ref,
    diag_ref,
    grad_mix_ref,
    grad_residual_ref,
    *scratch,
):
    combine_math(
        experts,
        capacity,
        g_ref,
        routes_ref,
        output_ref,
        router_ref,
        gain_ref,
        residual_ref,
        gates_ref,
        out_rows_ref,
        back_rows_ref,
        result_ref,
        branch_ref,
        router_grad_ref,
        gain_grad_ref,
        grad_mix_ref,
        grad_residual_ref,
    )

    def attend_back(pair, carry):
        attend_back_math(
            pair,
            length_ref[0],
            q_ref,
            k_ref,
            v_ref,
            grad_mix_ref,
            bias_ref,
            dq_ref,
            dk_ref,
            dv_ref,
            diag_ref,
            *scratch,
        )
        return carry

    lax.fori_loop(0, x_ref.shape[1] // LANES, attend_back, 0)
    finish_math(
        x_ref,
        query_ref,
        key_ref,
        value_ref,
        gain_ref,
        dq_ref,
        dk_ref,
        dv_ref,
        grad_residual_ref,
        gain_grad_ref,
        input_grad_ref,
    )


VMEM = pl.BlockSpec(memory_space=pltpu.VMEM)
SMEM = pl.BlockSpec(memory_space=pltpu.SMEM)


def layer_forward(index, experts, capacity, length, x, g, routes, routes_t, weights, router, gains, bias):
    _, tokens, width = x.shape
    blocks = tokens // LANES
    flat = jax.ShapeDtypeStruct((tokens, width), jnp.bfloat16)
    rows = pl.BlockSpec((None, tokens, width), lambda i: (index, 0, 0))
    return pl.pallas_call(
        functools.partial(forward_kernel, experts, capacity),
        grid=(1,),
        out_shape=(
            jax.ShapeDtypeStruct((experts * capacity // SLOTS, 2, SLOTS, width), jnp.bfloat16),
            flat,
            flat,
            flat,
            flat,
            flat,
            jax.ShapeDtypeStruct((tokens, width), jnp.float32),
            jax.ShapeDtypeStruct((tokens, LANES), jnp.float32),
        ),
        in_specs=[SMEM, rows, rows, *([VMEM] * 9)],
        out_specs=[VMEM] * 8,
        scratch_shapes=[
            pltpu.VMEM((tokens, width), jnp.bfloat16),
            pltpu.VMEM((2, blocks, LANES, LANES), jnp.float32),
        ],
        compiler_params=pltpu.CompilerParams(vmem_limit_bytes=56 * 2**20),
        cost_estimate=pl.CostEstimate(
            flops=2 * tokens * width * (4 * width + 4 * tokens + 6 * tokens),
            bytes_accessed=40 * tokens * width,
            transcendentals=tokens * tokens * 12,
        ),
        name="layer_forward",
    )(length, x, g, routes, routes_t, *weights, router, gains, bias)


def layer_backward(
    index, experts, capacity, length, x, g, routes, weights, router, gains, bias, saved, returned
):
    _, tokens, width = x.shape
    blocks = tokens // LANES
    flat = jax.ShapeDtypeStruct((tokens, width), jnp.bfloat16)
    _, count, _, slots, _ = returned.shape

    def one(array):
        return pl.BlockSpec((None, *array.shape[1:]), lambda i: (index, 0, 0))

    rows = one(x)

    def side(which):
        return pl.BlockSpec(
            (None, count, None, slots, width), lambda i: (index, 0, which, 0, 0)
        )

    return pl.pallas_call(
        functools.partial(backward_kernel, experts, capacity),
        grid=(1,),
        out_shape=(
            *([flat] * 6),
            jax.ShapeDtypeStruct((width, LANES), jnp.float32),
            jax.ShapeDtypeStruct((2, width), jnp.float32),
            jax.ShapeDtypeStruct(bias.shape, jnp.float32),
        ),
        in_specs=[
            SMEM,
            rows,
            rows,
            one(routes),
            *([VMEM] * 7),
            *map(one, saved),
            side(0),
            side(1),
        ],
        out_specs=[VMEM] * 9,
        scratch_shapes=[
            pltpu.VMEM((tokens, width), jnp.bfloat16),
            pltpu.VMEM((tokens, width), jnp.float32),
            pltpu.VMEM((2, blocks, LANES, LANES), jnp.float32),
            pltpu.VMEM((tokens, LANES), jnp.float32),
            pltpu.VMEM((tokens, LANES), jnp.float32),
            pltpu.VMEM((2, blocks, LANES, LANES), jnp.float32),
        ],
        compiler_params=pltpu.CompilerParams(vmem_limit_bytes=56 * 2**20),
        cost_estimate=pl.CostEstimate(
            flops=2 * tokens * width * (4 * width + 12 * tokens + 10 * tokens),
            bytes_accessed=40 * tokens * width,
            transcendentals=tokens * tokens * 12,
        ),
        name="layer_backward",
    )(length, x, g, routes, *weights, router, gains, bias, *saved, returned, returned)


def expert_kernel(count, x_ref, g_ref, *refs):
    inner_refs, outer_refs = refs[:count], refs[count : 2 * count]
    back_ref, hidden_ref, grad_ref = refs[2 * count :]
    shape = x_ref.shape
    inputs = x_ref[...].reshape(-1, shape[-1])
    grads = g_ref[...].reshape(-1, shape[-1])
    out = jnp.zeros(inputs.shape, jnp.float32)
    back = jnp.zeros(inputs.shape, jnp.float32)
    start = 0
    for inner_ref, outer_ref in zip(inner_refs, outer_refs):
        part = pl.ds(start, inner_ref.shape[1])
        start += inner_ref.shape[1]
        pre_act = jnp.dot(inputs, inner_ref[...], preferred_element_type=jnp.float32)
        activated, slope = gelu_parts(pre_act)
        hidden = activated.astype(jnp.bfloat16)
        grad_pre = (nt_dot(grads, outer_ref[...]) * slope).astype(jnp.bfloat16)
        hidden_ref[:, part] = hidden
        grad_ref[:, part] = grad_pre
        out = out + jnp.dot(hidden, outer_ref[...], preferred_element_type=jnp.float32)
        back = back + nt_dot(grad_pre, inner_ref[...])
    back_ref[:, 0] = out.astype(jnp.bfloat16).reshape(shape)
    back_ref[:, 1] = back.astype(jnp.bfloat16).reshape(shape)


def expert_pass(arrived, inner, outer):
    sources, _, capacity, width = arrived.shape
    total = sources * capacity
    units = sum(part.shape[1] for part in inner)
    group = sources // 4

    def side(which):
        return pl.BlockSpec((group, None, capacity, width), lambda i: (i, which, 0, 0))

    def whole(shape):
        return pl.BlockSpec(shape, lambda i: (0, 0), pipeline_mode=pl.Buffered(1))

    unit_spec = pl.BlockSpec((group * capacity, units), lambda i: (i, 0))
    deep = jax.ShapeDtypeStruct((total, units), jnp.bfloat16)
    return pl.pallas_call(
        functools.partial(expert_kernel, len(inner)),
        grid=(sources // group,),
        out_shape=(jax.ShapeDtypeStruct(arrived.shape, jnp.bfloat16), deep, deep),
        in_specs=[side(0), side(1), *(whole(part.shape) for part in (*inner, *outer))],
        out_specs=(
            pl.BlockSpec((group, 2, capacity, width), lambda i: (i, 0, 0, 0)),
            unit_spec,
            unit_spec,
        ),
        compiler_params=pltpu.CompilerParams(vmem_limit_bytes=60 * 2**20),
        cost_estimate=pl.CostEstimate(
            flops=8 * total * width * units,
            bytes_accessed=4 * (2 * width + units) * total + 4 * width * units,
            transcendentals=2 * total * units,
        ),
        name="expert_pass",
    )(arrived, arrived, *inner, *outer)


def weight_kernel(x0_ref, x1_ref, g0_ref, g1_ref, p0_ref, p1_ref, h0_ref, h1_ref, *out_refs):
    inner_ref, outer_ref = out_refs

    def flat(ref):
        return ref[...].reshape(-1, ref.shape[-1])

    inner = tn_dot(flat(x0_ref), p0_ref[...]) + tn_dot(flat(x1_ref), p1_ref[...])
    inner_ref[...] = inner.astype(jnp.bfloat16)
    outer = tn_dot(h0_ref[...], flat(g0_ref)) + tn_dot(h1_ref[...], flat(g1_ref))
    outer_ref[...] = outer.astype(jnp.bfloat16)


def weight_pass(first, count, chunks, arrived, pres, hiddens):
    sources, _, capacity, width = arrived[0].shape
    total = sources * capacity
    size = hiddens[0].shape[1] // chunks
    step = math.gcd(size, 256)
    steps = size // step

    def side(which):
        return pl.BlockSpec(
            (sources, None, capacity, width),
            lambda i: (0, which, 0, 0),
            pipeline_mode=pl.Buffered(1),
        )

    units = pl.BlockSpec((total, step), lambda i: (0, first * steps + i))
    inner, outer = pl.pallas_call(
        weight_kernel,
        grid=(count * steps,),
        out_shape=(
            jax.ShapeDtypeStruct((count, width, size), jnp.bfloat16),
            jax.ShapeDtypeStruct((count * size, width), jnp.bfloat16),
        ),
        in_specs=[side(0)] * 2 + [side(1)] * 2 + [units] * 4,
        out_specs=(
            pl.BlockSpec((None, width, step), lambda i: (i // steps, 0, i % steps)),
            pl.BlockSpec((step, width), lambda i: (i, 0)),
        ),
        compiler_params=pltpu.CompilerParams(vmem_limit_bytes=60 * 2**20),
        cost_estimate=pl.CostEstimate(
            flops=8 * total * width * count * size,
            bytes_accessed=8 * total * (width + count * size) + 4 * width * count * size,
            transcendentals=0,
        ),
        name="weight_pass",
    )(*arrived, *arrived, *pres, *hiddens)
    return list(inner), list(outer.reshape(count, size, width))


FOLD_ORDERS = (("x", "y", "zl", "zh"), ("y", "x", "zl", "zh"))
FOLD_STEPS = 9


def greet(axes):
    barrier = pltpu.get_barrier_semaphore()
    for axis in axes:
        pl.semaphore_signal(
            barrier,
            inc=1,
            device_id={axis: 1 - lax.axis_index(axis)},
            device_id_type=pl.DeviceIdType.MESH,
        )
    pl.semaphore_wait(barrier, len(axes))


def push(source, target, send_sem, recv_sem, axis):
    copy = pltpu.make_async_remote_copy(
        src_ref=source,
        dst_ref=target,
        send_sem=send_sem,
        recv_sem=recv_sem,
        device_id={axis: 1 - lax.axis_index(axis)},
        device_id_type=pl.DeviceIdType.MESH,
    )
    copy.start()
    return copy


def folder(operands, outs, grads, sums, inboxes, send_sem, recv_sem):
    count = len(outs)
    mine = {axis: lax.axis_index(axis) for axis in ("core", "y", "x", "zl", "zh")}
    core = mine["core"]
    orders = [FOLD_ORDERS[i % len(FOLD_ORDERS)] for i in range(count)]
    spread, joined = ("y", "x", "zl"), ("x", "zl")

    def cut(ref, i, depth, axes, partner=None):
        done = orders[i][:depth]
        place = dict(mine)
        if partner is not None:
            place[partner] = 1 - place[partner]
        index = [place[axis] if axis in done else slice(None) for axis in axes]
        columns = slice(None)
        if "zh" in done:
            width = ref.shape[-1] // 2
            columns = pl.ds(pl.multiple_of(place["zh"] * width, LANES), width)
        return ref.at[(*index, slice(None), columns)]

    def copy(i, k):
        if k == 0:
            source, target, axis = grads[i].at[:, 1 - core], inboxes[0][i], "core"
        elif k < 5:
            axis = orders[i][k - 1]
            source, target = cut(sums[i], i, k, spread, axis), inboxes[k][i]
        else:
            axis = [axis for axis in reversed(orders[i]) if axis != "y"][k - 5]
            source = target = cut(outs[i], i, orders[i].index(axis) + 1, joined)
        return pltpu.make_async_remote_copy(
            src_ref=source,
            dst_ref=target,
            send_sem=send_sem.at[i, k],
            recv_sem=recv_sem.at[i, k],
            device_id={axis: 1 - mine[axis]},
            device_id_type=pl.DeviceIdType.MESH,
        )

    def step(i, k):
        if k == 0:
            if operands[i] is not None:
                left_0, right_0, left_1, right_1 = operands[i]
                total = tn_dot(left_0[...], right_0[...]) + tn_dot(left_1[...], right_1[...])
                grads[i][...] = total.astype(jnp.bfloat16).reshape(grads[i].shape)
            copy(i, 0).start()
            return
        copy(i, k - 1).wait_recv()
        if k == 1:
            total = grads[i][:, core].astype(jnp.float32) + inboxes[0][i][...].astype(jnp.float32)
            sums[i][...] = total.astype(jnp.bfloat16)
        elif k < 6:
            kept = cut(sums[i], i, k - 1, spread)
            total = kept[...].astype(jnp.float32) + inboxes[k - 1][i][...].astype(jnp.float32)
            target = kept if k < 5 else cut(outs[i], i, 4, joined)
            target[...] = total.astype(jnp.bfloat16)
        if k < FOLD_STEPS - 1:
            copy(i, k).start()

    def finish():
        for i in range(count):
            for k in range(FOLD_STEPS - 1):
                copy(i, k).wait_send()

    return step, finish


PEER_AXES = ("y", "zl", "x")
PEER_BITS = {"x": 1, "zl": 2, "y": 4}
DENSE_AXES = ("zl", "y")
CHUNKS = 4


def peer_of(step):
    target, block = {}, 0
    for bit, axis in enumerate(reversed(PEER_AXES)):
        place = lax.axis_index(axis)
        if step >> bit & 1:
            place = 1 - place
            target[axis] = place
        block = block + place * (1 << bit)
    return target, block


def send(source, target, send_sem, recv_sem, device):
    copy = pltpu.make_async_remote_copy(
        src_ref=source,
        dst_ref=target,
        send_sem=send_sem,
        recv_sem=recv_sem,
        device_id=device,
        device_id_type=pl.DeviceIdType.MESH,
    )
    copy.start()
    return copy


def meet(devices):
    barrier = pltpu.get_barrier_semaphore()
    for device in devices:
        pl.semaphore_signal(
            barrier, inc=1, device_id=device, device_id_type=pl.DeviceIdType.MESH
        )
    pl.semaphore_wait(barrier, len(devices))


def across(axis):
    return {axis: 1 - lax.axis_index(axis)}


def head_kernel(
    experts,
    capacity,
    lengths_ref,
    x_ref,
    g_ref,
    routes_ref,
    routes_t_ref,
    inner_ref,
    outer_ref,
    *refs,
):
    count = 6
    parts, refs = refs[:count], refs[count:]
    wholes, refs = refs[:count], refs[count:]
    inner_outs, outer_outs, refs = refs[:4], refs[4:8], refs[8:]
    arrived_ref, refs = refs[0], refs[1:]
    normed_ref, q_ref, k_ref, v_ref, mix_ref, residual_ref, gates_ref, gain_ref, bias_ref = refs[:9]
    refs = refs[9:]
    sent_refs, token_refs, token_boxes, g_boxes, gate_boxes, route_boxes = refs[:6]
    relays, table_ref, refs = refs[6:8], refs[8], refs[9:]
    mixer_send, mixer_recv, move_send, move_recv, row_send, row_recv, local_sem = refs[:7]
    share_send, share_recv = refs[7:]
    core, y, x, zh = (lax.axis_index(axis) for axis in ("core", "y", "x", "zh"))
    at_home = zh == y
    away = zh != y
    batch, tokens, width = x_ref.shape

    meet([across("core"), across("zh"), *(peer_of(step)[0] for step in range(1, 8))])

    sources = (inner_ref, outer_ref)
    outs = (inner_outs, outer_outs)
    rows = inner_ref.shape[0] // CHUNKS

    def piece(ref, chunk):
        return ref.at[pl.ds(chunk * rows, rows)]

    class Moves:
        @staticmethod
        def copy(which, chunk, kind, source, target, axis):
            return pltpu.make_async_remote_copy(
                src_ref=piece(source, chunk),
                dst_ref=piece(target, chunk),
                send_sem=move_send.at[which, chunk, kind],
                recv_sem=move_recv.at[which, chunk, kind],
                device_id=across(axis),
                device_id_type=pl.DeviceIdType.MESH,
            )

    def move_z(which, chunk):
        source = sources[which]

        @pl.when(at_home)
        def _():
            Moves.copy(which, chunk, 0, source, outs[which][0], "zh").start()

        @pl.when(away)
        def _():
            Moves.copy(which, chunk, 0, source, relays[which], "zh").start()

    def move_first(which, chunk):
        source = sources[which]

        @pl.when(away)
        def _():
            Moves.copy(which, chunk, 1, source, outs[which][2], "y").start()

        @pl.when(at_home)
        def _():
            Moves.copy(which, chunk, 2, source, outs[which][1], "core").start()

    def relay_z(which, chunk):
        @pl.when(at_home)
        def _():
            Moves.copy(which, chunk, 0, sources[which], relays[which], "zh").wait_recv()
            Moves.copy(which, chunk, 1, relays[which], outs[which][2], "y").start()

        @pl.when(away)
        def _():
            Moves.copy(which, chunk, 0, sources[which], outs[which][0], "zh").wait_recv()
            Moves.copy(which, chunk, 2, outs[which][0], outs[which][1], "core").start()

    def relay_y(which, chunk):
        Moves.copy(which, chunk, 1, sources[which], outs[which][2], "y").wait_recv()
        Moves.copy(which, chunk, 3, outs[which][2], outs[which][3], "core").start()

    def finish(which, chunk):
        for kind, axis in ((2, "core"), (3, "core")):
            Moves.copy(which, chunk, kind, sources[which], outs[which][1], axis).wait_recv()
        for kind, axis in ((0, "zh"), (1, "y"), (2, "core"), (3, "core")):
            Moves.copy(which, chunk, kind, sources[which], outs[which][1], axis).wait_send()

    def half(part, which):
        size = part.shape[0] // 2
        return pl.ds(pl.multiple_of(which * size, size), size)

    def spot(part, whole, y_at, core_at, half_at=None):
        size = part.shape[0]
        start = (y_at * 2 + core_at) * size
        if half_at is not None:
            size = size // 2
            start = start + half_at * size
        return whole.at[pl.ds(pl.multiple_of(start, size), size)]

    shared = {}

    def share(b, kind, source, box):
        shared[b, kind] = send(
            source, box, share_send.at[b, kind], share_recv.at[b, kind], across(DENSE_AXES[b])
        )

    mixers = []
    for i, (part, whole) in enumerate(zip(parts, wholes)):
        for j, axis in enumerate(("y", "core")):
            source = part if axis == "core" else part.at[half(part, x)]
            place = spot(part, whole, y, core, x if axis == "y" else None)
            mixers.append(push(source, place, mixer_send.at[i, j], mixer_recv.at[i, j], axis))
    for chunk in range(CHUNKS):
        move_z(0, chunk)
    for b in range(batch):
        share(b, 0, g_ref.at[b], g_boxes.at[b])
        share(b, 1, routes_t_ref.at[b], route_boxes.at[b])
    for i, (part, whole) in enumerate(zip(parts, wholes)):
        spot(part, whole, y, core)[...] = part[...]
    for i, whole in enumerate(wholes):
        mixers[2 * i].wait_recv()
        place = spot(parts[i], whole, 1 - y, core, x)
        for j, axis in ((2, "x"), (3, "core")):
            mixers.append(push(place, place, mixer_send.at[i, j], mixer_recv.at[i, j], axis))
    for i, whole in enumerate(wholes):
        mixers[2 * count + 2 * i].wait_recv()
        place = spot(parts[i], whole, 1 - y, core, 1 - x)
        mixers.append(push(place, place, mixer_send.at[i, 4], mixer_recv.at[i, 4], "core"))
    for chunk in range(CHUNKS):
        move_first(0, chunk)

    @pl.when(at_home)
    def _():
        for which in range(2):
            pltpu.make_async_copy(sources[which], outs[which][0], local_sem.at[which]).start()

    for i in range(count):
        mixers[2 * i + 1].wait_recv()
        mixers[2 * count + 2 * i + 1].wait_recv()
        mixers[4 * count + i].wait_recv()

    misc = wholes[5][...].astype(jnp.float32)
    per_shard = misc.shape[0] // 4
    for i in range(2):
        line = sum(misc[s * per_shard + 3 + i : s * per_shard + 4 + i, :] for s in range(4))
        gain_ref[i : i + 1, :] = line
    for head in range(4 * 3):
        row = (head // 3) * per_shard + head % 3
        for offset in range(bias_ref.shape[2]):
            bias_ref[head // 2, head % 2, offset : offset + 1, :] = misc[
                row : row + 1, offset * 2 * LANES : (offset + 1) * 2 * LANES
            ]

    flying = []

    def forward(b):
        forward_math(
            lengths_ref[b],
            x_ref.at[b],
            routes_ref.at[b],
            *wholes[:5],
            gain_ref,
            bias_ref,
            token_refs.at[b],
            normed_ref.at[b],
            q_ref.at[b],
            k_ref.at[b],
            v_ref.at[b],
            mix_ref.at[b],
            residual_ref.at[b],
            gates_ref.at[b],
            table_ref,
        )
        share(b, 2, token_refs.at[b], token_boxes.at[b])
        share(b, 3, gates_ref.at[b], gate_boxes.at[b])

    def dispatch(b, relayed):
        axis = DENSE_AXES[b]
        bit = PEER_BITS[axis]
        if relayed:
            for kind in range(4):
                shared[b, kind].wait_recv()
            fill = dispatcher(
                experts,
                capacity,
                token_boxes.at[b],
                g_boxes.at[b],
                gate_boxes.at[b],
                route_boxes.at[b],
            )
        else:
            fill = dispatcher(
                experts,
                capacity,
                token_refs.at[b],
                g_ref.at[b],
                gates_ref.at[b],
                routes_t_ref.at[b],
            )
        _, source = peer_of(bit if relayed else 0)
        steps = [step for step in (7, 5, 6, 3, 4, 1, 2, 0) if not step & bit]
        for turn, step in enumerate(steps):
            target, block = peer_of(step)
            place = sent_refs.at[b, 4 * relayed + turn]
            fill(block, place)
            if step:
                copy = send(
                    place,
                    arrived_ref.at[b, source],
                    row_send.at[b, 4 * relayed + turn],
                    row_recv.at[b, source],
                    target,
                )
                flying.append(copy)
            else:
                copy = pltpu.make_async_copy(
                    place, arrived_ref.at[b, source], local_sem.at[2 + 2 * b + relayed]
                )
                copy.start()
                flying.append(copy)

    forward(0)
    for chunk in range(CHUNKS):
        move_z(1, chunk)
    dispatch(0, 0)
    forward(1)
    for chunk in range(CHUNKS):
        relay_z(0, chunk)
    dispatch(0, 1)
    dispatch(1, 0)
    for chunk in range(CHUNKS):
        move_first(1, chunk)
    dispatch(1, 1)
    for chunk in range(CHUNKS):
        relay_y(0, chunk)
    for chunk in range(CHUNKS):
        relay_z(1, chunk)
    for chunk in range(CHUNKS):
        relay_y(1, chunk)
    for which in range(2):
        for chunk in range(CHUNKS):
            finish(which, chunk)

    @pl.when(at_home)
    def _():
        for which in range(2):
            pltpu.make_async_copy(sources[which], outs[which][0], local_sem.at[which]).wait()

    for copy in mixers:
        copy.wait_send()
    for copy in flying:
        if copy.is_remote:
            copy.wait_send()
        else:
            copy.wait()
    for b in range(batch):
        for kind in range(4):
            shared[b, kind].wait_send()
        bit = PEER_BITS[DENSE_AXES[b]]
        for step in range(8):
            if step & ~bit:
                target, block = peer_of(step)
                pltpu.make_async_remote_copy(
                    src_ref=sent_refs.at[b, 0],
                    dst_ref=arrived_ref.at[b, block],
                    send_sem=row_send.at[b, 0],
                    recv_sem=row_recv.at[b, block],
                    device_id=target,
                    device_id_type=pl.DeviceIdType.MESH,
                ).wait_recv()


def layer_head(experts, capacity, lengths, x, g, routes, routes_t, inner, outer, parts, bias_shape):
    batch, tokens, width = x.shape
    blocks = tokens // LANES
    count = len(parts)
    shape = jax.ShapeDtypeStruct
    wholes = [shape((4 * part.shape[0], part.shape[1]), part.dtype) for part in parts]
    moved = shape(inner.shape, inner.dtype)
    exchange = (experts * capacity // SLOTS, 2, SLOTS, width)
    flat = shape(x.shape, jnp.bfloat16)
    anywhere = pl.BlockSpec(memory_space=pl.ANY)
    dma = pltpu.SemaphoreType.DMA
    results = pl.pallas_call(
        functools.partial(head_kernel, experts, capacity),
        out_shape=(
            *wholes,
            *([moved] * 8),
            shape((batch, *exchange), jnp.bfloat16),
            *([flat] * 5),
            shape(x.shape, jnp.float32),
            shape((batch, tokens, LANES), jnp.float32),
            shape((2, width), jnp.float32),
            shape(bias_shape, jnp.float32),
        ),
        in_specs=[SMEM, *([VMEM] * (6 + count))],
        out_specs=[*([VMEM] * count), *([anywhere] * 9), *([VMEM] * 9)],
        scratch_shapes=[
            pltpu.VMEM((batch, *exchange), jnp.bfloat16),
            *([pltpu.VMEM(x.shape, jnp.bfloat16)] * 3),
            pltpu.VMEM((batch, tokens, LANES), jnp.float32),
            pltpu.VMEM(routes_t.shape, jnp.int32),
            pltpu.VMEM(inner.shape, jnp.bfloat16),
            pltpu.VMEM(outer.shape, jnp.bfloat16),
            pltpu.VMEM((2, blocks, LANES, LANES), jnp.float32),
            dma((count, 5)),
            dma((count, 5)),
            dma((2, CHUNKS, 4)),
            dma((2, CHUNKS, 4)),
            dma((batch, 8)),
            dma((batch, 8)),
            dma((6,)),
            dma((batch, 4)),
            dma((batch, 4)),
        ],
        compiler_params=pltpu.CompilerParams(
            collective_id=1, has_side_effects=True, vmem_limit_bytes=60 * 2**20
        ),
        name="layer_head",
    )(lengths, x, g, routes, routes_t, inner, outer, *parts)
    wholes, rest = results[:count], results[count:]
    return wholes, rest[:4], rest[4:8], rest[8], rest[9:16], rest[16], rest[17]


def middle_kernel(arrived_ref, *refs):
    inner_refs, outer_refs, refs = refs[:4], refs[4:8], refs[8:]
    returned_ref, outs, refs = refs[0], refs[1:5], refs[5:]
    taken, going, inner_sums, outer_sums, refs = refs[0], refs[1], refs[2:6], refs[6:10], refs[10:]
    stage, inbox, take_sem, send_sem, recv_sem, local_sem, core_send, core_recv = refs
    y, zl, x = (lax.axis_index(axis) for axis in PEER_AXES)
    mine = y * 4 + zl * 2 + x
    batch, sources, _, slots, width = arrived_ref.shape
    groups = sources // 2
    total = batch * groups

    meet([across("core"), *(peer_of(step)[0] for step in range(1, 8))])
    for ref in (*inner_sums, *outer_sums):
        ref[...] = jnp.zeros_like(ref)

    def partner(i, side):
        turn = lax.rem(i, groups)
        step = turn if side == 0 else 2 * groups - 1 - turn
        places = {}
        for axis, place, flipped in (
            ("y", y, step // 4),
            ("zl", zl, lax.rem(step // 2, 2)),
            ("x", x, lax.rem(step, 2)),
        ):
            places[axis] = place + flipped - 2 * place * flipped
        return lax.div(i, groups), places, (places["y"] * 2 + places["zl"]) * 2 + places["x"]

    def take(i, side):
        b, _, block = partner(i, side)
        slot = lax.rem(i, 2)
        return pltpu.make_async_copy(
            arrived_ref.at[b, block], taken.at[slot, side], take_sem.at[slot, side]
        )

    def back(i, side, action):
        b, target, block = partner(i, side)
        slot = lax.rem(i, 2)

        def far():
            action(
                pltpu.make_async_remote_copy(
                    src_ref=going.at[slot, side],
                    dst_ref=returned_ref.at[b, mine],
                    send_sem=send_sem.at[b, block],
                    recv_sem=recv_sem.at[b, mine],
                    device_id=target,
                    device_id_type=pl.DeviceIdType.MESH,
                ),
                True,
            )

        if side:
            far()
            return
        pl.when(block != mine)(far)

        @pl.when(block == mine)
        def _():
            action(
                pltpu.make_async_copy(
                    going.at[slot, side], returned_ref.at[b, mine], local_sem.at[b]
                ),
                False,
            )

    def begin(copy, remote):
        copy.start()

    def sent(copy, remote):
        if remote:
            copy.wait_send()
        else:
            copy.wait()

    for side in range(2):
        take(0, side).start()

    def work(i, carry):
        slot = lax.rem(i, 2)

        @pl.when(i + 1 < total)
        def _():
            for side in range(2):
                take(i + 1, side).start()

        for side in range(2):
            take(i, side).wait()
        rows = taken[slot, :, 0].reshape(2 * slots, width)
        grads = taken[slot, :, 1].reshape(2 * slots, width)
        out = jnp.zeros((2 * slots, width), jnp.float32)
        result = jnp.zeros((2 * slots, width), jnp.float32)
        for part in range(4):
            inner, outer = inner_refs[part][...], outer_refs[part][...]
            pre_act = jnp.dot(rows, inner, preferred_element_type=jnp.float32)
            activated, slope = gelu_parts(pre_act)
            hidden = activated.astype(jnp.bfloat16)
            grad_pre = (nt_dot(grads, outer) * slope).astype(jnp.bfloat16)
            out = out + jnp.dot(hidden, outer, preferred_element_type=jnp.float32)
            result = result + nt_dot(grad_pre, inner)
            inner_sums[part][...] += tn_dot(rows, grad_pre)
            outer_sums[part][...] += tn_dot(hidden, grads)

        @pl.when(i >= 2)
        def _():
            for side in range(2):
                back(i - 2, side, sent)

        going[slot, :, 0] = out.astype(jnp.bfloat16).reshape(2, slots, width)
        going[slot, :, 1] = result.astype(jnp.bfloat16).reshape(2, slots, width)
        for side in range(2):
            back(i, side, begin)
        return carry

    lax.fori_loop(0, total, work, 0)
    crossing = []
    for index in range(4):
        sums = (inner_sums, outer_sums)[index % 2]
        stage[index] = sums[3 - 2 * (index // 2)][...].astype(jnp.bfloat16)
        crossing.append(
            send(
                stage.at[index],
                inbox.at[index],
                core_send.at[index],
                core_recv.at[index],
                across("core"),
            )
        )
    for index in range(4):
        sums = (inner_sums, outer_sums)[index % 2]
        crossing[index].wait()
        met = sums[2 - 2 * (index // 2)][...] + inbox[index].astype(jnp.float32)
        outs[index][...] = met.astype(jnp.bfloat16)
    for i in (total - 2, total - 1):
        for side in range(2):
            back(i, side, sent)
    for b in range(batch):
        for step in range(1, 8):
            target, block = peer_of(step)
            pltpu.make_async_remote_copy(
                src_ref=going.at[0, 0],
                dst_ref=returned_ref.at[b, block],
                send_sem=send_sem.at[b, block],
                recv_sem=recv_sem.at[b, block],
                device_id=target,
                device_id_type=pl.DeviceIdType.MESH,
            ).wait_recv()


def layer_middle(arrived, inner, outer):
    batch, sources, _, slots, width = arrived.shape
    quarter = inner[0].shape
    anywhere = pl.BlockSpec(memory_space=pl.ANY)
    dma = pltpu.SemaphoreType.DMA
    results = pl.pallas_call(
        middle_kernel,
        out_shape=(
            jax.ShapeDtypeStruct(arrived.shape, jnp.bfloat16),
            *([jax.ShapeDtypeStruct(quarter, jnp.bfloat16)] * 4),
        ),
        in_specs=[anywhere, *([VMEM] * 8)],
        out_specs=[anywhere, *([VMEM] * 4)],
        scratch_shapes=[
            pltpu.VMEM((2, 2, 2, slots, width), jnp.bfloat16),
            pltpu.VMEM((2, 2, 2, slots, width), jnp.bfloat16),
            *([pltpu.VMEM(quarter, jnp.float32)] * 8),
            pltpu.VMEM((4, *quarter), jnp.bfloat16),
            pltpu.VMEM((4, *quarter), jnp.bfloat16),
            dma((2, 2)),
            dma((batch, sources)),
            dma((batch, sources)),
            dma((batch,)),
            dma((4,)),
            dma((4,)),
        ],
        compiler_params=pltpu.CompilerParams(
            collective_id=3, has_side_effects=True, vmem_limit_bytes=63 * 2**20
        ),
        name="layer_middle",
    )(arrived, *inner, *outer)
    return results[0], results[1:]


def bias_columns(diagonals, shards, bucket_count):
    lines = diagonals.shape[1]
    width = lines
    row = row_iota(lines, 1)
    distance = (row // (2 * LANES)) * LANES + LANES - 1 - row % (2 * LANES)
    table = bucket_table(lines // (2 * LANES) * LANES)
    bucket = jnp.minimum(distance, 16)
    for value in range(17, bucket_count):
        bucket = bucket + (distance >= int(np.argmax(table >= value))).astype(jnp.int32)
    lane = column_iota(1, width)
    place = lane % (width // shards)
    heads = 3
    hot = one_hot((bucket == place % bucket_count) & (place < heads * bucket_count))
    sums = sum(jnp.dot(part, hot, preferred_element_type=jnp.float32) for part in split(diagonals))
    head = lane // (width // shards) * heads + place // bucket_count
    return jnp.sum(jnp.where(row_iota(sums.shape[0], width) == head, sums, 0.0), 0, keepdims=True)


FOLD_SPLIT = 4


def tail_kernel(experts, capacity, bucket_count, lengths_ref, *refs):
    x_ref, g_ref, routes_ref, refs = refs[0], refs[1], refs[2], refs[3:]
    weights, gain_ref, bias_ref, refs = refs[:5], refs[5], refs[6], refs[7:]
    normed_ref, q_ref, k_ref, v_ref, mix_ref, residual_ref, gates_ref, returned_ref = refs[:8]
    partials, refs = refs[8:12], refs[12:]
    result_ref, input_grad_ref, home_refs, outs, refs = (
        refs[0],
        refs[1],
        refs[2:4],
        refs[4:12],
        refs[12:],
    )
    out_rows, back_rows, branch, dq, dk, dv, router_grad, gain_grad, diag, refs = *refs[:9], refs[9:]
    grad_mix, grad_residual, scratch, refs = refs[0], refs[1], refs[2:6], refs[6:]
    grads, sums, refs = refs[:8], refs[8:16], refs[16:]
    inboxes, refs = [refs[8 * i : 8 * i + 8] for i in range(5)], refs[40:]
    fetched, landed, fold_send, fold_recv, move_send, move_recv, local_sem, own_sem = refs
    y, zh = lax.axis_index("y"), lax.axis_index("zh")
    at_home, away = zh == y, zh != y
    batch, tokens, width = x_ref.shape
    far, near = partials[:2], partials[2:]
    rows = far[0].shape[0] // CHUNKS
    cut_at = FOLD_SPLIT * LANES

    greet(("core", "y", "x", "zl", "zh"))

    def load(b):
        return [
            pltpu.make_async_copy(returned_ref.at[b, :, which], target, local_sem.at[which])
            for which, target in enumerate((out_rows, back_rows))
        ]

    def piece(ref, chunk):
        return ref.at[pl.ds(chunk * rows, rows)]

    def own(which, chunk):
        return pltpu.make_async_copy(
            piece(near[which], chunk),
            (out_rows, back_rows)[which].at[chunk],
            own_sem.at[which, chunk],
        )

    def copy(which, chunk, kind, source, target, axis):
        return pltpu.make_async_remote_copy(
            src_ref=piece(source, chunk),
            dst_ref=piece(target, chunk),
            send_sem=move_send.at[which, chunk, kind],
            recv_sem=move_recv.at[which, chunk, kind],
            device_id=across(axis),
            device_id_type=pl.DeviceIdType.MESH,
        )

    def move(index):
        which, chunk = index // CHUNKS, index % CHUNKS
        copy(which, chunk, 0, far[which], fetched.at[which], "y").wait_recv()

        @pl.when(at_home)
        def _():
            copy(which, chunk, 1, fetched.at[which], landed.at[which], "zh").start()

        @pl.when(away)
        def _():
            copy(which, chunk, 1, near[which], landed.at[which], "zh").start()

    order = [(which, chunk) for which in range(2) for chunk in range(CHUNKS)]
    for which, chunk in order:
        copy(which, chunk, 0, far[which], fetched.at[which], "y").start()
    for part in load(0):
        part.start()

    def columns(ref, b, first):
        return ref.at[b, :, :cut_at] if first else ref.at[b, :, cut_at:]

    operands = [(mix_ref.at[0], branch.at[0], mix_ref.at[1], branch.at[1])]
    for first in (True, False):
        for ref in (dq, dk, dv):
            operands.append(
                (
                    normed_ref.at[0],
                    columns(ref, 0, first),
                    normed_ref.at[1],
                    columns(ref, 1, first),
                )
            )
    operands.append(None)
    fold, fold_end = folder(operands, outs, grads, sums, inboxes, fold_send, fold_recv)
    early, late, small = (1, 2, 3), (4, 5, 6), 7

    for b in range(batch):
        for part in load(b):
            part.wait()
        combine_math(
            experts,
            capacity,
            g_ref.at[b],
            routes_ref.at[b],
            weights[3],
            weights[4],
            gain_ref,
            residual_ref.at[b],
            gates_ref.at[b],
            out_rows,
            back_rows,
            result_ref.at[b],
            branch.at[b],
            router_grad.at[b],
            gain_grad.at[b],
            grad_mix.at[b],
            grad_residual.at[b],
        )
        if b + 1 < batch:
            for part in load(b + 1):
                part.start()
            move(0)
        else:
            for which, chunk in order:
                own(which, chunk).start()
            move(1)
    fold(0, 0)

    actions = {
        0: [(fold, 0, 1), (move, 2)],
        3: [(fold, 0, 2), (move, 3)],
        5: [(move, 4)],
        7: [*((fold, i, 0) for i in early), (move, 5)],
        9: [*((fold, i, 1) for i in early), (fold, 0, 3)],
        10: [(move, 6)],
        11: [*((fold, i, 2) for i in early), (move, 7)],
    }

    def act(moment):
        for action, *values in actions[moment]:
            action(*values)

    def attend_back(item, carry):
        pair, b = item // 2, lax.rem(item, 2)
        attend_back_math(
            pair,
            lengths_ref[b],
            q_ref.at[b],
            k_ref.at[b],
            v_ref.at[b],
            grad_mix.at[b],
            bias_ref,
            dq.at[b],
            dk.at[b],
            dv.at[b],
            diag.at[b],
            *scratch,
        )
        for moment in actions:
            pl.when(item == moment)(functools.partial(act, moment))
        return carry

    lax.fori_loop(0, batch * (width // LANES), attend_back, 0)
    for i in late:
        fold(i, 0)
    for i in early:
        fold(i, 3)

    def finish(b):
        finish_math(
            x_ref.at[b],
            *weights[:3],
            gain_ref,
            dq.at[b],
            dk.at[b],
            dv.at[b],
            grad_residual.at[b],
            gain_grad.at[b],
            input_grad_ref.at[b],
        )

    finish(0)
    for i in late:
        fold(i, 1)
    fold(0, 4)
    finish(1)
    lines = [
        jnp.concatenate(
            [
                diag[0, head // 2, head % 2, offset : offset + 1, :]
                + diag[1, head // 2, head % 2, offset : offset + 1, :]
                for offset in range(diag.shape[3])
            ],
            1,
        )
        for head in range(2 * diag.shape[1])
    ]
    lines.append(jnp.zeros((16 - len(lines), width), jnp.float32))
    bias_line = bias_columns(jnp.concatenate(lines, 0), 4, bucket_count)
    gain_lines = gain_grad[0] + gain_grad[1]
    row = row_iota(LANES, width)
    stacked = jnp.where(
        row == 0,
        gain_lines[0:1, :],
        jnp.where(row == 1, gain_lines[1:2, :], jnp.where(row == 2, bias_line, 0.0)),
    )
    packed = jnp.concatenate([router_grad[0] + router_grad[1], stacked.T], 1)
    grads[small][...] = packed.astype(jnp.bfloat16).reshape(grads[small].shape)
    fold(small, 0)
    reached = {0: 5, small: 1, **dict.fromkeys(early, 4), **dict.fromkeys(late, 2)}
    while min(reached.values()) < FOLD_STEPS:
        for i in (*late, small, *early, 0):
            if reached[i] < FOLD_STEPS:
                fold(i, reached[i])
                reached[i] += 1
    fold_end()

    for which, chunk in order:
        own(which, chunk).wait()
        copy(which, chunk, 1, near[which], landed.at[which], "zh").wait()
        copy(which, chunk, 0, far[which], fetched.at[which], "y").wait_send()
        place = pl.ds(chunk * rows, rows)

        def settle(kept):
            total = kept.astype(jnp.float32) + landed[which, place].astype(jnp.float32)
            home_refs[which][place] = total.astype(jnp.bfloat16)

        pl.when(at_home)(lambda: settle((out_rows, back_rows)[which][chunk]))
        pl.when(away)(lambda: settle(fetched[which, place]))


def layer_tail(experts, capacity, bucket_count, lengths, x, g, routes, weights, gains, bias, saved, returned, partials):
    batch, tokens, width = x.shape
    blocks = tokens // LANES
    shape, dma = jax.ShapeDtypeStruct, pltpu.SemaphoreType.DMA
    anywhere = pl.BlockSpec(memory_space=pl.ANY)
    flat = shape(x.shape, jnp.bfloat16)
    quarter = partials[0].shape
    cut_at = FOLD_SPLIT * LANES
    widths = [width, *([cut_at] * 3), *([width - cut_at] * 3), 2 * LANES]
    sizes = [(width // 16, columns) for columns in widths]
    boxes = []
    for depth in range(5):
        for i, (part, columns) in enumerate(sizes):
            done = FOLD_ORDERS[i % len(FOLD_ORDERS)][:depth]
            lead = [2] * (3 - sum(axis != "zh" for axis in done))
            boxes.append(
                pltpu.VMEM(
                    (*lead, part, columns // 2 if "zh" in done else columns), jnp.bfloat16
                )
            )
    side = returned.shape[1:2] + returned.shape[3:]
    results = pl.pallas_call(
        functools.partial(tail_kernel, experts, capacity, bucket_count),
        out_shape=(
            flat,
            flat,
            *([shape(quarter, jnp.bfloat16)] * 2),
            *(shape((2, 2, *size), jnp.bfloat16) for size in sizes),
        ),
        in_specs=[SMEM, *([VMEM] * (3 + 5 + 2 + 7)), *([anywhere] * 5)],
        out_specs=[VMEM] * 12,
        scratch_shapes=[
            pltpu.VMEM(side, jnp.bfloat16),
            pltpu.VMEM(side, jnp.bfloat16),
            *([pltpu.VMEM(x.shape, jnp.bfloat16)] * 4),
            pltpu.VMEM((batch, width, LANES), jnp.float32),
            pltpu.VMEM((batch, 2, width), jnp.float32),
            pltpu.VMEM((batch, *bias.shape), jnp.float32),
            pltpu.VMEM((batch, tokens, width), jnp.bfloat16),
            pltpu.VMEM((batch, tokens, width), jnp.float32),
            pltpu.VMEM((2, blocks, LANES, LANES), jnp.float32),
            pltpu.VMEM((tokens, LANES), jnp.float32),
            pltpu.VMEM((tokens, LANES), jnp.float32),
            pltpu.VMEM((2, blocks, LANES, LANES), jnp.float32),
            *(pltpu.VMEM((2, 2, 2, 2, *size), jnp.bfloat16) for size in sizes),
            *(pltpu.VMEM((2, 2, 2, *size), jnp.bfloat16) for size in sizes),
            *boxes,
            pltpu.VMEM((2, *quarter), jnp.bfloat16),
            pltpu.VMEM((2, *quarter), jnp.bfloat16),
            dma((8, FOLD_STEPS - 1)),
            dma((8, FOLD_STEPS - 1)),
            dma((2, CHUNKS, 2)),
            dma((2, CHUNKS, 2)),
            dma((2,)),
            dma((2, CHUNKS)),
        ],
        compiler_params=pltpu.CompilerParams(
            collective_id=2, has_side_effects=True, vmem_limit_bytes=63 * 2**20
        ),
        name="layer_tail",
    )(lengths, x, g, routes, *weights, gains, bias, *saved, returned, *partials)
    output, *rest, packed = (
        out.reshape(-1, out.shape[-1]).astype(jnp.float32) for out in results[4:]
    )
    folded = [jnp.concatenate(pair, 1) for pair in zip(rest[:3], rest[3:])]
    folded += [output, packed]
    homes = [home.astype(jnp.float32) for home in results[2:4]]
    return results[0], results[1], folded, homes


class Grouped:
    swap_axes = "expert"

    def begin(self, sizes, lengths, x, g, routes, routes_t, inner, outer, parts, bias_shape):
        wholes = [lax.all_gather(part, "shard", axis=0, tiled=True) for part in parts]
        misc = wholes[5].reshape(-1, *parts[5].shape).astype(jnp.float32)
        gains = jnp.sum(misc[:, -2:], 0)
        bias_rows = misc[:, :-2].reshape(bias_shape)
        inner, outer = (list(lax.all_gather(part, "shard", axis=0)) for part in (inner, outer))
        arrived, saved = [], []
        for index in range(x.shape[0]):
            sent, *kept = layer_forward(
                index,
                *sizes,
                lengths[index : index + 1],
                x,
                g,
                routes[index],
                routes_t[index],
                wholes[:4],
                wholes[4],
                gains,
                bias_rows,
            )
            saved.append(kept)
            arrived.append(self.swap(sent))
        saved = [jnp.stack(pair) for pair in zip(*saved)]
        return wholes, inner, outer, arrived, saved, gains, bias_rows

    def swap(self, blocks):
        experts = lax.axis_size("expert")
        count, _, slots, width = blocks.shape
        merged = blocks.swapaxes(0, 1).reshape(2, experts, -1, width).swapaxes(0, 1)
        merged = lax.all_to_all(merged, "expert", split_axis=0, concat_axis=0, tiled=True)
        return merged.swapaxes(0, 1).reshape(2, count, slots, width).swapaxes(0, 1)

    def finish(
        self,
        sizes,
        bucket_count,
        lengths,
        x,
        g,
        routes,
        wholes,
        gains,
        bias_rows,
        saved,
        arrived,
        inner,
        outer,
        likes,
    ):
        returned, units = [], []
        for rows in arrived:
            going, *unit_pair = expert_pass(rows, inner, outer)
            units.append(unit_pair)
            returned.append(self.swap(going))
        returned = jnp.stack(returned)
        hiddens, pres = zip(*units)
        chunks = len(inner)
        passes = weight_pass(0, chunks, chunks, arrived, pres, hiddens)
        homes = [
            lax.psum_scatter(jnp.stack(grads), "shard", scatter_dimension=0).astype(jnp.float32)
            for grads in passes
        ]
        normed, queries, key_rows, value_rows, mixture, residual, gates = saved
        results, input_grads, grads, small = [], [], [], []
        for index in range(x.shape[0]):
            result, input_grad, branch, dq, dk, dv, *rest = layer_backward(
                index,
                *sizes,
                lengths[index : index + 1],
                x,
                g,
                routes,
                wholes[:4],
                wholes[4],
                gains,
                bias_rows,
                (queries, key_rows, value_rows, residual, gates),
                returned,
            )
            results.append(result)
            input_grads.append(input_grad)
            lefts = (normed[index],) * 3 + (mixture[index],)
            grads.append([tn_dot(*pair) for pair in zip(lefts, (dq, dk, dv, branch))])
            small.append(rest)
        router_grad, gain_grad, diagonals = (sum(parts) for parts in zip(*small))
        bias_grad = jnp.dot(
            diagonals.reshape(bias_rows.shape[0] * 2, -1),
            jnp.asarray(collect_hot(x.shape[1], bucket_count)),
            precision=HIGH,
        )
        small = (router_grad[:, : sizes[0]], gain_grad[0], gain_grad[1], bias_grad)
        shares = [
            lax.psum_scatter(
                sum(pair).astype(jnp.bfloat16), "shard", scatter_dimension=0, tiled=True
            ).astype(jnp.float32)
            for pair in (*zip(*grads), *((part,) for part in small))
        ]
        return jnp.stack(results), jnp.stack(input_grads), lax.psum(shares, "expert"), homes

    def shard_index(self):
        return lax.axis_index("shard")


class Halved:
    swap_axes = ("y", "zl", "x")

    def begin(self, sizes, lengths, x, g, routes, routes_t, inner, outer, parts, bias_shape):
        misc = jnp.pad(parts[5], ((0, 32 - parts[5].shape[0]), (0, 0)))
        return layer_head(
            *sizes, lengths, x, g, routes, routes_t, inner, outer, [*parts[:5], misc], bias_shape
        )

    def shard_index(self):
        return lax.axis_index("y") * 2 + lax.axis_index("core")

    def finish(
        self,
        sizes,
        bucket_count,
        lengths,
        x,
        g,
        routes,
        wholes,
        gains,
        bias_rows,
        saved,
        arrived,
        inner,
        outer,
        likes,
    ):
        returned, partials = layer_middle(arrived, inner, outer)
        result, input_grad, folded, homes = layer_tail(
            *sizes,
            bucket_count,
            lengths,
            x,
            g,
            routes,
            wholes[:5],
            gains,
            bias_rows,
            saved,
            returned,
            partials,
        )
        *large, packed = folded
        router, gain_one, gain_two, bias = likes
        small = [
            packed[:, : router.shape[1]],
            packed[:, LANES],
            packed[:, LANES + 1],
            packed[: bias.size, LANES + 2].reshape(bias.shape),
        ]
        return result, input_grad, [*large, *small], homes


def body(
    plan,
    tokens,
    cotangent,
    lengths,
    dealing,
    routes,
    query_weight,
    key_weight,
    value_weight,
    output_weight,
    router_weight,
    first_gain,
    second_gain,
    position_bias,
    inner_weight,
    outer_weight,
):
    batch, seq_len, model_width = tokens.shape
    experts = lax.axis_size(plan.swap_axes)
    capacity = 4 * seq_len // experts
    bucket_count = position_bias.shape[1]
    shard_rows = query_weight.shape[0]
    shards = model_width // shard_rows
    small_shard = (router_weight, first_gain, second_gain, position_bias)
    lane_shard = jnp.arange(model_width) // shard_rows
    bias_shard = jnp.dot(
        position_bias.astype(jnp.float32),
        jnp.asarray(spread_hot(seq_len, bucket_count)),
        precision=HIGH,
    ).astype(jnp.bfloat16)
    gain_shard = jnp.where(
        lane_shard == plan.shard_index(),
        jnp.tile(jnp.stack([first_gain, second_gain]), (1, shards)),
        0,
    )
    parts = [
        query_weight,
        key_weight,
        value_weight,
        output_weight,
        jnp.pad(router_weight, ((0, 0), (0, LANES - experts))),
        jnp.concatenate([bias_shard, gain_shard], 0),
    ]
    heads = shards * position_bias.shape[0]
    bias_shape = (heads // 2, 2, seq_len // LANES, 2 * LANES)
    seq_numbers = jnp.arange(lengths.shape[0], dtype=jnp.int32)
    seq_lengths = jnp.sum(jnp.where(seq_numbers == dealing[:, None], lengths, 0), 1)
    sizes = (experts, capacity)
    wholes, inner_parts, outer_parts, arrived, saved, gains, bias_rows = plan.begin(
        sizes,
        seq_lengths,
        tokens,
        cotangent,
        routes,
        jnp.pad(routes.swapaxes(1, 2), ((0, 0), (0, 6), (0, 0))),
        inner_weight[0],
        outer_weight[0],
        parts,
        bias_shape,
    )
    results, input_grads, large_and_small, homes = plan.finish(
        sizes,
        bucket_count,
        seq_lengths,
        tokens,
        cotangent,
        routes,
        wholes,
        gains,
        bias_rows,
        saved,
        arrived,
        inner_parts,
        outer_parts,
        small_shard,
    )
    return (results, input_grads, *large_and_small, homes[0][None], homes[1][None])


def solution(mesh):
    experts, shards = mesh.shape["expert"], mesh.shape["shard"]
    if (experts, shards) == (8, 4):
        plan = Halved()
        mesh = jax.sharding.Mesh(
            mesh.devices.reshape(2, 2, 2, 2, 2), ("zh", "zl", "x", "y", "core")
        )
        expert_axes, shard_axes = ("zh", "zl", "x"), ("y", "core")
    else:
        plan = Grouped()
        expert_axes, shard_axes = ("expert",), ("shard",)
    both = (*expert_axes, *shard_axes)
    rows = P(both, None, None)
    weight = P(shard_axes, None)
    in_specs = (rows, rows, P(), P(both), rows, *([weight] * 5))
    in_specs += (P(shard_axes), P(shard_axes), weight)
    in_specs += (P(expert_axes, None, shard_axes), P(expert_axes, shard_axes, None))
    out_specs = (rows, rows, *([weight] * 5), P(shard_axes), P(shard_axes), weight)
    out_specs += (P(expert_axes, None, shard_axes), P(expert_axes, shard_axes, None))
    return jax.shard_map(
        functools.partial(body, plan),
        mesh=mesh,
        in_specs=in_specs,
        out_specs=out_specs,
        check_vma=False,
    )
```

```python
import functools
import math

import jax
import jax.numpy as jnp
import numpy as np
from jax import lax
from jax.experimental import pallas as pl
from jax.experimental.pallas import tpu as pltpu
from jax.sharding import PartitionSpec as P

EPSILON = 1e-06
HIGH = lax.Precision.HIGHEST
NEGATIVE = -1000000000.0
INV_ROOT_TWO = 1.0 / math.sqrt(2.0)
INV_ROOT_TAU = 1.0 / math.sqrt(2.0 * math.pi)
LANES = 128


def bucket_table(length):
    distance = np.arange(length)
    scaled = 16 + np.floor(np.log(np.maximum(distance, 1) / 16.0) / np.log(8.0) * 16.0)
    return np.where(distance < 16, distance, np.minimum(scaled, 31)).astype(np.int32)


def gelu_parts(pre_act):
    normal_cdf = 0.5 * (1.0 + lax.erf(pre_act * INV_ROOT_TWO))
    return (
        pre_act * normal_cdf,
        normal_cdf + pre_act * jnp.exp(-0.5 * pre_act * pre_act) * INV_ROOT_TAU,
    )


def distance_table(length):
    offsets = np.arange(length // LANES)[:, None] * LANES
    return offsets, np.arange(2 * LANES)[None, :]


def spread_hot(length, bucket_count):
    offsets, lanes = distance_table(length)
    signed = np.where(lanes < LANES, lanes, lanes - 2 * LANES)
    distance = np.clip(offsets - signed, 0, length - 1).reshape(-1)
    return (bucket_table(length)[distance][None, :] == np.arange(bucket_count)[:, None]).astype(
        np.float32
    )


def collect_hot(length, bucket_count):
    offsets, lanes = distance_table(length)
    distance = (offsets + LANES - 1 - lanes).reshape(-1)
    inside = (distance >= 0) & (distance < length)
    table = bucket_table(length)[np.clip(distance, 0, length - 1)]
    return ((table[:, None] == np.arange(bucket_count)[None, :]) & inside[:, None]).astype(
        np.float32
    )


def half_mask(head):
    lane = lax.broadcasted_iota(jnp.int32, (1, LANES), 1)
    return (lane < LANES // 2) if head == 0 else (lane >= LANES // 2)


def only(value, head):
    return jnp.where(half_mask(head), value, jnp.zeros_like(value))


def nt_dot(left, right):
    return lax.dot_general(
        left, right, (((1,), (1,)), ((), ())), preferred_element_type=jnp.float32
    )


def tn_dot(left, right):
    return lax.dot_general(
        left, right, (((0,), (0,)), ((), ())), preferred_element_type=jnp.float32
    )


def toeplitz_block(row):
    spread = pltpu.roll(
        jnp.broadcast_to(row, (LANES, 2 * LANES)), 0, 1, stride=1, stride_axis=0
    )
    return spread[:, :LANES]


def fill_bias(bias_ref, table_ref, blocks):
    for head in range(2):
        for offset in range(blocks):
            table_ref[head, offset] = toeplitz_block(bias_ref[0, head, offset, :][None, :])


def masked_logits(query, keys, table_ref, head, block, length):
    width = (block + 1) * LANES
    bias = jnp.concatenate([table_ref[head, block - j] for j in range(block + 1)], 1)
    logits = nt_dot(query, keys) * ((LANES // 2) ** (-0.5)) + bias
    row = lax.broadcasted_iota(jnp.int32, (LANES, width), 0) + block * LANES
    column = lax.broadcasted_iota(jnp.int32, (LANES, width), 1)
    return jnp.where((column <= row) & (column < length), logits, NEGATIVE)


SLOTS = 192


def unit(value):
    return lax.rsqrt(jnp.mean(value * value, -1, keepdims=True) + EPSILON)


def column_iota(rows, columns):
    return lax.broadcasted_iota(jnp.int32, (rows, columns), 1)


def row_iota(rows, columns):
    return lax.broadcasted_iota(jnp.int32, (rows, columns), 0)


def row_places(routes_t_ref, experts, capacity):
    tokens = routes_t_ref.shape[1]
    padded = -(-experts // 16) * 16
    expert = row_iota(padded, tokens)
    hot = [expert == routes_t_ref[pick : pick + 1, :] for pick in range(2)]
    both = jnp.where(hot[0] | hot[1], 1.0, 0.0).astype(jnp.bfloat16)
    before = (row_iota(tokens, tokens) < column_iota(tokens, tokens)).astype(jnp.float32)
    rank = jnp.dot(both, before.astype(jnp.bfloat16), preferred_element_type=jnp.float32)
    slot = rank + (expert * capacity).astype(jnp.float32)
    return [jnp.sum(jnp.where(chosen, slot, 0.0), 0, keepdims=True) for chosen in hot]


def column_places(routes_ref, experts, capacity):
    tokens = routes_ref.shape[0]
    expert = column_iota(tokens, LANES)
    hot = [expert == routes_ref[:, pick : pick + 1] for pick in range(2)]
    both = jnp.where(hot[0] | hot[1], 1.0, 0.0).astype(jnp.bfloat16)
    before = (column_iota(tokens, tokens) < row_iota(tokens, tokens)).astype(jnp.float32)
    rank = jnp.dot(before.astype(jnp.bfloat16), both, preferred_element_type=jnp.float32)
    slot = rank + (expert * capacity).astype(jnp.float32)
    return [jnp.sum(jnp.where(chosen, slot, 0.0), 1, keepdims=True) for chosen in hot], hot


def one_hot(condition):
    return jnp.where(condition, 1.0, 0.0).astype(jnp.bfloat16)


def forward_math(
    length,
    x_ref,
    routes_ref,
    query_ref,
    key_ref,
    value_ref,
    output_ref,
    router_ref,
    gain_ref,
    bias_ref,
    tokens_ref,
    normed_ref,
    q_ref,
    k_ref,
    v_ref,
    mix_ref,
    residual_ref,
    gates_ref,
    table_ref,
):
    tokens, width = x_ref.shape
    blocks = tokens // LANES
    inputs = x_ref[...].astype(jnp.float32)
    normed = (inputs * unit(inputs) * gain_ref[0:1, :]).astype(jnp.bfloat16)
    normed_ref[...] = normed
    for weight, out in ((query_ref, q_ref), (key_ref, k_ref), (value_ref, v_ref)):
        out[...] = jnp.dot(normed, weight[...], preferred_element_type=jnp.float32).astype(
            jnp.bfloat16
        )

    def attend(pair, carry):
        lanes = pl.ds(pl.multiple_of(pair * LANES, LANES), LANES)
        fill_bias(bias_ref.at[pl.ds(pair, 1)], table_ref, blocks)
        for block in range(blocks):
            rows = pl.ds(block * LANES, LANES)
            reach = (block + 1) * LANES
            mixed = jnp.zeros((LANES, LANES), jnp.float32)
            for head in range(2):
                logits = masked_logits(
                    only(q_ref[rows, lanes], head),
                    k_ref[:reach, lanes],
                    table_ref,
                    head,
                    block,
                    length,
                )
                exponent = jnp.exp(logits - jnp.max(logits, 1, keepdims=True))
                soft = exponent / jnp.sum(exponent, 1, keepdims=True)
                mixed = mixed + jnp.dot(
                    soft.astype(jnp.bfloat16),
                    only(v_ref[:reach, lanes], head),
                    preferred_element_type=jnp.float32,
                )
            mix_ref[rows, lanes] = mixed.astype(jnp.bfloat16)
        return carry

    lax.fori_loop(0, width // LANES, attend, 0)
    residual = inputs + jnp.dot(
        mix_ref[...], output_ref[...], preferred_element_type=jnp.float32
    )
    residual_ref[...] = residual
    normed = (residual * unit(residual) * gain_ref[1:2, :]).astype(jnp.bfloat16)
    tokens_ref[...] = normed
    router = jnp.dot(normed, router_ref[...], preferred_element_type=jnp.float32)
    lane = column_iota(tokens, LANES)
    chosen = [
        jnp.sum(jnp.where(lane == routes_ref[:, pick : pick + 1], router, 0.0), 1, keepdims=True)
        for pick in range(2)
    ]
    top = jnp.maximum(chosen[0], chosen[1])
    gates = [jnp.exp(value - top) for value in chosen]
    total = gates[0] + gates[1]
    gates = [value / total for value in gates]
    gates_ref[...] = jnp.where(lane == 0, gates[0], jnp.where(lane == 1, gates[1], 0.0))


def dispatcher(experts, capacity, tokens_ref, g_ref, gates_ref, routes_t_ref):
    tokens = tokens_ref.shape[0]
    places = row_places(routes_t_ref, experts, capacity)
    grads = [
        (g_ref[...].astype(jnp.float32) * gates_ref[:, pick : pick + 1]).astype(jnp.bfloat16)
        for pick in range(2)
    ]

    def fill(index, block_ref):
        slots = block_ref.shape[1]
        slot = (row_iota(slots, tokens) + index * slots).astype(jnp.float32)
        hot = [jnp.where(slot == place, 1.0, 0.0) for place in places]
        block_ref[0] = jnp.dot(
            (hot[0] + hot[1]).astype(jnp.bfloat16),
            tokens_ref[...],
            preferred_element_type=jnp.float32,
        ).astype(jnp.bfloat16)
        block_ref[1] = (
            jnp.dot(hot[0].astype(jnp.bfloat16), grads[0], preferred_element_type=jnp.float32)
            + jnp.dot(hot[1].astype(jnp.bfloat16), grads[1], preferred_element_type=jnp.float32)
        ).astype(jnp.bfloat16)

    return fill


def forward_kernel(experts, capacity, length_ref, x_ref, g_ref, routes_ref, routes_t_ref, *refs):
    refs, (sent_ref, *outs, gates_ref, tokens_ref, table_ref) = refs[:7], refs[7:]
    forward_math(
        length_ref[0], x_ref, routes_ref, *refs, tokens_ref, *outs, gates_ref, table_ref
    )
    fill = dispatcher(experts, capacity, tokens_ref, g_ref, gates_ref, routes_t_ref)
    for index in range(sent_ref.shape[0]):
        fill(index, sent_ref.at[index])


def split(value):
    high = value.astype(jnp.bfloat16)
    return high, (value - high.astype(jnp.float32)).astype(jnp.bfloat16)


def norm_back(value, gain, grad):
    scale = unit(value)
    rows = value * scale
    grad_unit = grad * gain
    grad_gain = jnp.sum(grad * rows, 0, keepdims=True)
    mean = jnp.mean(grad_unit * rows, -1, keepdims=True)
    return scale * (grad_unit - rows * mean), grad_gain


def combine_math(
    experts,
    capacity,
    g_ref,
    routes_ref,
    output_ref,
    router_ref,
    gain_ref,
    residual_ref,
    gates_ref,
    out_rows_ref,
    back_rows_ref,
    result_ref,
    branch_ref,
    router_grad_ref,
    gain_grad_ref,
    grad_mix_ref,
    grad_residual_ref,
    tick=lambda: None,
):
    tokens, width = g_ref.shape
    grad_result = g_ref[...].astype(jnp.float32)
    residual = residual_ref[...]
    places, picks = column_places(routes_ref, experts, capacity)
    gates = [gates_ref[:, pick : pick + 1] for pick in range(2)]
    slots = out_rows_ref.shape[1]
    picked = [jnp.zeros((tokens, width), jnp.float32) for _ in range(2)]
    grad_normed = jnp.zeros((tokens, width), jnp.float32)
    for index in range(0, out_rows_ref.shape[0], 2):
        slot = (column_iota(tokens, 2 * slots) + index * slots).astype(jnp.float32)
        hot = [jnp.where(slot == place, 1.0, 0.0) for place in places]
        out_rows = out_rows_ref[index : index + 2].reshape(2 * slots, width)
        back_rows = back_rows_ref[index : index + 2].reshape(2 * slots, width)
        for pick in range(2):
            picked[pick] = picked[pick] + jnp.dot(
                hot[pick].astype(jnp.bfloat16), out_rows, preferred_element_type=jnp.float32
            )
        grad_normed = grad_normed + jnp.dot(
            (hot[0] + hot[1]).astype(jnp.bfloat16), back_rows, preferred_element_type=jnp.float32
        )
    result_ref[...] = (residual + (gates[0] * picked[0] + gates[1] * picked[1])).astype(
        jnp.bfloat16
    )
    tick()
    grad_gates = [jnp.sum(grad_result * rows, 1, keepdims=True) for rows in picked]
    common = gates[0] * grad_gates[0] + gates[1] * grad_gates[1]
    grad_router = jnp.zeros((tokens, LANES), jnp.float32)
    for pick in range(2):
        grad_router = grad_router + jnp.where(
            picks[pick], gates[pick] * (grad_gates[pick] - common), 0.0
        )
    normed = (residual * unit(residual) * gain_ref[1:2, :]).astype(jnp.bfloat16)
    router_grad = jnp.zeros((width, LANES), jnp.float32)
    for part in split(grad_router):
        grad_normed = grad_normed + nt_dot(part, router_ref[...])
        router_grad = router_grad + tn_dot(normed, part)
    router_grad_ref[...] = router_grad
    from_norm, grad_gain = norm_back(residual, gain_ref[1:2, :], grad_normed)
    gain_grad_ref[1:2, :] = grad_gain
    grad_residual = grad_result + from_norm
    grad_residual_ref[...] = grad_residual
    branch = grad_residual.astype(jnp.bfloat16)
    branch_ref[...] = branch
    grad_mix_ref[...] = nt_dot(branch, output_ref[...]).astype(jnp.bfloat16)


def attend_back_math(
    pair,
    length,
    q_ref,
    k_ref,
    v_ref,
    grad_mix_ref,
    bias_ref,
    dq_ref,
    dk_ref,
    dv_ref,
    diag_ref,
    table_ref,
    dk_sum,
    dv_sum,
    skew_ref,
):
    blocks = q_ref.shape[0] // LANES
    scale = (LANES // 2) ** (-0.5)
    upside = (row_iota(LANES, LANES) + column_iota(LANES, LANES) == LANES - 1).astype(jnp.float32)
    lanes = pl.ds(pl.multiple_of(pair * LANES, LANES), LANES)
    fill_bias(bias_ref.at[pl.ds(pair, 1)], table_ref, blocks)
    dk_sum[...] = jnp.zeros_like(dk_sum)
    dv_sum[...] = jnp.zeros_like(dv_sum)
    skew_ref[...] = jnp.zeros_like(skew_ref)
    for block in range(blocks):
        rows = pl.ds(block * LANES, LANES)
        reach = (block + 1) * LANES
        dq = jnp.zeros((LANES, LANES), jnp.float32)
        for head in range(2):
            query = only(q_ref[rows, lanes], head)
            grad = only(grad_mix_ref[rows, lanes], head)
            keys = k_ref[:reach, lanes]
            logits = masked_logits(query, keys, table_ref, head, block, length)
            exponent = jnp.exp(logits - jnp.max(logits, 1, keepdims=True))
            soft = exponent / jnp.sum(exponent, 1, keepdims=True)
            grad_soft = nt_dot(grad, v_ref[:reach, lanes])
            inner = jnp.sum(soft * grad_soft, 1, keepdims=True)
            grad_logits = (soft * (grad_soft - inner)).astype(jnp.bfloat16)
            dv_sum[:reach, :] += tn_dot(soft.astype(jnp.bfloat16), grad)
            dk_sum[:reach, :] += tn_dot(grad_logits, query)
            dq = dq + jnp.dot(
                grad_logits, only(keys, head), preferred_element_type=jnp.float32
            )
            wide = grad_logits.astype(jnp.float32)
            for j in range(block + 1):
                skew_ref[head, block - j] += wide[:, j * LANES : (j + 1) * LANES]
        dq_ref[rows, lanes] = (dq * scale).astype(jnp.bfloat16)
    dk_ref[:, lanes] = (dk_sum[...] * scale).astype(jnp.bfloat16)
    dv_ref[:, lanes] = dv_sum[...].astype(jnp.bfloat16)
    for head in range(2):
        for offset in range(blocks):
            flipped = jnp.dot(
                upside,
                skew_ref[head, offset],
                precision=HIGH,
                preferred_element_type=jnp.float32,
            )
            padded = jnp.concatenate([flipped, jnp.zeros_like(flipped)], 1)
            lined = pltpu.roll(padded, 0, 1, stride=1, stride_axis=0)
            diag_ref[pair, head, offset, :] = jnp.sum(lined, 0)


def finish_math(
    x_ref,
    query_ref,
    key_ref,
    value_ref,
    gain_ref,
    dq_ref,
    dk_ref,
    dv_ref,
    grad_residual_ref,
    gain_grad_ref,
    input_grad_ref,
):
    grad_normed = nt_dot(dq_ref[...], query_ref[...])
    grad_normed = grad_normed + nt_dot(dk_ref[...], key_ref[...])
    grad_normed = grad_normed + nt_dot(dv_ref[...], value_ref[...])
    inputs = x_ref[...].astype(jnp.float32)
    from_norm, grad_gain = norm_back(inputs, gain_ref[0:1, :], grad_normed)
    gain_grad_ref[0:1, :] = grad_gain
    input_grad_ref[...] = (grad_residual_ref[...] + from_norm).astype(jnp.bfloat16)


def backward_kernel(
    experts,
    capacity,
    length_ref,
    x_ref,
    g_ref,
    routes_ref,
    query_ref,
    key_ref,
    value_ref,
    output_ref,
    router_ref,
    gain_ref,
    bias_ref,
    q_ref,
    k_ref,
    v_ref,
    residual_ref,
    gates_ref,
    out_rows_ref,
    back_rows_ref,
    result_ref,
    input_grad_ref,
    branch_ref,
    dq_ref,
    dk_ref,
    dv_ref,
    router_grad_ref,
    gain_grad_ref,
    diag_ref,
    grad_mix_ref,
    grad_residual_ref,
    *scratch,
):
    combine_math(
        experts,
        capacity,
        g_ref,
        routes_ref,
        output_ref,
        router_ref,
        gain_ref,
        residual_ref,
        gates_ref,
        out_rows_ref,
        back_rows_ref,
        result_ref,
        branch_ref,
        router_grad_ref,
        gain_grad_ref,
        grad_mix_ref,
        grad_residual_ref,
    )

    def attend_back(pair, carry):
        attend_back_math(
            pair,
            length_ref[0],
            q_ref,
            k_ref,
            v_ref,
            grad_mix_ref,
            bias_ref,
            dq_ref,
            dk_ref,
            dv_ref,
            diag_ref,
            *scratch,
        )
        return carry

    lax.fori_loop(0, x_ref.shape[1] // LANES, attend_back, 0)
    finish_math(
        x_ref,
        query_ref,
        key_ref,
        value_ref,
        gain_ref,
        dq_ref,
        dk_ref,
        dv_ref,
        grad_residual_ref,
        gain_grad_ref,
        input_grad_ref,
    )


VMEM = pl.BlockSpec(memory_space=pltpu.VMEM)
SMEM = pl.BlockSpec(memory_space=pltpu.SMEM)


def layer_forward(index, experts, capacity, length, x, g, routes, routes_t, weights, router, gains, bias):
    _, tokens, width = x.shape
    blocks = tokens // LANES
    flat = jax.ShapeDtypeStruct((tokens, width), jnp.bfloat16)
    rows = pl.BlockSpec((None, tokens, width), lambda i: (index, 0, 0))
    return pl.pallas_call(
        functools.partial(forward_kernel, experts, capacity),
        grid=(1,),
        out_shape=(
            jax.ShapeDtypeStruct((experts * capacity // SLOTS, 2, SLOTS, width), jnp.bfloat16),
            flat,
            flat,
            flat,
            flat,
            flat,
            jax.ShapeDtypeStruct((tokens, width), jnp.float32),
            jax.ShapeDtypeStruct((tokens, LANES), jnp.float32),
        ),
        in_specs=[SMEM, rows, rows, *([VMEM] * 9)],
        out_specs=[VMEM] * 8,
        scratch_shapes=[
            pltpu.VMEM((tokens, width), jnp.bfloat16),
            pltpu.VMEM((2, blocks, LANES, LANES), jnp.float32),
        ],
        compiler_params=pltpu.CompilerParams(vmem_limit_bytes=56 * 2**20),
        cost_estimate=pl.CostEstimate(
            flops=2 * tokens * width * (4 * width + 4 * tokens + 6 * tokens),
            bytes_accessed=40 * tokens * width,
            transcendentals=tokens * tokens * 12,
        ),
        name="layer_forward",
    )(length, x, g, routes, routes_t, *weights, router, gains, bias)


def layer_backward(
    index, experts, capacity, length, x, g, routes, weights, router, gains, bias, saved, returned
):
    _, tokens, width = x.shape
    blocks = tokens // LANES
    flat = jax.ShapeDtypeStruct((tokens, width), jnp.bfloat16)
    _, count, _, slots, _ = returned.shape

    def one(array):
        return pl.BlockSpec((None, *array.shape[1:]), lambda i: (index, 0, 0))

    rows = one(x)

    def side(which):
        return pl.BlockSpec(
            (None, count, None, slots, width), lambda i: (index, 0, which, 0, 0)
        )

    return pl.pallas_call(
        functools.partial(backward_kernel, experts, capacity),
        grid=(1,),
        out_shape=(
            *([flat] * 6),
            jax.ShapeDtypeStruct((width, LANES), jnp.float32),
            jax.ShapeDtypeStruct((2, width), jnp.float32),
            jax.ShapeDtypeStruct(bias.shape, jnp.float32),
        ),
        in_specs=[
            SMEM,
            rows,
            rows,
            one(routes),
            *([VMEM] * 7),
            *map(one, saved),
            side(0),
            side(1),
        ],
        out_specs=[VMEM] * 9,
        scratch_shapes=[
            pltpu.VMEM((tokens, width), jnp.bfloat16),
            pltpu.VMEM((tokens, width), jnp.float32),
            pltpu.VMEM((2, blocks, LANES, LANES), jnp.float32),
            pltpu.VMEM((tokens, LANES), jnp.float32),
            pltpu.VMEM((tokens, LANES), jnp.float32),
            pltpu.VMEM((2, blocks, LANES, LANES), jnp.float32),
        ],
        compiler_params=pltpu.CompilerParams(vmem_limit_bytes=56 * 2**20),
        cost_estimate=pl.CostEstimate(
            flops=2 * tokens * width * (4 * width + 12 * tokens + 10 * tokens),
            bytes_accessed=40 * tokens * width,
            transcendentals=tokens * tokens * 12,
        ),
        name="layer_backward",
    )(length, x, g, routes, *weights, router, gains, bias, *saved, returned, returned)


def expert_kernel(count, x_ref, g_ref, *refs):
    inner_refs, outer_refs = refs[:count], refs[count : 2 * count]
    back_ref, hidden_ref, grad_ref = refs[2 * count :]
    shape = x_ref.shape
    inputs = x_ref[...].reshape(-1, shape[-1])
    grads = g_ref[...].reshape(-1, shape[-1])
    out = jnp.zeros(inputs.shape, jnp.float32)
    back = jnp.zeros(inputs.shape, jnp.float32)
    start = 0
    for inner_ref, outer_ref in zip(inner_refs, outer_refs):
        part = pl.ds(start, inner_ref.shape[1])
        start += inner_ref.shape[1]
        pre_act = jnp.dot(inputs, inner_ref[...], preferred_element_type=jnp.float32)
        activated, slope = gelu_parts(pre_act)
        hidden = activated.astype(jnp.bfloat16)
        grad_pre = (nt_dot(grads, outer_ref[...]) * slope).astype(jnp.bfloat16)
        hidden_ref[:, part] = hidden
        grad_ref[:, part] = grad_pre
        out = out + jnp.dot(hidden, outer_ref[...], preferred_element_type=jnp.float32)
        back = back + nt_dot(grad_pre, inner_ref[...])
    back_ref[:, 0] = out.astype(jnp.bfloat16).reshape(shape)
    back_ref[:, 1] = back.astype(jnp.bfloat16).reshape(shape)


def expert_pass(arrived, inner, outer):
    sources, _, capacity, width = arrived.shape
    total = sources * capacity
    units = sum(part.shape[1] for part in inner)
    group = sources // 4

    def side(which):
        return pl.BlockSpec((group, None, capacity, width), lambda i: (i, which, 0, 0))

    def whole(shape):
        return pl.BlockSpec(shape, lambda i: (0, 0), pipeline_mode=pl.Buffered(1))

    unit_spec = pl.BlockSpec((group * capacity, units), lambda i: (i, 0))
    deep = jax.ShapeDtypeStruct((total, units), jnp.bfloat16)
    return pl.pallas_call(
        functools.partial(expert_kernel, len(inner)),
        grid=(sources // group,),
        out_shape=(jax.ShapeDtypeStruct(arrived.shape, jnp.bfloat16), deep, deep),
        in_specs=[side(0), side(1), *(whole(part.shape) for part in (*inner, *outer))],
        out_specs=(
            pl.BlockSpec((group, 2, capacity, width), lambda i: (i, 0, 0, 0)),
            unit_spec,
            unit_spec,
        ),
        compiler_params=pltpu.CompilerParams(vmem_limit_bytes=60 * 2**20),
        cost_estimate=pl.CostEstimate(
            flops=8 * total * width * units,
            bytes_accessed=4 * (2 * width + units) * total + 4 * width * units,
            transcendentals=2 * total * units,
        ),
        name="expert_pass",
    )(arrived, arrived, *inner, *outer)


def weight_kernel(x0_ref, x1_ref, g0_ref, g1_ref, p0_ref, p1_ref, h0_ref, h1_ref, *out_refs):
    inner_ref, outer_ref = out_refs

    def flat(ref):
        return ref[...].reshape(-1, ref.shape[-1])

    inner = tn_dot(flat(x0_ref), p0_ref[...]) + tn_dot(flat(x1_ref), p1_ref[...])
    inner_ref[...] = inner.astype(jnp.bfloat16)
    outer = tn_dot(h0_ref[...], flat(g0_ref)) + tn_dot(h1_ref[...], flat(g1_ref))
    outer_ref[...] = outer.astype(jnp.bfloat16)


def weight_pass(first, count, chunks, arrived, pres, hiddens):
    sources, _, capacity, width = arrived[0].shape
    total = sources * capacity
    size = hiddens[0].shape[1] // chunks
    step = math.gcd(size, 256)
    steps = size // step

    def side(which):
        return pl.BlockSpec(
            (sources, None, capacity, width),
            lambda i: (0, which, 0, 0),
            pipeline_mode=pl.Buffered(1),
        )

    units = pl.BlockSpec((total, step), lambda i: (0, first * steps + i))
    inner, outer = pl.pallas_call(
        weight_kernel,
        grid=(count * steps,),
        out_shape=(
            jax.ShapeDtypeStruct((count, width, size), jnp.bfloat16),
            jax.ShapeDtypeStruct((count * size, width), jnp.bfloat16),
        ),
        in_specs=[side(0)] * 2 + [side(1)] * 2 + [units] * 4,
        out_specs=(
            pl.BlockSpec((None, width, step), lambda i: (i // steps, 0, i % steps)),
            pl.BlockSpec((step, width), lambda i: (i, 0)),
        ),
        compiler_params=pltpu.CompilerParams(vmem_limit_bytes=60 * 2**20),
        cost_estimate=pl.CostEstimate(
            flops=8 * total * width * count * size,
            bytes_accessed=8 * total * (width + count * size) + 4 * width * count * size,
            transcendentals=0,
        ),
        name="weight_pass",
    )(*arrived, *arrived, *pres, *hiddens)
    return list(inner), list(outer.reshape(count, size, width))


FOLD_ORDERS = (("x", "y", "zl", "zh"), ("y", "x", "zl", "zh"))
FOLD_STEPS = 9


def greet(axes):
    barrier = pltpu.get_barrier_semaphore()
    for axis in axes:
        pl.semaphore_signal(
            barrier,
            inc=1,
            device_id={axis: 1 - lax.axis_index(axis)},
            device_id_type=pl.DeviceIdType.MESH,
        )
    pl.semaphore_wait(barrier, len(axes))


def push(source, target, send_sem, recv_sem, axis):
    copy = pltpu.make_async_remote_copy(
        src_ref=source,
        dst_ref=target,
        send_sem=send_sem,
        recv_sem=recv_sem,
        device_id={axis: 1 - lax.axis_index(axis)},
        device_id_type=pl.DeviceIdType.MESH,
    )
    copy.start()
    return copy


def folder(operands, outs, grads, sums, inboxes, send_sem, recv_sem):
    count = len(outs)
    mine = {axis: lax.axis_index(axis) for axis in ("core", "y", "x", "zl", "zh")}
    core = mine["core"]
    orders = [FOLD_ORDERS[i % len(FOLD_ORDERS)] for i in range(count)]
    spread, joined = ("y", "x", "zl"), ("x", "zl")

    def cut(ref, i, depth, axes, partner=None):
        done = orders[i][:depth]
        place = dict(mine)
        if partner is not None:
            place[partner] = 1 - place[partner]
        index = [place[axis] if axis in done else slice(None) for axis in axes]
        columns = slice(None)
        if "zh" in done:
            width = ref.shape[-1] // 2
            columns = pl.ds(pl.multiple_of(place["zh"] * width, LANES), width)
        return ref.at[(*index, slice(None), columns)]

    def copy(i, k):
        if k == 0:
            source, target, axis = grads[i].at[:, 1 - core], inboxes[0][i], "core"
        elif k < 5:
            axis = orders[i][k - 1]
            source, target = cut(sums[i], i, k, spread, axis), inboxes[k][i]
        else:
            axis = [axis for axis in reversed(orders[i]) if axis != "y"][k - 5]
            source = target = cut(outs[i], i, orders[i].index(axis) + 1, joined)
        return pltpu.make_async_remote_copy(
            src_ref=source,
            dst_ref=target,
            send_sem=send_sem.at[i, k],
            recv_sem=recv_sem.at[i, k],
            device_id={axis: 1 - mine[axis]},
            device_id_type=pl.DeviceIdType.MESH,
        )

    def step(i, k):
        if k == 0:
            if operands[i] is not None:
                left_0, right_0, left_1, right_1 = operands[i]
                total = tn_dot(left_0[...], right_0[...]) + tn_dot(left_1[...], right_1[...])
                grads[i][...] = total.astype(jnp.bfloat16).reshape(grads[i].shape)
            copy(i, 0).start()
            return
        copy(i, k - 1).wait_recv()
        if k == 1:
            total = grads[i][:, core].astype(jnp.float32) + inboxes[0][i][...].astype(jnp.float32)
            sums[i][...] = total.astype(jnp.bfloat16)
        elif k < 6:
            kept = cut(sums[i], i, k - 1, spread)
            total = kept[...].astype(jnp.float32) + inboxes[k - 1][i][...].astype(jnp.float32)
            target = kept if k < 5 else cut(outs[i], i, 4, joined)
            target[...] = total.astype(jnp.bfloat16)
        if k < FOLD_STEPS - 1:
            copy(i, k).start()

    def finish():
        for i in range(count):
            for k in range(FOLD_STEPS - 1):
                copy(i, k).wait_send()

    return step, finish


PEER_AXES = ("y", "zl", "x")
PEER_BITS = {"x": 1, "zl": 2, "y": 4}
DENSE_AXES = ("zl", "y")
CHUNKS = 4


def peer_of(step):
    target, block = {}, 0
    for bit, axis in enumerate(reversed(PEER_AXES)):
        place = lax.axis_index(axis)
        if step >> bit & 1:
            place = 1 - place
            target[axis] = place
        block = block + place * (1 << bit)
    return target, block


def send_later(source, target, send_sem, recv_sem, device):
    return pltpu.make_async_remote_copy(
        src_ref=source,
        dst_ref=target,
        send_sem=send_sem,
        recv_sem=recv_sem,
        device_id=device,
        device_id_type=pl.DeviceIdType.MESH,
    )


def send(*values):
    copy = send_later(*values)
    copy.start()
    return copy


def meet(devices):
    barrier = pltpu.get_barrier_semaphore()
    for device in devices:
        pl.semaphore_signal(
            barrier, inc=1, device_id=device, device_id_type=pl.DeviceIdType.MESH
        )
    pl.semaphore_wait(barrier, len(devices))


def across(axis):
    return {axis: 1 - lax.axis_index(axis)}


def head_kernel(
    experts,
    capacity,
    lengths_ref,
    dealing_ref,
    x_ref,
    g_ref,
    routes_ref,
    routes_t_ref,
    inner_ref,
    outer_ref,
    *refs,
):
    count = 6
    parts, refs = refs[:count], refs[count:]
    wholes, refs = refs[:count], refs[count:]
    inner_outs, outer_outs, refs = refs[:4], refs[4:8], refs[8:]
    arrived_ref, refs = refs[0], refs[1:]
    targets, gates_ref, gain_ref, bias_ref, refs = refs[:6], *refs[6:9], refs[9:]
    sent_refs, token_refs, token_boxes, g_boxes, gate_boxes, route_boxes = refs[:6]
    relays, table_ref, refs = refs[6:8], refs[8], refs[9:]
    mixer_send, mixer_recv, move_send, move_recv, row_send, row_recv, local_sem = refs[:7]
    share_send, share_recv, keep_sem, *kept = refs[7:]
    normed_ref, q_ref, k_ref, v_ref, mix_ref, residual_ref = kept[:6]
    whole_targets, wholes = wholes[:5], [*kept[6:], wholes[5]]
    core, y, x, zh = (lax.axis_index(axis) for axis in ("core", "y", "x", "zh"))
    at_home = zh == y
    away = zh != y
    batch, tokens, width = x_ref.shape

    meet([across("core"), across("zh"), *(peer_of(step)[0] for step in range(1, 8))])

    sources = (inner_ref, outer_ref)
    outs = (inner_outs, outer_outs)
    rows = inner_ref.shape[0] // CHUNKS

    def piece(ref, chunk):
        return ref.at[pl.ds(chunk * rows, rows)]

    class Moves:
        @staticmethod
        def copy(which, chunk, kind, source, target, axis):
            return pltpu.make_async_remote_copy(
                src_ref=piece(source, chunk),
                dst_ref=piece(target, chunk),
                send_sem=move_send.at[which, chunk, kind],
                recv_sem=move_recv.at[which, chunk, kind],
                device_id=across(axis),
                device_id_type=pl.DeviceIdType.MESH,
            )

    def move_z(which, chunk):
        source = sources[which]

        @pl.when(at_home)
        def _():
            Moves.copy(which, chunk, 0, source, outs[which][0], "zh").start()

        @pl.when(away)
        def _():
            Moves.copy(which, chunk, 0, source, relays[which], "zh").start()

    def move_first(which, chunk):
        source = sources[which]

        @pl.when(away)
        def _():
            Moves.copy(which, chunk, 1, source, outs[which][2], "y").start()

        @pl.when(at_home)
        def _():
            Moves.copy(which, chunk, 2, source, outs[which][1], "core").start()

    def relay_z(which, chunk):
        @pl.when(at_home)
        def _():
            Moves.copy(which, chunk, 0, sources[which], relays[which], "zh").wait_recv()
            Moves.copy(which, chunk, 1, relays[which], outs[which][2], "y").start()

        @pl.when(away)
        def _():
            Moves.copy(which, chunk, 0, sources[which], outs[which][0], "zh").wait_recv()
            Moves.copy(which, chunk, 2, outs[which][0], outs[which][1], "core").start()

    def relay_y(which, chunk):
        Moves.copy(which, chunk, 1, sources[which], outs[which][2], "y").wait_recv()
        Moves.copy(which, chunk, 3, outs[which][2], outs[which][3], "core").start()

    def finish(which, chunk):
        for kind, axis in ((2, "core"), (3, "core")):
            Moves.copy(which, chunk, kind, sources[which], outs[which][1], axis).wait_recv()
        for kind, axis in ((0, "zh"), (1, "y"), (2, "core"), (3, "core")):
            Moves.copy(which, chunk, kind, sources[which], outs[which][1], axis).wait_send()

    def half(part, which):
        size = part.shape[0] // 2
        return pl.ds(pl.multiple_of(which * size, size), size)

    def spot(part, whole, y_at, core_at, half_at=None):
        size = part.shape[0]
        start = (y_at * 2 + core_at) * size
        if half_at is not None:
            size = size // 2
            start = start + half_at * size
        return whole.at[pl.ds(pl.multiple_of(start, size), size)]

    def share(b, kind):
        source = (g_ref, routes_t_ref, token_refs, gates_ref)[kind]
        box = (g_boxes, route_boxes, token_boxes, gate_boxes)[kind]
        return send_later(
            source.at[b],
            box.at[b],
            share_send.at[b, kind],
            share_recv.at[b, kind],
            across(DENSE_AXES[b]),
        )

    mixers = []
    for i, (part, whole) in enumerate(zip(parts, wholes)):
        for j, axis in enumerate(("y", "core")):
            source = part if axis == "core" else part.at[half(part, x)]
            place = spot(part, whole, y, core, x if axis == "y" else None)
            mixers.append(push(source, place, mixer_send.at[i, j], mixer_recv.at[i, j], axis))
    for chunk in range(CHUNKS):
        move_z(0, chunk)
    for b in range(batch):
        share(b, 0).start()
        share(b, 1).start()
    for i, (part, whole) in enumerate(zip(parts, wholes)):
        spot(part, whole, y, core)[...] = part[...]
    for i, whole in enumerate(wholes):
        mixers[2 * i].wait_recv()
        place = spot(parts[i], whole, 1 - y, core, x)
        for j, axis in ((2, "x"), (3, "core")):
            mixers.append(push(place, place, mixer_send.at[i, j], mixer_recv.at[i, j], axis))
    for i, whole in enumerate(wholes):
        mixers[2 * count + 2 * i].wait_recv()
        place = spot(parts[i], whole, 1 - y, core, 1 - x)
        mixers.append(push(place, place, mixer_send.at[i, 4], mixer_recv.at[i, 4], "core"))
    for chunk in range(CHUNKS):
        move_first(0, chunk)

    @pl.when(at_home)
    def _():
        for which in range(2):
            pltpu.make_async_copy(sources[which], outs[which][0], local_sem.at[which]).start()

    for i in range(count):
        mixers[2 * i + 1].wait_recv()
        mixers[2 * count + 2 * i + 1].wait_recv()
        mixers[4 * count + i].wait_recv()

    misc = wholes[5][...].astype(jnp.float32)
    per_shard = misc.shape[0] // 4
    for i in range(2):
        line = sum(misc[s * per_shard + 3 + i : s * per_shard + 4 + i, :] for s in range(4))
        gain_ref[i : i + 1, :] = line
    for head in range(4 * 3):
        row = (head // 3) * per_shard + head % 3
        for offset in range(bias_ref.shape[2]):
            bias_ref[head // 2, head % 2, offset : offset + 1, :] = misc[
                row : row + 1, offset * 2 * LANES : (offset + 1) * 2 * LANES
            ]

    keeps = [
        pltpu.make_async_copy(source, target, keep_sem.at[index])
        for index, (source, target) in enumerate(zip(wholes, whole_targets))
    ]
    for part in keeps:
        part.start()

    def keep(b):
        return [
            pltpu.make_async_copy(source.at[b], target.at[b], keep_sem.at[5 + 6 * b + index])
            for index, (source, target) in enumerate(zip(kept, targets))
        ]

    def forward(b, carry):
        forward_math(
            lengths_ref[dealing_ref[b]],
            x_ref.at[b],
            routes_ref.at[b],
            *wholes[:5],
            gain_ref,
            bias_ref,
            token_refs.at[b],
            normed_ref.at[b],
            q_ref.at[b],
            k_ref.at[b],
            v_ref.at[b],
            mix_ref.at[b],
            residual_ref.at[b],
            gates_ref.at[b],
            table_ref,
        )
        for part in keep(b):
            part.start()

        @pl.when(b == 0)
        def _():
            for kind in (2, 3):
                share(0, kind).start()
            for chunk in range(CHUNKS):
                move_z(1, chunk)
            dispatch(0, 0)

        @pl.when(b == 1)
        def _():
            for kind in (2, 3):
                share(1, kind).start()

        return carry

    def steps_of(b):
        bit = PEER_BITS[DENSE_AXES[b]]
        return [step for step in (7, 5, 6, 3, 4, 1, 2, 0) if not step & bit]

    def row_copy(b, relayed, turn):
        _, source = peer_of(PEER_BITS[DENSE_AXES[b]] if relayed else 0)
        step = steps_of(b)[turn]
        place = sent_refs.at[b, 4 * relayed + turn]
        if step:
            return send_later(
                place,
                arrived_ref.at[b, source],
                row_send.at[b, 4 * relayed + turn],
                row_recv.at[b, source],
                peer_of(step)[0],
            )
        return pltpu.make_async_copy(
            place, arrived_ref.at[b, source], local_sem.at[2 + 2 * b + relayed]
        )

    def dispatch(b, relayed):
        if relayed:
            for kind in range(4):
                share(b, kind).wait_recv()
            fill = dispatcher(
                experts,
                capacity,
                token_boxes.at[b],
                g_boxes.at[b],
                gate_boxes.at[b],
                route_boxes.at[b],
            )
        else:
            fill = dispatcher(
                experts,
                capacity,
                token_refs.at[b],
                g_ref.at[b],
                gates_ref.at[b],
                routes_t_ref.at[b],
            )
        for turn, step in enumerate(steps_of(b)):
            fill(peer_of(step)[1], sent_refs.at[b, 4 * relayed + turn])
            row_copy(b, relayed, turn).start()

    lax.fori_loop(0, batch, forward, 0)
    for chunk in range(CHUNKS):
        relay_z(0, chunk)
    dispatch(0, 1)
    dispatch(1, 0)
    for chunk in range(CHUNKS):
        move_first(1, chunk)
    dispatch(1, 1)
    for chunk in range(CHUNKS):
        relay_y(0, chunk)
    for chunk in range(CHUNKS):
        relay_z(1, chunk)
    for chunk in range(CHUNKS):
        relay_y(1, chunk)
    for which in range(2):
        for chunk in range(CHUNKS):
            finish(which, chunk)

    @pl.when(at_home)
    def _():
        for which in range(2):
            pltpu.make_async_copy(sources[which], outs[which][0], local_sem.at[which]).wait()

    for part in (*keeps, *keep(0), *keep(1)):
        part.wait()
    for copy in mixers:
        copy.wait_send()
    for b in range(batch):
        for relayed in range(2):
            for turn, step in enumerate(steps_of(b)):
                if step:
                    row_copy(b, relayed, turn).wait_send()
                else:
                    row_copy(b, relayed, turn).wait()
        for kind in range(4):
            share(b, kind).wait_send()
        bit = PEER_BITS[DENSE_AXES[b]]
        for step in range(8):
            if step & ~bit:
                target, block = peer_of(step)
                pltpu.make_async_remote_copy(
                    src_ref=sent_refs.at[b, 0],
                    dst_ref=arrived_ref.at[b, block],
                    send_sem=row_send.at[b, 0],
                    recv_sem=row_recv.at[b, block],
                    device_id=target,
                    device_id_type=pl.DeviceIdType.MESH,
                ).wait_recv()


def layer_head(experts, capacity, lengths, x, g, routes, routes_t, inner, outer, parts, bias_shape):
    batch, tokens, width = x.shape
    blocks = tokens // LANES
    count = len(parts)
    shape = jax.ShapeDtypeStruct
    wholes = [shape((4 * part.shape[0], part.shape[1]), part.dtype) for part in parts]
    moved = shape(inner.shape, inner.dtype)
    exchange = (experts * capacity // SLOTS, 2, SLOTS, width)
    flat = shape(x.shape, jnp.bfloat16)
    anywhere = pl.BlockSpec(memory_space=pl.ANY)
    dma = pltpu.SemaphoreType.DMA
    results = pl.pallas_call(
        functools.partial(head_kernel, experts, capacity),
        out_shape=(
            *wholes,
            *([moved] * 8),
            shape((batch, *exchange), jnp.bfloat16),
            *([flat] * 5),
            shape(x.shape, jnp.float32),
            shape((batch, tokens, LANES), jnp.float32),
            shape((2, width), jnp.float32),
            shape(bias_shape, jnp.float32),
        ),
        in_specs=[SMEM, SMEM, *([VMEM] * (6 + count))],
        out_specs=[*([anywhere] * 5), VMEM, *([anywhere] * 9), *([anywhere] * 6), *([VMEM] * 3)],
        scratch_shapes=[
            pltpu.VMEM((batch, *exchange), jnp.bfloat16),
            *([pltpu.VMEM(x.shape, jnp.bfloat16)] * 3),
            pltpu.VMEM((batch, tokens, LANES), jnp.float32),
            pltpu.VMEM(routes_t.shape, jnp.int32),
            pltpu.VMEM(inner.shape, jnp.bfloat16),
            pltpu.VMEM(outer.shape, jnp.bfloat16),
            pltpu.VMEM((2, blocks, LANES, LANES), jnp.float32),
            dma((count, 5)),
            dma((count, 5)),
            dma((2, CHUNKS, 4)),
            dma((2, CHUNKS, 4)),
            dma((batch, 8)),
            dma((batch, 8)),
            dma((6,)),
            dma((batch, 4)),
            dma((batch, 4)),
            dma((5 + 6 * batch,)),
            *([pltpu.VMEM(x.shape, jnp.bfloat16)] * 5),
            pltpu.VMEM(x.shape, jnp.float32),
            *(pltpu.VMEM(whole.shape, jnp.bfloat16) for whole in wholes[:5]),
        ],
        compiler_params=pltpu.CompilerParams(
            collective_id=1, has_side_effects=True, vmem_limit_bytes=60 * 2**20
        ),
        name="layer_head",
    )(*lengths, x, g, routes, routes_t, inner, outer, *parts)
    wholes, rest = results[:count], results[count:]
    return wholes, rest[:4], rest[4:8], rest[8], rest[9:16], rest[16], rest[17]


def middle_kernel(arrived_ref, *refs):
    sources, refs = refs[:8], refs[8:]
    returned_ref, outs, refs = refs[0], refs[1:5], refs[5:]
    taken, going, inner_sums, outer_sums, refs = refs[0], refs[1], refs[2:6], refs[6:10], refs[10:]
    stage, inbox, take_sem, send_sem, recv_sem, local_sem, core_send, core_recv = refs[:8]
    fetch_sem, *weights = refs[8:]
    inner_refs, outer_refs = weights[:4], weights[4:]
    fetches = [
        pltpu.make_async_copy(source, target, fetch_sem.at[index])
        for index, (source, target) in enumerate(zip(sources, weights))
    ]
    for part in fetches:
        part.start()
    y, zl, x = (lax.axis_index(axis) for axis in PEER_AXES)
    mine = y * 4 + zl * 2 + x
    batch, blocks, _, slots, width = arrived_ref.shape
    groups = blocks // 2
    total = batch * groups

    meet([across("core"), *(peer_of(step)[0] for step in range(1, 8))])
    for ref in (*inner_sums, *outer_sums):
        ref[...] = jnp.zeros_like(ref)

    def partner(i, side):
        turn = lax.rem(i, groups)
        step = turn if side == 0 else 2 * groups - 1 - turn
        places = {}
        for axis, place, flipped in (
            ("y", y, step // 4),
            ("zl", zl, lax.rem(step // 2, 2)),
            ("x", x, lax.rem(step, 2)),
        ):
            places[axis] = place + flipped - 2 * place * flipped
        return lax.div(i, groups), places, (places["y"] * 2 + places["zl"]) * 2 + places["x"]

    def take(i, side):
        b, _, block = partner(i, side)
        slot = lax.rem(i, 2)
        return pltpu.make_async_copy(
            arrived_ref.at[b, block], taken.at[slot, side], take_sem.at[slot, side]
        )

    def back(i, side, action):
        b, target, block = partner(i, side)
        slot = lax.rem(i, 2)

        def far():
            action(
                pltpu.make_async_remote_copy(
                    src_ref=going.at[slot, side],
                    dst_ref=returned_ref.at[b, mine],
                    send_sem=send_sem.at[b, block],
                    recv_sem=recv_sem.at[b, mine],
                    device_id=target,
                    device_id_type=pl.DeviceIdType.MESH,
                ),
                True,
            )

        if side:
            far()
            return
        pl.when(block != mine)(far)

        @pl.when(block == mine)
        def _():
            action(
                pltpu.make_async_copy(
                    going.at[slot, side], returned_ref.at[b, mine], local_sem.at[b]
                ),
                False,
            )

    def begin(copy, remote):
        copy.start()

    def sent(copy, remote):
        if remote:
            copy.wait_send()
        else:
            copy.wait()

    for side in range(2):
        take(0, side).start()
    for part in fetches:
        part.wait()

    def work(i, carry):
        slot = lax.rem(i, 2)

        @pl.when(i + 1 < total)
        def _():
            for side in range(2):
                take(i + 1, side).start()

        for side in range(2):
            take(i, side).wait()
        rows = taken[slot, :, 0].reshape(2 * slots, width)
        grads = taken[slot, :, 1].reshape(2 * slots, width)
        out = jnp.zeros((2 * slots, width), jnp.float32)
        result = jnp.zeros((2 * slots, width), jnp.float32)
        for part in range(4):
            inner, outer = inner_refs[part][...], outer_refs[part][...]
            pre_act = jnp.dot(rows, inner, preferred_element_type=jnp.float32)
            activated, slope = gelu_parts(pre_act)
            hidden = activated.astype(jnp.bfloat16)
            grad_pre = (nt_dot(grads, outer) * slope).astype(jnp.bfloat16)
            out = out + jnp.dot(hidden, outer, preferred_element_type=jnp.float32)
            result = result + nt_dot(grad_pre, inner)
            inner_sums[part][...] += tn_dot(rows, grad_pre)
            outer_sums[part][...] += tn_dot(hidden, grads)

        @pl.when(i >= 2)
        def _():
            for side in range(2):
                back(i - 2, side, sent)

        going[slot, :, 0] = out.astype(jnp.bfloat16).reshape(2, slots, width)
        going[slot, :, 1] = result.astype(jnp.bfloat16).reshape(2, slots, width)
        for side in range(2):
            back(i, side, begin)
        return carry

    lax.fori_loop(0, total, work, 0)
    crossing = []
    for index in range(4):
        sums = (inner_sums, outer_sums)[index % 2]
        stage[index] = sums[3 - 2 * (index // 2)][...].astype(jnp.bfloat16)
        crossing.append(
            send(
                stage.at[index],
                inbox.at[index],
                core_send.at[index],
                core_recv.at[index],
                across("core"),
            )
        )
    for index in range(4):
        sums = (inner_sums, outer_sums)[index % 2]
        crossing[index].wait()
        met = sums[2 - 2 * (index // 2)][...] + inbox[index].astype(jnp.float32)
        outs[index][...] = met.astype(jnp.bfloat16)
    for i in (total - 2, total - 1):
        for side in range(2):
            back(i, side, sent)
    for b in range(batch):
        for step in range(1, 8):
            target, block = peer_of(step)
            pltpu.make_async_remote_copy(
                src_ref=going.at[0, 0],
                dst_ref=returned_ref.at[b, block],
                send_sem=send_sem.at[b, block],
                recv_sem=recv_sem.at[b, block],
                device_id=target,
                device_id_type=pl.DeviceIdType.MESH,
            ).wait_recv()


def layer_middle(arrived, inner, outer):
    batch, sources, _, slots, width = arrived.shape
    quarter = inner[0].shape
    anywhere = pl.BlockSpec(memory_space=pl.ANY)
    dma = pltpu.SemaphoreType.DMA
    results = pl.pallas_call(
        middle_kernel,
        out_shape=(
            jax.ShapeDtypeStruct(arrived.shape, jnp.bfloat16),
            *([jax.ShapeDtypeStruct(quarter, jnp.bfloat16)] * 4),
        ),
        in_specs=[anywhere] * 9,
        out_specs=[anywhere, *([VMEM] * 4)],
        scratch_shapes=[
            pltpu.VMEM((2, 2, 2, slots, width), jnp.bfloat16),
            pltpu.VMEM((2, 2, 2, slots, width), jnp.bfloat16),
            *([pltpu.VMEM(quarter, jnp.float32)] * 8),
            pltpu.VMEM((4, *quarter), jnp.bfloat16),
            pltpu.VMEM((4, *quarter), jnp.bfloat16),
            dma((2, 2)),
            dma((batch, sources)),
            dma((batch, sources)),
            dma((batch,)),
            dma((4,)),
            dma((4,)),
            dma((8,)),
            *([pltpu.VMEM(quarter, jnp.bfloat16)] * 8),
        ],
        compiler_params=pltpu.CompilerParams(
            collective_id=3, has_side_effects=True, vmem_limit_bytes=63 * 2**20
        ),
        name="layer_middle",
    )(arrived, *inner, *outer)
    return results[0], results[1:]


def bias_columns(diagonals, shards, bucket_count):
    lines = diagonals.shape[1]
    width = lines
    row = row_iota(lines, 1)
    distance = (row // (2 * LANES)) * LANES + LANES - 1 - row % (2 * LANES)
    table = bucket_table(lines // (2 * LANES) * LANES)
    bucket = jnp.minimum(distance, 16)
    for value in range(17, bucket_count):
        bucket = bucket + (distance >= int(np.argmax(table >= value))).astype(jnp.int32)
    lane = column_iota(1, width)
    place = lane % (width // shards)
    heads = 3
    hot = one_hot((bucket == place % bucket_count) & (place < heads * bucket_count))
    sums = sum(jnp.dot(part, hot, preferred_element_type=jnp.float32) for part in split(diagonals))
    head = lane // (width // shards) * heads + place // bucket_count
    return jnp.sum(jnp.where(row_iota(sums.shape[0], width) == head, sums, 0.0), 0, keepdims=True)


FOLD_SPLIT = 4


def tail_kernel(experts, capacity, bucket_count, lengths_ref, dealing_ref, *refs):
    x_ref, g_ref, routes_ref, refs = refs[0], refs[1], refs[2], refs[3:]
    weights, gain_ref, bias_ref, refs = refs[:5], refs[5], refs[6], refs[7:]
    normed_ref, q_ref, k_ref, v_ref, mix_ref, residual_ref, gates_ref, returned_ref = refs[:8]
    partials, refs = refs[8:12], refs[12:]
    result_ref, input_grad_ref, home_refs, outs, refs = (
        refs[0],
        refs[1],
        refs[2:4],
        refs[4:12],
        refs[12:],
    )
    out_rows, back_rows, branch, dq, dk, dv, router_grad, gain_grad, diag, refs = *refs[:9], refs[9:]
    grad_mix, grad_residual, scratch, refs = refs[0], refs[1], refs[2:6], refs[6:]
    grads, sums, refs = refs[:8], refs[8:16], refs[16:]
    inboxes, refs = [refs[8 * i : 8 * i + 8] for i in range(5)], refs[40:]
    fetched, landed, fold_send, fold_recv, move_send, move_recv, local_sem, own_sem = refs[:8]
    fetch_sem, *fetch_to = refs[8:]
    fetch_from = [mix_ref, q_ref, k_ref, v_ref, normed_ref, *weights[:3]]
    mix_ref, q_ref, k_ref, v_ref, normed_ref = fetch_to[:5]
    weights = [*fetch_to[5:], *weights[3:]]
    y, zh = lax.axis_index("y"), lax.axis_index("zh")
    at_home, away = zh == y, zh != y
    batch, tokens, width = x_ref.shape
    far, near = partials[:2], partials[2:]
    rows = far[0].shape[0] // CHUNKS
    cut_at = FOLD_SPLIT * LANES

    fetches = [
        pltpu.make_async_copy(source, target, fetch_sem.at[index])
        for index, (source, target) in enumerate(zip(fetch_from, fetch_to))
    ]

    def load(b):
        return [
            pltpu.make_async_copy(returned_ref.at[b, :, which], target, local_sem.at[which])
            for which, target in enumerate((out_rows, back_rows))
        ]

    def piece(ref, chunk):
        return ref.at[pl.ds(chunk * rows, rows)]

    for part in (*load(0), *fetches):
        part.start()
    greet(("core", "y", "x", "zl", "zh"))

    def own(which, chunk):
        return pltpu.make_async_copy(
            piece(near[which], chunk),
            (out_rows, back_rows)[which].at[chunk],
            own_sem.at[which, chunk],
        )

    def copy(which, chunk, kind, source, target, axis):
        return pltpu.make_async_remote_copy(
            src_ref=piece(source, chunk),
            dst_ref=piece(target, chunk),
            send_sem=move_send.at[which, chunk, kind],
            recv_sem=move_recv.at[which, chunk, kind],
            device_id=across(axis),
            device_id_type=pl.DeviceIdType.MESH,
        )

    def move(index):
        which, chunk = index // CHUNKS, index % CHUNKS
        copy(which, chunk, 0, far[which], fetched.at[which], "y").wait_recv()

        @pl.when(at_home)
        def _():
            copy(which, chunk, 1, fetched.at[which], landed.at[which], "zh").start()

        @pl.when(away)
        def _():
            copy(which, chunk, 1, near[which], landed.at[which], "zh").start()

    order = [(which, chunk) for which in range(2) for chunk in range(CHUNKS)]
    for which, chunk in order:
        copy(which, chunk, 0, far[which], fetched.at[which], "y").start()

    def columns(ref, b, first):
        return ref.at[b, :, :cut_at] if first else ref.at[b, :, cut_at:]

    operands = [(mix_ref.at[0], branch.at[0], mix_ref.at[1], branch.at[1])]
    for first in (True, False):
        for ref in (dq, dk, dv):
            operands.append(
                (
                    normed_ref.at[0],
                    columns(ref, 0, first),
                    normed_ref.at[1],
                    columns(ref, 1, first),
                )
            )
    operands.append(None)
    fold, fold_end = folder(operands, outs, grads, sums, inboxes, fold_send, fold_recv)
    early, late, small = (1, 2, 3), (4, 5, 6), 7

    def each(b, actions):
        for index, action in enumerate(actions):
            pl.when(b == index)(action)

    def combine(b, carry):
        for part in load(b):
            part.wait()
        combine_math(
            experts,
            capacity,
            g_ref.at[b],
            routes_ref.at[b],
            weights[3],
            weights[4],
            gain_ref,
            residual_ref.at[b],
            gates_ref.at[b],
            out_rows,
            back_rows,
            result_ref.at[b],
            branch.at[b],
            router_grad.at[b],
            gain_grad.at[b],
            grad_mix.at[b],
            grad_residual.at[b],
            lambda: each(b, [lambda: move(0), lambda: move(2)]),
        )

        def first():
            for part in load(1):
                part.start()
            move(1)

        def second():
            for which, chunk in order:
                own(which, chunk).start()
            move(3)

        each(b, [first, second])
        return carry

    lax.fori_loop(0, batch, combine, 0)
    for part in fetches:
        part.wait()
    fold(0, 0)

    actions = {
        0: [(fold, 0, 1), (move, 4)],
        3: [(fold, 0, 2), (move, 5)],
        6: [(move, 6)],
        7: [*((fold, i, 0) for i in early)],
        8: [(fold, 0, 3)],
        9: [*((fold, i, 1) for i in early)],
        11: [*((fold, i, 2) for i in early), (move, 7)],
    }

    def act(moment):
        for action, *values in actions[moment]:
            action(*values)

    def attend_back(item, carry):
        pair, b = item // 2, lax.rem(item, 2)
        attend_back_math(
            pair,
            lengths_ref[dealing_ref[b]],
            q_ref.at[b],
            k_ref.at[b],
            v_ref.at[b],
            grad_mix.at[b],
            bias_ref,
            dq.at[b],
            dk.at[b],
            dv.at[b],
            diag.at[b],
            *scratch,
        )
        for moment in actions:
            pl.when(item == moment)(functools.partial(act, moment))
        return carry

    lax.fori_loop(0, batch * (width // LANES), attend_back, 0)
    for i in late:
        fold(i, 0)
    for i in early:
        fold(i, 3)

    def finish(b, carry):
        finish_math(
            x_ref.at[b],
            *weights[:3],
            gain_ref,
            dq.at[b],
            dk.at[b],
            dv.at[b],
            grad_residual.at[b],
            gain_grad.at[b],
            input_grad_ref.at[b],
        )

        @pl.when(b == 0)
        def _():
            for i in late:
                fold(i, 1)

        return carry

    lax.fori_loop(0, batch, finish, 0)
    lines = [
        jnp.concatenate(
            [
                diag[0, head // 2, head % 2, offset : offset + 1, :]
                + diag[1, head // 2, head % 2, offset : offset + 1, :]
                for offset in range(diag.shape[3])
            ],
            1,
        )
        for head in range(2 * diag.shape[1])
    ]
    lines.append(jnp.zeros((16 - len(lines), width), jnp.float32))
    bias_line = bias_columns(jnp.concatenate(lines, 0), 4, bucket_count)
    gain_lines = gain_grad[0] + gain_grad[1]
    row = row_iota(LANES, width)
    stacked = jnp.where(
        row == 0,
        gain_lines[0:1, :],
        jnp.where(row == 1, gain_lines[1:2, :], jnp.where(row == 2, bias_line, 0.0)),
    )
    packed = jnp.concatenate([router_grad[0] + router_grad[1], stacked.T], 1)
    grads[small][...] = packed.astype(jnp.bfloat16).reshape(grads[small].shape)
    fold(small, 0)
    reached = {0: 4, **dict.fromkeys(early, 4), **dict.fromkeys(late, 2), small: 1}
    for k in range(1, FOLD_STEPS):
        for i in reached:
            if reached[i] == k:
                fold(i, k)
                reached[i] += 1
    fold_end()

    for which, chunk in order:
        own(which, chunk).wait()
        copy(which, chunk, 1, near[which], landed.at[which], "zh").wait()
        copy(which, chunk, 0, far[which], fetched.at[which], "y").wait_send()
        place = pl.ds(chunk * rows, rows)

        def settle(kept):
            total = kept.astype(jnp.float32) + landed[which, place].astype(jnp.float32)
            home_refs[which][place] = total.astype(jnp.bfloat16)

        pl.when(at_home)(lambda: settle((out_rows, back_rows)[which][chunk]))
        pl.when(away)(lambda: settle(fetched[which, place]))


def layer_tail(experts, capacity, bucket_count, lengths, x, g, routes, weights, gains, bias, saved, returned, partials):
    batch, tokens, width = x.shape
    blocks = tokens // LANES
    shape, dma = jax.ShapeDtypeStruct, pltpu.SemaphoreType.DMA
    anywhere = pl.BlockSpec(memory_space=pl.ANY)
    flat = shape(x.shape, jnp.bfloat16)
    quarter = partials[0].shape
    cut_at = FOLD_SPLIT * LANES
    widths = [width, *([cut_at] * 3), *([width - cut_at] * 3), 2 * LANES]
    sizes = [(width // 16, columns) for columns in widths]
    boxes = []
    for depth in range(5):
        for i, (part, columns) in enumerate(sizes):
            done = FOLD_ORDERS[i % len(FOLD_ORDERS)][:depth]
            lead = [2] * (3 - sum(axis != "zh" for axis in done))
            boxes.append(
                pltpu.VMEM(
                    (*lead, part, columns // 2 if "zh" in done else columns), jnp.bfloat16
                )
            )
    side = returned.shape[1:2] + returned.shape[3:]
    results = pl.pallas_call(
        functools.partial(tail_kernel, experts, capacity, bucket_count),
        out_shape=(
            flat,
            flat,
            *([shape(quarter, jnp.bfloat16)] * 2),
            *(shape((2, 2, *size), jnp.bfloat16) for size in sizes),
        ),
        in_specs=[
            SMEM,
            SMEM,
            *([VMEM] * 3),
            *([anywhere] * 3),
            *([VMEM] * 4),
            *([anywhere] * 5),
            *([VMEM] * 2),
            *([anywhere] * 5),
        ],
        out_specs=[VMEM] * 12,
        scratch_shapes=[
            pltpu.VMEM(side, jnp.bfloat16),
            pltpu.VMEM(side, jnp.bfloat16),
            *([pltpu.VMEM(x.shape, jnp.bfloat16)] * 4),
            pltpu.VMEM((batch, width, LANES), jnp.float32),
            pltpu.VMEM((batch, 2, width), jnp.float32),
            pltpu.VMEM((batch, *bias.shape), jnp.float32),
            pltpu.VMEM((batch, tokens, width), jnp.bfloat16),
            pltpu.VMEM((batch, tokens, width), jnp.float32),
            pltpu.VMEM((2, blocks, LANES, LANES), jnp.float32),
            pltpu.VMEM((tokens, LANES), jnp.float32),
            pltpu.VMEM((tokens, LANES), jnp.float32),
            pltpu.VMEM((2, blocks, LANES, LANES), jnp.float32),
            *(pltpu.VMEM((2, 2, 2, 2, *size), jnp.bfloat16) for size in sizes),
            *(pltpu.VMEM((2, 2, 2, *size), jnp.bfloat16) for size in sizes),
            *boxes,
            pltpu.VMEM((2, *quarter), jnp.bfloat16),
            pltpu.VMEM((2, *quarter), jnp.bfloat16),
            dma((8, FOLD_STEPS - 1)),
            dma((8, FOLD_STEPS - 1)),
            dma((2, CHUNKS, 2)),
            dma((2, CHUNKS, 2)),
            dma((2,)),
            dma((2, CHUNKS)),
            dma((8,)),
            *([pltpu.VMEM(x.shape, jnp.bfloat16)] * 5),
            *([pltpu.VMEM(weights[0].shape, jnp.bfloat16)] * 3),
        ],
        compiler_params=pltpu.CompilerParams(
            collective_id=2, has_side_effects=True, vmem_limit_bytes=63 * 2**20
        ),
        name="layer_tail",
    )(*lengths, x, g, routes, *weights, gains, bias, *saved, returned, *partials)
    output, *rest, packed = (
        out.reshape(-1, out.shape[-1]).astype(jnp.float32) for out in results[4:]
    )
    folded = [jnp.concatenate(pair, 1) for pair in zip(rest[:3], rest[3:])]
    folded += [output, packed]
    homes = [home.astype(jnp.float32) for home in results[2:4]]
    return results[0], results[1], folded, homes


class Grouped:
    swap_axes = "expert"

    def begin(self, sizes, lengths, x, g, routes, routes_t, inner, outer, parts, bias_shape):
        lengths = jnp.take(*lengths)
        wholes = [lax.all_gather(part, "shard", axis=0, tiled=True) for part in parts]
        misc = wholes[5].reshape(-1, *parts[5].shape).astype(jnp.float32)
        gains = jnp.sum(misc[:, -2:], 0)
        bias_rows = misc[:, :-2].reshape(bias_shape)
        inner, outer = (list(lax.all_gather(part, "shard", axis=0)) for part in (inner, outer))
        arrived, saved = [], []
        for index in range(x.shape[0]):
            sent, *kept = layer_forward(
                index,
                *sizes,
                lengths[index : index + 1],
                x,
                g,
                routes[index],
                routes_t[index],
                wholes[:4],
                wholes[4],
                gains,
                bias_rows,
            )
            saved.append(kept)
            arrived.append(self.swap(sent))
        saved = [jnp.stack(pair) for pair in zip(*saved)]
        return wholes, inner, outer, arrived, saved, gains, bias_rows

    def swap(self, blocks):
        experts = lax.axis_size("expert")
        count, _, slots, width = blocks.shape
        merged = blocks.swapaxes(0, 1).reshape(2, experts, -1, width).swapaxes(0, 1)
        merged = lax.all_to_all(merged, "expert", split_axis=0, concat_axis=0, tiled=True)
        return merged.swapaxes(0, 1).reshape(2, count, slots, width).swapaxes(0, 1)

    def finish(
        self,
        sizes,
        bucket_count,
        lengths,
        x,
        g,
        routes,
        wholes,
        gains,
        bias_rows,
        saved,
        arrived,
        inner,
        outer,
        likes,
    ):
        lengths = jnp.take(*lengths)
        returned, units = [], []
        for rows in arrived:
            going, *unit_pair = expert_pass(rows, inner, outer)
            units.append(unit_pair)
            returned.append(self.swap(going))
        returned = jnp.stack(returned)
        hiddens, pres = zip(*units)
        chunks = len(inner)
        passes = weight_pass(0, chunks, chunks, arrived, pres, hiddens)
        homes = [
            lax.psum_scatter(jnp.stack(grads), "shard", scatter_dimension=0).astype(jnp.float32)
            for grads in passes
        ]
        normed, queries, key_rows, value_rows, mixture, residual, gates = saved
        results, input_grads, grads, small = [], [], [], []
        for index in range(x.shape[0]):
            result, input_grad, branch, dq, dk, dv, *rest = layer_backward(
                index,
                *sizes,
                lengths[index : index + 1],
                x,
                g,
                routes,
                wholes[:4],
                wholes[4],
                gains,
                bias_rows,
                (queries, key_rows, value_rows, residual, gates),
                returned,
            )
            results.append(result)
            input_grads.append(input_grad)
            lefts = (normed[index],) * 3 + (mixture[index],)
            grads.append([tn_dot(*pair) for pair in zip(lefts, (dq, dk, dv, branch))])
            small.append(rest)
        router_grad, gain_grad, diagonals = (sum(parts) for parts in zip(*small))
        bias_grad = jnp.dot(
            diagonals.reshape(bias_rows.shape[0] * 2, -1),
            jnp.asarray(collect_hot(x.shape[1], bucket_count)),
            precision=HIGH,
        )
        small = (router_grad[:, : sizes[0]], gain_grad[0], gain_grad[1], bias_grad)
        shares = [
            lax.psum_scatter(
                sum(pair).astype(jnp.bfloat16), "shard", scatter_dimension=0, tiled=True
            ).astype(jnp.float32)
            for pair in (*zip(*grads), *((part,) for part in small))
        ]
        return jnp.stack(results), jnp.stack(input_grads), lax.psum(shares, "expert"), homes

    def shard_index(self):
        return lax.axis_index("shard")


class Halved:
    swap_axes = ("y", "zl", "x")

    def begin(self, sizes, lengths, x, g, routes, routes_t, inner, outer, parts, bias_shape):
        misc = jnp.pad(parts[5], ((0, 32 - parts[5].shape[0]), (0, 0)))
        return layer_head(
            *sizes, lengths, x, g, routes, routes_t, inner, outer, [*parts[:5], misc], bias_shape
        )

    def shard_index(self):
        return lax.axis_index("y") * 2 + lax.axis_index("core")

    def finish(
        self,
        sizes,
        bucket_count,
        lengths,
        x,
        g,
        routes,
        wholes,
        gains,
        bias_rows,
        saved,
        arrived,
        inner,
        outer,
        likes,
    ):
        returned, partials = layer_middle(arrived, inner, outer)
        result, input_grad, folded, homes = layer_tail(
            *sizes,
            bucket_count,
            lengths,
            x,
            g,
            routes,
            wholes[:5],
            gains,
            bias_rows,
            saved,
            returned,
            partials,
        )
        *large, packed = folded
        router, gain_one, gain_two, bias = likes
        small = [
            packed[:, : router.shape[1]],
            packed[:, LANES],
            packed[:, LANES + 1],
            packed[: bias.size, LANES + 2].reshape(bias.shape),
        ]
        return result, input_grad, [*large, *small], homes


def body(
    plan,
    tokens,
    cotangent,
    lengths,
    dealing,
    routes,
    query_weight,
    key_weight,
    value_weight,
    output_weight,
    router_weight,
    first_gain,
    second_gain,
    position_bias,
    inner_weight,
    outer_weight,
):
    batch, seq_len, model_width = tokens.shape
    experts = lax.axis_size(plan.swap_axes)
    capacity = 4 * seq_len // experts
    bucket_count = position_bias.shape[1]
    shard_rows = query_weight.shape[0]
    shards = model_width // shard_rows
    small_shard = (router_weight, first_gain, second_gain, position_bias)
    lane_shard = jnp.arange(model_width) // shard_rows
    bias_shard = jnp.dot(
        position_bias.astype(jnp.float32),
        jnp.asarray(spread_hot(seq_len, bucket_count)),
        precision=HIGH,
    ).astype(jnp.bfloat16)
    gain_shard = jnp.where(
        lane_shard == plan.shard_index(),
        jnp.tile(jnp.stack([first_gain, second_gain]), (1, shards)),
        0,
    )
    parts = [
        query_weight,
        key_weight,
        value_weight,
        output_weight,
        jnp.pad(router_weight, ((0, 0), (0, LANES - experts))),
        jnp.concatenate([bias_shard, gain_shard], 0),
    ]
    heads = shards * position_bias.shape[0]
    bias_shape = (heads // 2, 2, seq_len // LANES, 2 * LANES)
    sizes = (experts, capacity)
    wholes, inner_parts, outer_parts, arrived, saved, gains, bias_rows = plan.begin(
        sizes,
        (lengths, dealing),
        tokens,
        cotangent,
        routes,
        jnp.pad(routes.swapaxes(1, 2), ((0, 0), (0, 6), (0, 0))),
        inner_weight[0],
        outer_weight[0],
        parts,
        bias_shape,
    )
    results, input_grads, large_and_small, homes = plan.finish(
        sizes,
        bucket_count,
        (lengths, dealing),
        tokens,
        cotangent,
        routes,
        wholes,
        gains,
        bias_rows,
        saved,
        arrived,
        inner_parts,
        outer_parts,
        small_shard,
    )
    return (results, input_grads, *large_and_small, homes[0][None], homes[1][None])


def solution(mesh):
    experts, shards = mesh.shape["expert"], mesh.shape["shard"]
    if (experts, shards) == (8, 4):
        plan = Halved()
        mesh = jax.sharding.Mesh(
            mesh.devices.reshape(2, 2, 2, 2, 2), ("zh", "zl", "x", "y", "core")
        )
        expert_axes, shard_axes = ("zh", "zl", "x"), ("y", "core")
    else:
        plan = Grouped()
        expert_axes, shard_axes = ("expert",), ("shard",)
    both = (*expert_axes, *shard_axes)
    rows = P(both, None, None)
    weight = P(shard_axes, None)
    in_specs = (rows, rows, P(), P(both), rows, *([weight] * 5))
    in_specs += (P(shard_axes), P(shard_axes), weight)
    in_specs += (P(expert_axes, None, shard_axes), P(expert_axes, shard_axes, None))
    out_specs = (rows, rows, *([weight] * 5), P(shard_axes), P(shard_axes), weight)
    out_specs += (P(expert_axes, None, shard_axes), P(expert_axes, shard_axes, None))
    return jax.shard_map(
        functools.partial(body, plan),
        mesh=mesh,
        in_specs=in_specs,
        out_specs=out_specs,
        check_vma=False,
    )
```

```python
import functools
import math

import jax
import jax.numpy as jnp
import numpy as np
from jax import lax
from jax.experimental import pallas as pl
from jax.experimental.pallas import tpu as pltpu
from jax.sharding import PartitionSpec as P

EPSILON = 1e-06
HIGH = lax.Precision.HIGHEST
NEGATIVE = -1000000000.0
INV_ROOT_TWO = 1.0 / math.sqrt(2.0)
INV_ROOT_TAU = 1.0 / math.sqrt(2.0 * math.pi)
LANES = 128


def bucket_table(length):
    distance = np.arange(length)
    scaled = 16 + np.floor(np.log(np.maximum(distance, 1) / 16.0) / np.log(8.0) * 16.0)
    return np.where(distance < 16, distance, np.minimum(scaled, 31)).astype(np.int32)


def gelu_parts(pre_act):
    normal_cdf = 0.5 * (1.0 + lax.erf(pre_act * INV_ROOT_TWO))
    return (
        pre_act * normal_cdf,
        normal_cdf + pre_act * jnp.exp(-0.5 * pre_act * pre_act) * INV_ROOT_TAU,
    )


def distance_table(length):
    offsets = np.arange(length // LANES)[:, None] * LANES
    return offsets, np.arange(2 * LANES)[None, :]


def spread_hot(length, bucket_count):
    offsets, lanes = distance_table(length)
    signed = np.where(lanes < LANES, lanes, lanes - 2 * LANES)
    distance = np.clip(offsets - signed, 0, length - 1).reshape(-1)
    return (bucket_table(length)[distance][None, :] == np.arange(bucket_count)[:, None]).astype(
        np.float32
    )


def collect_hot(length, bucket_count):
    offsets, lanes = distance_table(length)
    distance = (offsets + LANES - 1 - lanes).reshape(-1)
    inside = (distance >= 0) & (distance < length)
    table = bucket_table(length)[np.clip(distance, 0, length - 1)]
    return ((table[:, None] == np.arange(bucket_count)[None, :]) & inside[:, None]).astype(
        np.float32
    )


def half_mask(head):
    lane = lax.broadcasted_iota(jnp.int32, (1, LANES), 1)
    return (lane < LANES // 2) if head == 0 else (lane >= LANES // 2)


def only(value, head):
    return jnp.where(half_mask(head), value, jnp.zeros_like(value))


def nt_dot(left, right):
    return lax.dot_general(
        left, right, (((1,), (1,)), ((), ())), preferred_element_type=jnp.float32
    )


def tn_dot(left, right):
    return lax.dot_general(
        left, right, (((0,), (0,)), ((), ())), preferred_element_type=jnp.float32
    )


def toeplitz_block(row):
    spread = pltpu.roll(
        jnp.broadcast_to(row, (LANES, 2 * LANES)), 0, 1, stride=1, stride_axis=0
    )
    return spread[:, :LANES]


def fill_bias(bias_ref, table_ref, blocks):
    for head in range(2):
        for offset in range(blocks):
            table_ref[head, offset] = toeplitz_block(bias_ref[0, head, offset, :][None, :])


def masked_logits(query, keys, table_ref, head, block, length):
    width = (block + 1) * LANES
    bias = jnp.concatenate([table_ref[head, block - j] for j in range(block + 1)], 1)
    logits = nt_dot(query, keys) * ((LANES // 2) ** (-0.5)) + bias
    row = lax.broadcasted_iota(jnp.int32, (LANES, width), 0) + block * LANES
    column = lax.broadcasted_iota(jnp.int32, (LANES, width), 1)
    return jnp.where((column <= row) & (column < length), logits, NEGATIVE)


SLOTS = 192


def unit(value):
    return lax.rsqrt(jnp.mean(value * value, -1, keepdims=True) + EPSILON)


def column_iota(rows, columns):
    return lax.broadcasted_iota(jnp.int32, (rows, columns), 1)


def row_iota(rows, columns):
    return lax.broadcasted_iota(jnp.int32, (rows, columns), 0)


def row_places(routes_t_ref, experts, capacity):
    tokens = routes_t_ref.shape[1]
    padded = -(-experts // 16) * 16
    expert = row_iota(padded, tokens)
    hot = [expert == routes_t_ref[pick : pick + 1, :] for pick in range(2)]
    both = jnp.where(hot[0] | hot[1], 1.0, 0.0).astype(jnp.bfloat16)
    before = (row_iota(tokens, tokens) < column_iota(tokens, tokens)).astype(jnp.float32)
    rank = jnp.dot(both, before.astype(jnp.bfloat16), preferred_element_type=jnp.float32)
    slot = rank + (expert * capacity).astype(jnp.float32)
    return [jnp.sum(jnp.where(chosen, slot, 0.0), 0, keepdims=True) for chosen in hot]


def column_places(routes_ref, experts, capacity):
    tokens = routes_ref.shape[0]
    expert = column_iota(tokens, LANES)
    hot = [expert == routes_ref[:, pick : pick + 1] for pick in range(2)]
    both = jnp.where(hot[0] | hot[1], 1.0, 0.0).astype(jnp.bfloat16)
    before = (column_iota(tokens, tokens) < row_iota(tokens, tokens)).astype(jnp.float32)
    rank = jnp.dot(before.astype(jnp.bfloat16), both, preferred_element_type=jnp.float32)
    slot = rank + (expert * capacity).astype(jnp.float32)
    return [jnp.sum(jnp.where(chosen, slot, 0.0), 1, keepdims=True) for chosen in hot], hot


def one_hot(condition):
    return jnp.where(condition, 1.0, 0.0).astype(jnp.bfloat16)


def forward_math(
    length,
    x_ref,
    routes_ref,
    query_ref,
    key_ref,
    value_ref,
    output_ref,
    router_ref,
    gain_ref,
    bias_ref,
    tokens_ref,
    normed_ref,
    q_ref,
    k_ref,
    v_ref,
    mix_ref,
    residual_ref,
    gates_ref,
    table_ref,
):
    tokens, width = x_ref.shape
    blocks = tokens // LANES
    inputs = x_ref[...].astype(jnp.float32)
    normed = (inputs * unit(inputs) * gain_ref[0:1, :]).astype(jnp.bfloat16)
    normed_ref[...] = normed
    for weight, out in ((query_ref, q_ref), (key_ref, k_ref), (value_ref, v_ref)):
        out[...] = jnp.dot(normed, weight[...], preferred_element_type=jnp.float32).astype(
            jnp.bfloat16
        )

    def attend(pair, carry):
        lanes = pl.ds(pl.multiple_of(pair * LANES, LANES), LANES)
        fill_bias(bias_ref.at[pl.ds(pair, 1)], table_ref, blocks)
        for block in range(blocks):
            rows = pl.ds(block * LANES, LANES)
            reach = (block + 1) * LANES
            mixed = jnp.zeros((LANES, LANES), jnp.float32)
            for head in range(2):
                logits = masked_logits(
                    only(q_ref[rows, lanes], head),
                    k_ref[:reach, lanes],
                    table_ref,
                    head,
                    block,
                    length,
                )
                exponent = jnp.exp(logits - jnp.max(logits, 1, keepdims=True))
                soft = exponent / jnp.sum(exponent, 1, keepdims=True)
                mixed = mixed + jnp.dot(
                    soft.astype(jnp.bfloat16),
                    only(v_ref[:reach, lanes], head),
                    preferred_element_type=jnp.float32,
                )
            mix_ref[rows, lanes] = mixed.astype(jnp.bfloat16)
        return carry

    lax.fori_loop(0, width // LANES, attend, 0)
    residual = inputs + jnp.dot(
        mix_ref[...], output_ref[...], preferred_element_type=jnp.float32
    )
    residual_ref[...] = residual
    normed = (residual * unit(residual) * gain_ref[1:2, :]).astype(jnp.bfloat16)
    tokens_ref[...] = normed
    router = jnp.dot(normed, router_ref[...], preferred_element_type=jnp.float32)
    lane = column_iota(tokens, LANES)
    chosen = [
        jnp.sum(jnp.where(lane == routes_ref[:, pick : pick + 1], router, 0.0), 1, keepdims=True)
        for pick in range(2)
    ]
    top = jnp.maximum(chosen[0], chosen[1])
    gates = [jnp.exp(value - top) for value in chosen]
    total = gates[0] + gates[1]
    gates = [value / total for value in gates]
    gates_ref[...] = jnp.where(lane == 0, gates[0], jnp.where(lane == 1, gates[1], 0.0))


def dispatcher(experts, capacity, tokens_ref, g_ref, gates_ref, routes_t_ref):
    tokens = tokens_ref.shape[0]
    places = row_places(routes_t_ref, experts, capacity)
    grads = [
        (g_ref[...].astype(jnp.float32) * gates_ref[:, pick : pick + 1]).astype(jnp.bfloat16)
        for pick in range(2)
    ]

    def fill(index, block_ref):
        slots = block_ref.shape[1]
        slot = (row_iota(slots, tokens) + index * slots).astype(jnp.float32)
        hot = [jnp.where(slot == place, 1.0, 0.0) for place in places]
        block_ref[0] = jnp.dot(
            (hot[0] + hot[1]).astype(jnp.bfloat16),
            tokens_ref[...],
            preferred_element_type=jnp.float32,
        ).astype(jnp.bfloat16)
        block_ref[1] = (
            jnp.dot(hot[0].astype(jnp.bfloat16), grads[0], preferred_element_type=jnp.float32)
            + jnp.dot(hot[1].astype(jnp.bfloat16), grads[1], preferred_element_type=jnp.float32)
        ).astype(jnp.bfloat16)

    return fill


def forward_kernel(experts, capacity, length_ref, x_ref, g_ref, routes_ref, routes_t_ref, *refs):
    refs, (sent_ref, *outs, gates_ref, tokens_ref, table_ref) = refs[:7], refs[7:]
    forward_math(
        length_ref[0], x_ref, routes_ref, *refs, tokens_ref, *outs, gates_ref, table_ref
    )
    fill = dispatcher(experts, capacity, tokens_ref, g_ref, gates_ref, routes_t_ref)
    for index in range(sent_ref.shape[0]):
        fill(index, sent_ref.at[index])


def split(value):
    high = value.astype(jnp.bfloat16)
    return high, (value - high.astype(jnp.float32)).astype(jnp.bfloat16)


def norm_back(value, gain, grad):
    scale = unit(value)
    rows = value * scale
    grad_unit = grad * gain
    grad_gain = jnp.sum(grad * rows, 0, keepdims=True)
    mean = jnp.mean(grad_unit * rows, -1, keepdims=True)
    return scale * (grad_unit - rows * mean), grad_gain


def combine_math(
    experts,
    capacity,
    g_ref,
    routes_ref,
    output_ref,
    router_ref,
    gain_ref,
    residual_ref,
    gates_ref,
    out_rows_ref,
    back_rows_ref,
    result_ref,
    branch_ref,
    router_grad_ref,
    gain_grad_ref,
    grad_mix_ref,
    grad_residual_ref,
    tick=lambda: None,
):
    tokens, width = g_ref.shape
    grad_result = g_ref[...].astype(jnp.float32)
    residual = residual_ref[...]
    places, picks = column_places(routes_ref, experts, capacity)
    gates = [gates_ref[:, pick : pick + 1] for pick in range(2)]
    slots = out_rows_ref.shape[1]
    picked = [jnp.zeros((tokens, width), jnp.float32) for _ in range(2)]
    grad_normed = jnp.zeros((tokens, width), jnp.float32)
    for index in range(0, out_rows_ref.shape[0], 2):
        slot = (column_iota(tokens, 2 * slots) + index * slots).astype(jnp.float32)
        hot = [jnp.where(slot == place, 1.0, 0.0) for place in places]
        out_rows = out_rows_ref[index : index + 2].reshape(2 * slots, width)
        back_rows = back_rows_ref[index : index + 2].reshape(2 * slots, width)
        for pick in range(2):
            picked[pick] = picked[pick] + jnp.dot(
                hot[pick].astype(jnp.bfloat16), out_rows, preferred_element_type=jnp.float32
            )
        grad_normed = grad_normed + jnp.dot(
            (hot[0] + hot[1]).astype(jnp.bfloat16), back_rows, preferred_element_type=jnp.float32
        )
    result_ref[...] = (residual + (gates[0] * picked[0] + gates[1] * picked[1])).astype(
        jnp.bfloat16
    )
    tick()
    grad_gates = [jnp.sum(grad_result * rows, 1, keepdims=True) for rows in picked]
    common = gates[0] * grad_gates[0] + gates[1] * grad_gates[1]
    grad_router = jnp.zeros((tokens, LANES), jnp.float32)
    for pick in range(2):
        grad_router = grad_router + jnp.where(
            picks[pick], gates[pick] * (grad_gates[pick] - common), 0.0
        )
    normed = (residual * unit(residual) * gain_ref[1:2, :]).astype(jnp.bfloat16)
    router_grad = jnp.zeros((width, LANES), jnp.float32)
    for part in split(grad_router):
        grad_normed = grad_normed + nt_dot(part, router_ref[...])
        router_grad = router_grad + tn_dot(normed, part)
    router_grad_ref[...] = router_grad
    from_norm, grad_gain = norm_back(residual, gain_ref[1:2, :], grad_normed)
    gain_grad_ref[1:2, :] = grad_gain
    grad_residual = grad_result + from_norm
    grad_residual_ref[...] = grad_residual
    branch = grad_residual.astype(jnp.bfloat16)
    branch_ref[...] = branch
    grad_mix_ref[...] = nt_dot(branch, output_ref[...]).astype(jnp.bfloat16)


def attend_back_math(
    pair,
    length,
    q_ref,
    k_ref,
    v_ref,
    grad_mix_ref,
    bias_ref,
    dq_ref,
    dk_ref,
    dv_ref,
    diag_ref,
    table_ref,
    dk_sum,
    dv_sum,
    skew_ref,
):
    blocks = q_ref.shape[0] // LANES
    scale = (LANES // 2) ** (-0.5)
    upside = (row_iota(LANES, LANES) + column_iota(LANES, LANES) == LANES - 1).astype(jnp.float32)
    lanes = pl.ds(pl.multiple_of(pair * LANES, LANES), LANES)
    fill_bias(bias_ref.at[pl.ds(pair, 1)], table_ref, blocks)
    dk_sum[...] = jnp.zeros_like(dk_sum)
    dv_sum[...] = jnp.zeros_like(dv_sum)
    skew_ref[...] = jnp.zeros_like(skew_ref)
    for block in range(blocks):
        rows = pl.ds(block * LANES, LANES)
        reach = (block + 1) * LANES
        dq = jnp.zeros((LANES, LANES), jnp.float32)
        for head in range(2):
            query = only(q_ref[rows, lanes], head)
            grad = only(grad_mix_ref[rows, lanes], head)
            keys = k_ref[:reach, lanes]
            logits = masked_logits(query, keys, table_ref, head, block, length)
            exponent = jnp.exp(logits - jnp.max(logits, 1, keepdims=True))
            soft = exponent / jnp.sum(exponent, 1, keepdims=True)
            grad_soft = nt_dot(grad, v_ref[:reach, lanes])
            inner = jnp.sum(soft * grad_soft, 1, keepdims=True)
            grad_logits = (soft * (grad_soft - inner)).astype(jnp.bfloat16)
            dv_sum[:reach, :] += tn_dot(soft.astype(jnp.bfloat16), grad)
            dk_sum[:reach, :] += tn_dot(grad_logits, query)
            dq = dq + jnp.dot(
                grad_logits, only(keys, head), preferred_element_type=jnp.float32
            )
            wide = grad_logits.astype(jnp.float32)
            for j in range(block + 1):
                skew_ref[head, block - j] += wide[:, j * LANES : (j + 1) * LANES]
        dq_ref[rows, lanes] = (dq * scale).astype(jnp.bfloat16)
    dk_ref[:, lanes] = (dk_sum[...] * scale).astype(jnp.bfloat16)
    dv_ref[:, lanes] = dv_sum[...].astype(jnp.bfloat16)
    for head in range(2):
        for offset in range(blocks):
            flipped = jnp.dot(
                upside,
                skew_ref[head, offset],
                precision=HIGH,
                preferred_element_type=jnp.float32,
            )
            padded = jnp.concatenate([flipped, jnp.zeros_like(flipped)], 1)
            lined = pltpu.roll(padded, 0, 1, stride=1, stride_axis=0)
            diag_ref[pair, head, offset, :] = jnp.sum(lined, 0)


def finish_math(
    x_ref,
    query_ref,
    key_ref,
    value_ref,
    gain_ref,
    dq_ref,
    dk_ref,
    dv_ref,
    grad_residual_ref,
    gain_grad_ref,
    input_grad_ref,
):
    grad_normed = nt_dot(dq_ref[...], query_ref[...])
    grad_normed = grad_normed + nt_dot(dk_ref[...], key_ref[...])
    grad_normed = grad_normed + nt_dot(dv_ref[...], value_ref[...])
    inputs = x_ref[...].astype(jnp.float32)
    from_norm, grad_gain = norm_back(inputs, gain_ref[0:1, :], grad_normed)
    gain_grad_ref[0:1, :] = grad_gain
    input_grad_ref[...] = (grad_residual_ref[...] + from_norm).astype(jnp.bfloat16)


def backward_kernel(
    experts,
    capacity,
    length_ref,
    x_ref,
    g_ref,
    routes_ref,
    query_ref,
    key_ref,
    value_ref,
    output_ref,
    router_ref,
    gain_ref,
    bias_ref,
    q_ref,
    k_ref,
    v_ref,
    residual_ref,
    gates_ref,
    out_rows_ref,
    back_rows_ref,
    result_ref,
    input_grad_ref,
    branch_ref,
    dq_ref,
    dk_ref,
    dv_ref,
    router_grad_ref,
    gain_grad_ref,
    diag_ref,
    grad_mix_ref,
    grad_residual_ref,
    *scratch,
):
    combine_math(
        experts,
        capacity,
        g_ref,
        routes_ref,
        output_ref,
        router_ref,
        gain_ref,
        residual_ref,
        gates_ref,
        out_rows_ref,
        back_rows_ref,
        result_ref,
        branch_ref,
        router_grad_ref,
        gain_grad_ref,
        grad_mix_ref,
        grad_residual_ref,
    )

    def attend_back(pair, carry):
        attend_back_math(
            pair,
            length_ref[0],
            q_ref,
            k_ref,
            v_ref,
            grad_mix_ref,
            bias_ref,
            dq_ref,
            dk_ref,
            dv_ref,
            diag_ref,
            *scratch,
        )
        return carry

    lax.fori_loop(0, x_ref.shape[1] // LANES, attend_back, 0)
    finish_math(
        x_ref,
        query_ref,
        key_ref,
        value_ref,
        gain_ref,
        dq_ref,
        dk_ref,
        dv_ref,
        grad_residual_ref,
        gain_grad_ref,
        input_grad_ref,
    )


VMEM = pl.BlockSpec(memory_space=pltpu.VMEM)
SMEM = pl.BlockSpec(memory_space=pltpu.SMEM)


def layer_forward(index, experts, capacity, length, x, g, routes, routes_t, weights, router, gains, bias):
    _, tokens, width = x.shape
    blocks = tokens // LANES
    flat = jax.ShapeDtypeStruct((tokens, width), jnp.bfloat16)
    rows = pl.BlockSpec((None, tokens, width), lambda i: (index, 0, 0))
    return pl.pallas_call(
        functools.partial(forward_kernel, experts, capacity),
        grid=(1,),
        out_shape=(
            jax.ShapeDtypeStruct((experts * capacity // SLOTS, 2, SLOTS, width), jnp.bfloat16),
            flat,
            flat,
            flat,
            flat,
            flat,
            jax.ShapeDtypeStruct((tokens, width), jnp.float32),
            jax.ShapeDtypeStruct((tokens, LANES), jnp.float32),
        ),
        in_specs=[SMEM, rows, rows, *([VMEM] * 9)],
        out_specs=[VMEM] * 8,
        scratch_shapes=[
            pltpu.VMEM((tokens, width), jnp.bfloat16),
            pltpu.VMEM((2, blocks, LANES, LANES), jnp.float32),
        ],
        compiler_params=pltpu.CompilerParams(vmem_limit_bytes=56 * 2**20),
        cost_estimate=pl.CostEstimate(
            flops=2 * tokens * width * (4 * width + 4 * tokens + 6 * tokens),
            bytes_accessed=40 * tokens * width,
            transcendentals=tokens * tokens * 12,
        ),
        name="layer_forward",
    )(length, x, g, routes, routes_t, *weights, router, gains, bias)


def layer_backward(
    index, experts, capacity, length, x, g, routes, weights, router, gains, bias, saved, returned
):
    _, tokens, width = x.shape
    blocks = tokens // LANES
    flat = jax.ShapeDtypeStruct((tokens, width), jnp.bfloat16)
    _, count, _, slots, _ = returned.shape

    def one(array):
        return pl.BlockSpec((None, *array.shape[1:]), lambda i: (index, 0, 0))

    rows = one(x)

    def side(which):
        return pl.BlockSpec(
            (None, count, None, slots, width), lambda i: (index, 0, which, 0, 0)
        )

    return pl.pallas_call(
        functools.partial(backward_kernel, experts, capacity),
        grid=(1,),
        out_shape=(
            *([flat] * 6),
            jax.ShapeDtypeStruct((width, LANES), jnp.float32),
            jax.ShapeDtypeStruct((2, width), jnp.float32),
            jax.ShapeDtypeStruct(bias.shape, jnp.float32),
        ),
        in_specs=[
            SMEM,
            rows,
            rows,
            one(routes),
            *([VMEM] * 7),
            *map(one, saved),
            side(0),
            side(1),
        ],
        out_specs=[VMEM] * 9,
        scratch_shapes=[
            pltpu.VMEM((tokens, width), jnp.bfloat16),
            pltpu.VMEM((tokens, width), jnp.float32),
            pltpu.VMEM((2, blocks, LANES, LANES), jnp.float32),
            pltpu.VMEM((tokens, LANES), jnp.float32),
            pltpu.VMEM((tokens, LANES), jnp.float32),
            pltpu.VMEM((2, blocks, LANES, LANES), jnp.float32),
        ],
        compiler_params=pltpu.CompilerParams(vmem_limit_bytes=56 * 2**20),
        cost_estimate=pl.CostEstimate(
            flops=2 * tokens * width * (4 * width + 12 * tokens + 10 * tokens),
            bytes_accessed=40 * tokens * width,
            transcendentals=tokens * tokens * 12,
        ),
        name="layer_backward",
    )(length, x, g, routes, *weights, router, gains, bias, *saved, returned, returned)


def expert_kernel(count, x_ref, g_ref, *refs):
    inner_refs, outer_refs = refs[:count], refs[count : 2 * count]
    back_ref, hidden_ref, grad_ref = refs[2 * count :]
    shape = x_ref.shape
    inputs = x_ref[...].reshape(-1, shape[-1])
    grads = g_ref[...].reshape(-1, shape[-1])
    out = jnp.zeros(inputs.shape, jnp.float32)
    back = jnp.zeros(inputs.shape, jnp.float32)
    start = 0
    for inner_ref, outer_ref in zip(inner_refs, outer_refs):
        part = pl.ds(start, inner_ref.shape[1])
        start += inner_ref.shape[1]
        pre_act = jnp.dot(inputs, inner_ref[...], preferred_element_type=jnp.float32)
        activated, slope = gelu_parts(pre_act)
        hidden = activated.astype(jnp.bfloat16)
        grad_pre = (nt_dot(grads, outer_ref[...]) * slope).astype(jnp.bfloat16)
        hidden_ref[:, part] = hidden
        grad_ref[:, part] = grad_pre
        out = out + jnp.dot(hidden, outer_ref[...], preferred_element_type=jnp.float32)
        back = back + nt_dot(grad_pre, inner_ref[...])
    back_ref[:, 0] = out.astype(jnp.bfloat16).reshape(shape)
    back_ref[:, 1] = back.astype(jnp.bfloat16).reshape(shape)


def expert_pass(arrived, inner, outer):
    sources, _, capacity, width = arrived.shape
    total = sources * capacity
    units = sum(part.shape[1] for part in inner)
    group = sources // 4

    def side(which):
        return pl.BlockSpec((group, None, capacity, width), lambda i: (i, which, 0, 0))

    def whole(shape):
        return pl.BlockSpec(shape, lambda i: (0, 0), pipeline_mode=pl.Buffered(1))

    unit_spec = pl.BlockSpec((group * capacity, units), lambda i: (i, 0))
    deep = jax.ShapeDtypeStruct((total, units), jnp.bfloat16)
    return pl.pallas_call(
        functools.partial(expert_kernel, len(inner)),
        grid=(sources // group,),
        out_shape=(jax.ShapeDtypeStruct(arrived.shape, jnp.bfloat16), deep, deep),
        in_specs=[side(0), side(1), *(whole(part.shape) for part in (*inner, *outer))],
        out_specs=(
            pl.BlockSpec((group, 2, capacity, width), lambda i: (i, 0, 0, 0)),
            unit_spec,
            unit_spec,
        ),
        compiler_params=pltpu.CompilerParams(vmem_limit_bytes=60 * 2**20),
        cost_estimate=pl.CostEstimate(
            flops=8 * total * width * units,
            bytes_accessed=4 * (2 * width + units) * total + 4 * width * units,
            transcendentals=2 * total * units,
        ),
        name="expert_pass",
    )(arrived, arrived, *inner, *outer)


def weight_kernel(x0_ref, x1_ref, g0_ref, g1_ref, p0_ref, p1_ref, h0_ref, h1_ref, *out_refs):
    inner_ref, outer_ref = out_refs

    def flat(ref):
        return ref[...].reshape(-1, ref.shape[-1])

    inner = tn_dot(flat(x0_ref), p0_ref[...]) + tn_dot(flat(x1_ref), p1_ref[...])
    inner_ref[...] = inner.astype(jnp.bfloat16)
    outer = tn_dot(h0_ref[...], flat(g0_ref)) + tn_dot(h1_ref[...], flat(g1_ref))
    outer_ref[...] = outer.astype(jnp.bfloat16)


def weight_pass(first, count, chunks, arrived, pres, hiddens):
    sources, _, capacity, width = arrived[0].shape
    total = sources * capacity
    size = hiddens[0].shape[1] // chunks
    step = math.gcd(size, 256)
    steps = size // step

    def side(which):
        return pl.BlockSpec(
            (sources, None, capacity, width),
            lambda i: (0, which, 0, 0),
            pipeline_mode=pl.Buffered(1),
        )

    units = pl.BlockSpec((total, step), lambda i: (0, first * steps + i))
    inner, outer = pl.pallas_call(
        weight_kernel,
        grid=(count * steps,),
        out_shape=(
            jax.ShapeDtypeStruct((count, width, size), jnp.bfloat16),
            jax.ShapeDtypeStruct((count * size, width), jnp.bfloat16),
        ),
        in_specs=[side(0)] * 2 + [side(1)] * 2 + [units] * 4,
        out_specs=(
            pl.BlockSpec((None, width, step), lambda i: (i // steps, 0, i % steps)),
            pl.BlockSpec((step, width), lambda i: (i, 0)),
        ),
        compiler_params=pltpu.CompilerParams(vmem_limit_bytes=60 * 2**20),
        cost_estimate=pl.CostEstimate(
            flops=8 * total * width * count * size,
            bytes_accessed=8 * total * (width + count * size) + 4 * width * count * size,
            transcendentals=0,
        ),
        name="weight_pass",
    )(*arrived, *arrived, *pres, *hiddens)
    return list(inner), list(outer.reshape(count, size, width))


FOLD_ORDERS = (("x", "y", "zl", "zh"), ("y", "x", "zl", "zh"))
FOLD_STEPS = 9


def greet(axes):
    barrier = pltpu.get_barrier_semaphore()
    for axis in axes:
        pl.semaphore_signal(
            barrier,
            inc=1,
            device_id={axis: 1 - lax.axis_index(axis)},
            device_id_type=pl.DeviceIdType.MESH,
        )
    pl.semaphore_wait(barrier, len(axes))


def push(source, target, send_sem, recv_sem, axis):
    copy = pltpu.make_async_remote_copy(
        src_ref=source,
        dst_ref=target,
        send_sem=send_sem,
        recv_sem=recv_sem,
        device_id={axis: 1 - lax.axis_index(axis)},
        device_id_type=pl.DeviceIdType.MESH,
    )
    copy.start()
    return copy


def folder(operands, outs, grads, sums, inboxes, send_sem, recv_sem):
    count = len(outs)
    mine = {axis: lax.axis_index(axis) for axis in ("core", "y", "x", "zl", "zh")}
    core = mine["core"]
    orders = [FOLD_ORDERS[i % len(FOLD_ORDERS)] for i in range(count)]
    spread, joined = ("y", "x", "zl"), ("x", "zl")

    def cut(ref, i, depth, axes, partner=None):
        done = orders[i][:depth]
        place = dict(mine)
        if partner is not None:
            place[partner] = 1 - place[partner]
        index = [place[axis] if axis in done else slice(None) for axis in axes]
        columns = slice(None)
        if "zh" in done:
            width = ref.shape[-1] // 2
            columns = pl.ds(pl.multiple_of(place["zh"] * width, LANES), width)
        return ref.at[(*index, slice(None), columns)]

    def copy(i, k):
        if k == 0:
            source, target, axis = grads[i].at[:, 1 - core], inboxes[0][i], "core"
        elif k < 5:
            axis = orders[i][k - 1]
            source, target = cut(sums[i], i, k, spread, axis), inboxes[k][i]
        else:
            axis = [axis for axis in reversed(orders[i]) if axis != "y"][k - 5]
            source = target = cut(outs[i], i, orders[i].index(axis) + 1, joined)
        return pltpu.make_async_remote_copy(
            src_ref=source,
            dst_ref=target,
            send_sem=send_sem.at[i, k],
            recv_sem=recv_sem.at[i, k],
            device_id={axis: 1 - mine[axis]},
            device_id_type=pl.DeviceIdType.MESH,
        )

    def step(i, k):
        if k == 0:
            if operands[i] is not None:
                left_0, right_0, left_1, right_1 = operands[i]
                total = tn_dot(left_0[...], right_0[...]) + tn_dot(left_1[...], right_1[...])
                grads[i][...] = total.astype(jnp.bfloat16).reshape(grads[i].shape)
            copy(i, 0).start()
            return
        copy(i, k - 1).wait_recv()
        if k == 1:
            total = grads[i][:, core].astype(jnp.float32) + inboxes[0][i][...].astype(jnp.float32)
            sums[i][...] = total.astype(jnp.bfloat16)
        elif k < 6:
            kept = cut(sums[i], i, k - 1, spread)
            total = kept[...].astype(jnp.float32) + inboxes[k - 1][i][...].astype(jnp.float32)
            target = kept if k < 5 else cut(outs[i], i, 4, joined)
            target[...] = total.astype(jnp.bfloat16)
        if k < FOLD_STEPS - 1:
            copy(i, k).start()

    def finish():
        for i in range(count):
            for k in range(FOLD_STEPS - 1):
                copy(i, k).wait_send()

    return step, finish


PEER_AXES = ("y", "zl", "x")
PEER_BITS = {"x": 1, "zl": 2, "y": 4}
DENSE_AXES = ("zl", "y")
CHUNKS = 4


def peer_of(step):
    target, block = {}, 0
    for bit, axis in enumerate(reversed(PEER_AXES)):
        place = lax.axis_index(axis)
        if step >> bit & 1:
            place = 1 - place
            target[axis] = place
        block = block + place * (1 << bit)
    return target, block


def send_later(source, target, send_sem, recv_sem, device):
    return pltpu.make_async_remote_copy(
        src_ref=source,
        dst_ref=target,
        send_sem=send_sem,
        recv_sem=recv_sem,
        device_id=device,
        device_id_type=pl.DeviceIdType.MESH,
    )


def send(*values):
    copy = send_later(*values)
    copy.start()
    return copy


def meet(devices):
    barrier = pltpu.get_barrier_semaphore()
    for device in devices:
        pl.semaphore_signal(
            barrier, inc=1, device_id=device, device_id_type=pl.DeviceIdType.MESH
        )
    pl.semaphore_wait(barrier, len(devices))


def across(axis):
    return {axis: 1 - lax.axis_index(axis)}


def head_kernel(
    experts,
    capacity,
    lengths_ref,
    dealing_ref,
    x_ref,
    g_ref,
    routes_ref,
    routes_t_ref,
    inner_ref,
    outer_ref,
    *refs,
):
    count = 6
    parts, refs = refs[:count], refs[count:]
    wholes, refs = refs[:count], refs[count:]
    inner_outs, outer_outs, refs = refs[:4], refs[4:8], refs[8:]
    arrived_ref, refs = refs[0], refs[1:]
    targets, gates_ref, gain_ref, bias_ref, refs = refs[:6], *refs[6:9], refs[9:]
    sent_refs, token_refs, token_boxes, g_boxes, gate_boxes, route_boxes = refs[:6]
    relays, table_ref, refs = refs[6:8], refs[8], refs[9:]
    mixer_send, mixer_recv, move_send, move_recv, row_send, row_recv, local_sem = refs[:7]
    share_send, share_recv, keep_sem, gate_lines, *kept = refs[7:]
    normed_ref, q_ref, k_ref, v_ref, mix_ref, residual_ref = kept[:6]
    whole_targets, wholes = wholes[:5], [*kept[6:], wholes[5]]
    core, y, x, zh = (lax.axis_index(axis) for axis in ("core", "y", "x", "zh"))
    at_home = zh == y
    away = zh != y
    batch, tokens, width = x_ref.shape

    meet([across("core"), across("zh"), *(peer_of(step)[0] for step in range(1, 8))])

    sources = (inner_ref, outer_ref)
    outs = (inner_outs, outer_outs)
    rows = inner_ref.shape[0] // CHUNKS

    def piece(ref, chunk):
        return ref.at[pl.ds(chunk * rows, rows)]

    class Moves:
        @staticmethod
        def copy(which, chunk, kind, source, target, axis):
            return pltpu.make_async_remote_copy(
                src_ref=piece(source, chunk),
                dst_ref=piece(target, chunk),
                send_sem=move_send.at[which, chunk, kind],
                recv_sem=move_recv.at[which, chunk, kind],
                device_id=across(axis),
                device_id_type=pl.DeviceIdType.MESH,
            )

    def move_z(which, chunk):
        source = sources[which]

        @pl.when(at_home)
        def _():
            Moves.copy(which, chunk, 0, source, outs[which][0], "zh").start()

        @pl.when(away)
        def _():
            Moves.copy(which, chunk, 0, source, relays[which], "zh").start()

    def move_first(which, chunk):
        source = sources[which]

        @pl.when(away)
        def _():
            Moves.copy(which, chunk, 1, source, outs[which][2], "y").start()

        @pl.when(at_home)
        def _():
            Moves.copy(which, chunk, 2, source, outs[which][1], "core").start()

    def relay_z(which, chunk):
        @pl.when(at_home)
        def _():
            Moves.copy(which, chunk, 0, sources[which], relays[which], "zh").wait_recv()
            Moves.copy(which, chunk, 1, relays[which], outs[which][2], "y").start()

        @pl.when(away)
        def _():
            Moves.copy(which, chunk, 0, sources[which], outs[which][0], "zh").wait_recv()
            Moves.copy(which, chunk, 2, outs[which][0], outs[which][1], "core").start()

    def relay_y(which, chunk):
        Moves.copy(which, chunk, 1, sources[which], outs[which][2], "y").wait_recv()
        Moves.copy(which, chunk, 3, outs[which][2], outs[which][3], "core").start()

    def finish(which, chunk):
        for kind, axis in ((2, "core"), (3, "core")):
            Moves.copy(which, chunk, kind, sources[which], outs[which][1], axis).wait_recv()
        for kind, axis in ((0, "zh"), (1, "y"), (2, "core"), (3, "core")):
            Moves.copy(which, chunk, kind, sources[which], outs[which][1], axis).wait_send()

    def half(part, which):
        size = part.shape[0] // 2
        return pl.ds(pl.multiple_of(which * size, size), size)

    def spot(part, whole, y_at, core_at, half_at=None):
        size = part.shape[0]
        start = (y_at * 2 + core_at) * size
        if half_at is not None:
            size = size // 2
            start = start + half_at * size
        return whole.at[pl.ds(pl.multiple_of(start, size), size)]

    def share(b, kind):
        source = (g_ref, routes_t_ref, token_refs, gate_lines)[kind]
        box = (g_boxes, route_boxes, token_boxes, gate_boxes)[kind]
        return send_later(
            source.at[b],
            box.at[b],
            share_send.at[b, kind],
            share_recv.at[b, kind],
            across(DENSE_AXES[b]),
        )

    mixers = []
    for i, (part, whole) in enumerate(zip(parts, wholes)):
        for j, axis in enumerate(("y", "core")):
            source = part if axis == "core" else part.at[half(part, x)]
            place = spot(part, whole, y, core, x if axis == "y" else None)
            mixers.append(push(source, place, mixer_send.at[i, j], mixer_recv.at[i, j], axis))
    for chunk in range(CHUNKS):
        move_z(0, chunk)
    for b in range(batch):
        share(b, 0).start()
        share(b, 1).start()
    for i, (part, whole) in enumerate(zip(parts, wholes)):
        spot(part, whole, y, core)[...] = part[...]
    for i, whole in enumerate(wholes):
        mixers[2 * i].wait_recv()
        place = spot(parts[i], whole, 1 - y, core, x)
        for j, axis in ((2, "x"), (3, "core")):
            mixers.append(push(place, place, mixer_send.at[i, j], mixer_recv.at[i, j], axis))
    for i, whole in enumerate(wholes):
        mixers[2 * count + 2 * i].wait_recv()
        place = spot(parts[i], whole, 1 - y, core, 1 - x)
        mixers.append(push(place, place, mixer_send.at[i, 4], mixer_recv.at[i, 4], "core"))
    for chunk in range(CHUNKS):
        move_first(0, chunk)

    @pl.when(at_home)
    def _():
        for which in range(2):
            pltpu.make_async_copy(sources[which], outs[which][0], local_sem.at[which]).start()

    for i in range(count):
        mixers[2 * i + 1].wait_recv()
        mixers[2 * count + 2 * i + 1].wait_recv()
        mixers[4 * count + i].wait_recv()

    misc = wholes[5][...].astype(jnp.float32)
    per_shard = misc.shape[0] // 4
    for i in range(2):
        line = sum(misc[s * per_shard + 3 + i : s * per_shard + 4 + i, :] for s in range(4))
        gain_ref[i : i + 1, :] = line
    for head in range(4 * 3):
        row = (head // 3) * per_shard + head % 3
        for offset in range(bias_ref.shape[2]):
            bias_ref[head // 2, head % 2, offset : offset + 1, :] = misc[
                row : row + 1, offset * 2 * LANES : (offset + 1) * 2 * LANES
            ]

    keeps = [
        pltpu.make_async_copy(source, target, keep_sem.at[index])
        for index, (source, target) in enumerate(zip(wholes, whole_targets))
    ]
    for part in keeps:
        part.start()

    def keep(b):
        return [
            pltpu.make_async_copy(source.at[b], target.at[b], keep_sem.at[5 + 6 * b + index])
            for index, (source, target) in enumerate(zip(kept, targets))
        ]

    def forward(b, carry):
        forward_math(
            lengths_ref[dealing_ref[b]],
            x_ref.at[b],
            routes_ref.at[b],
            *wholes[:5],
            gain_ref,
            bias_ref,
            token_refs.at[b],
            normed_ref.at[b],
            q_ref.at[b],
            k_ref.at[b],
            v_ref.at[b],
            mix_ref.at[b],
            residual_ref.at[b],
            gates_ref.at[b],
            table_ref,
        )
        gate_lines[b] = gates_ref[b].T[: gate_lines.shape[1]]
        for part in keep(b):
            part.start()

        @pl.when(b == 0)
        def _():
            for kind in (2, 3):
                share(0, kind).start()
            for chunk in range(CHUNKS):
                move_z(1, chunk)
            dispatch(0, 0)

        @pl.when(b == 1)
        def _():
            for kind in (2, 3):
                share(1, kind).start()

        return carry

    def steps_of(b):
        bit = PEER_BITS[DENSE_AXES[b]]
        return [step for step in (7, 5, 6, 3, 4, 1, 2, 0) if not step & bit]

    def row_copy(b, relayed, turn):
        _, source = peer_of(PEER_BITS[DENSE_AXES[b]] if relayed else 0)
        step = steps_of(b)[turn]
        place = sent_refs.at[b, 4 * relayed + turn]
        if step:
            return send_later(
                place,
                arrived_ref.at[b, source],
                row_send.at[b, 4 * relayed + turn],
                row_recv.at[b, source],
                peer_of(step)[0],
            )
        return pltpu.make_async_copy(
            place, arrived_ref.at[b, source], local_sem.at[2 + 2 * b + relayed]
        )

    def dispatch(b, relayed):
        if relayed:
            for kind in range(4):
                share(b, kind).wait_recv()
            fill = dispatcher(
                experts,
                capacity,
                token_boxes.at[b],
                g_boxes.at[b],
                jnp.concatenate([gate_boxes[b], jnp.zeros((LANES - 8, tokens), jnp.float32)], 0).T,
                route_boxes.at[b],
            )
        else:
            fill = dispatcher(
                experts,
                capacity,
                token_refs.at[b],
                g_ref.at[b],
                gates_ref.at[b],
                routes_t_ref.at[b],
            )
        for turn, step in enumerate(steps_of(b)):
            fill(peer_of(step)[1], sent_refs.at[b, 4 * relayed + turn])
            row_copy(b, relayed, turn).start()

    lax.fori_loop(0, batch, forward, 0)
    for chunk in range(CHUNKS):
        relay_z(0, chunk)
    dispatch(0, 1)
    dispatch(1, 0)
    for chunk in range(CHUNKS):
        move_first(1, chunk)
    dispatch(1, 1)
    for chunk in range(CHUNKS):
        relay_y(0, chunk)
    for chunk in range(CHUNKS):
        relay_z(1, chunk)
    for chunk in range(CHUNKS):
        relay_y(1, chunk)
    for which in range(2):
        for chunk in range(CHUNKS):
            finish(which, chunk)

    @pl.when(at_home)
    def _():
        for which in range(2):
            pltpu.make_async_copy(sources[which], outs[which][0], local_sem.at[which]).wait()

    for part in (*keeps, *keep(0), *keep(1)):
        part.wait()
    for copy in mixers:
        copy.wait_send()
    for b in range(batch):
        for relayed in range(2):
            for turn, step in enumerate(steps_of(b)):
                if step:
                    row_copy(b, relayed, turn).wait_send()
                else:
                    row_copy(b, relayed, turn).wait()
        for kind in range(4):
            share(b, kind).wait_send()
        bit = PEER_BITS[DENSE_AXES[b]]
        for step in range(8):
            if step & ~bit:
                target, block = peer_of(step)
                pltpu.make_async_remote_copy(
                    src_ref=sent_refs.at[b, 0],
                    dst_ref=arrived_ref.at[b, block],
                    send_sem=row_send.at[b, 0],
                    recv_sem=row_recv.at[b, block],
                    device_id=target,
                    device_id_type=pl.DeviceIdType.MESH,
                ).wait_recv()


def layer_head(experts, capacity, lengths, x, g, routes, routes_t, inner, outer, parts, bias_shape):
    batch, tokens, width = x.shape
    blocks = tokens // LANES
    count = len(parts)
    shape = jax.ShapeDtypeStruct
    wholes = [shape((4 * part.shape[0], part.shape[1]), part.dtype) for part in parts]
    moved = shape(inner.shape, inner.dtype)
    exchange = (experts * capacity // SLOTS, 2, SLOTS, width)
    flat = shape(x.shape, jnp.bfloat16)
    anywhere = pl.BlockSpec(memory_space=pl.ANY)
    dma = pltpu.SemaphoreType.DMA
    results = pl.pallas_call(
        functools.partial(head_kernel, experts, capacity),
        out_shape=(
            *wholes,
            *([moved] * 8),
            shape((batch, *exchange), jnp.bfloat16),
            *([flat] * 5),
            shape(x.shape, jnp.float32),
            shape((batch, tokens, LANES), jnp.float32),
            shape((2, width), jnp.float32),
            shape(bias_shape, jnp.float32),
        ),
        in_specs=[SMEM, SMEM, *([VMEM] * (6 + count))],
        out_specs=[*([anywhere] * 5), VMEM, *([anywhere] * 9), *([anywhere] * 6), *([VMEM] * 3)],
        scratch_shapes=[
            pltpu.VMEM((batch, *exchange), jnp.bfloat16),
            *([pltpu.VMEM(x.shape, jnp.bfloat16)] * 3),
            pltpu.VMEM((batch, 8, tokens), jnp.float32),
            pltpu.VMEM(routes_t.shape, jnp.int32),
            pltpu.VMEM(inner.shape, jnp.bfloat16),
            pltpu.VMEM(outer.shape, jnp.bfloat16),
            pltpu.VMEM((2, blocks, LANES, LANES), jnp.float32),
            dma((count, 5)),
            dma((count, 5)),
            dma((2, CHUNKS, 4)),
            dma((2, CHUNKS, 4)),
            dma((batch, 8)),
            dma((batch, 8)),
            dma((6,)),
            dma((batch, 4)),
            dma((batch, 4)),
            dma((5 + 6 * batch,)),
            pltpu.VMEM((batch, 8, tokens), jnp.float32),
            *([pltpu.VMEM(x.shape, jnp.bfloat16)] * 5),
            pltpu.VMEM(x.shape, jnp.float32),
            *(pltpu.VMEM(whole.shape, jnp.bfloat16) for whole in wholes[:5]),
        ],
        compiler_params=pltpu.CompilerParams(
            collective_id=1, has_side_effects=True, vmem_limit_bytes=60 * 2**20
        ),
        name="layer_head",
    )(*lengths, x, g, routes, routes_t, inner, outer, *parts)
    wholes, rest = results[:count], results[count:]
    return wholes, rest[:4], rest[4:8], rest[8], rest[9:16], rest[16], rest[17]


def middle_kernel(arrived_ref, *refs):
    sources, refs = refs[:8], refs[8:]
    returned_ref, outs, refs = refs[0], refs[1:5], refs[5:]
    taken, going, inner_sums, outer_sums, refs = refs[0], refs[1], refs[2:6], refs[6:10], refs[10:]
    stage, inbox, take_sem, send_sem, recv_sem, local_sem, core_send, core_recv = refs[:8]
    fetch_sem, *weights = refs[8:]
    inner_refs, outer_refs = weights[:4], weights[4:]
    fetches = [
        pltpu.make_async_copy(source, target, fetch_sem.at[index])
        for index, (source, target) in enumerate(zip(sources, weights))
    ]
    for part in fetches:
        part.start()
    y, zl, x = (lax.axis_index(axis) for axis in PEER_AXES)
    mine = y * 4 + zl * 2 + x
    batch, blocks, _, slots, width = arrived_ref.shape
    groups = blocks // 2
    total = batch * groups

    meet([across("core"), *(peer_of(step)[0] for step in range(1, 8))])
    for ref in (*inner_sums, *outer_sums):
        ref[...] = jnp.zeros_like(ref)

    def partner(i, side):
        turn = lax.rem(i, groups)
        step = turn if side == 0 else 2 * groups - 1 - turn
        places = {}
        for axis, place, flipped in (
            ("y", y, step // 4),
            ("zl", zl, lax.rem(step // 2, 2)),
            ("x", x, lax.rem(step, 2)),
        ):
            places[axis] = place + flipped - 2 * place * flipped
        return lax.div(i, groups), places, (places["y"] * 2 + places["zl"]) * 2 + places["x"]

    def take(i, side):
        b, _, block = partner(i, side)
        slot = lax.rem(i, 2)
        return pltpu.make_async_copy(
            arrived_ref.at[b, block], taken.at[slot, side], take_sem.at[slot, side]
        )

    def back(i, side, action):
        b, target, block = partner(i, side)
        slot = lax.rem(i, 2)

        def far():
            action(
                pltpu.make_async_remote_copy(
                    src_ref=going.at[slot, side],
                    dst_ref=returned_ref.at[b, mine],
                    send_sem=send_sem.at[b, block],
                    recv_sem=recv_sem.at[b, mine],
                    device_id=target,
                    device_id_type=pl.DeviceIdType.MESH,
                ),
                True,
            )

        if side:
            far()
            return
        pl.when(block != mine)(far)

        @pl.when(block == mine)
        def _():
            action(
                pltpu.make_async_copy(
                    going.at[slot, side], returned_ref.at[b, mine], local_sem.at[b]
                ),
                False,
            )

    def begin(copy, remote):
        copy.start()

    def sent(copy, remote):
        if remote:
            copy.wait_send()
        else:
            copy.wait()

    for side in range(2):
        take(0, side).start()
    for part in fetches:
        part.wait()

    def work(i, carry):
        slot = lax.rem(i, 2)

        @pl.when(i + 1 < total)
        def _():
            for side in range(2):
                take(i + 1, side).start()

        for side in range(2):
            take(i, side).wait()
        rows = taken[slot, :, 0].reshape(2 * slots, width)
        grads = taken[slot, :, 1].reshape(2 * slots, width)
        out = jnp.zeros((2 * slots, width), jnp.float32)
        result = jnp.zeros((2 * slots, width), jnp.float32)
        for part in range(4):
            inner, outer = inner_refs[part][...], outer_refs[part][...]
            pre_act = jnp.dot(rows, inner, preferred_element_type=jnp.float32)
            activated, slope = gelu_parts(pre_act)
            hidden = activated.astype(jnp.bfloat16)
            grad_pre = (nt_dot(grads, outer) * slope).astype(jnp.bfloat16)
            out = out + jnp.dot(hidden, outer, preferred_element_type=jnp.float32)
            result = result + nt_dot(grad_pre, inner)
            inner_sums[part][...] += tn_dot(rows, grad_pre)
            outer_sums[part][...] += tn_dot(hidden, grads)

        @pl.when(i >= 2)
        def _():
            for side in range(2):
                back(i - 2, side, sent)

        going[slot, :, 0] = out.astype(jnp.bfloat16).reshape(2, slots, width)
        going[slot, :, 1] = result.astype(jnp.bfloat16).reshape(2, slots, width)
        for side in range(2):
            back(i, side, begin)
        return carry

    lax.fori_loop(0, total, work, 0)
    crossing = []
    for index in range(4):
        sums = (inner_sums, outer_sums)[index % 2]
        stage[index] = sums[3 - 2 * (index // 2)][...].astype(jnp.bfloat16)
        crossing.append(
            send(
                stage.at[index],
                inbox.at[index],
                core_send.at[index],
                core_recv.at[index],
                across("core"),
            )
        )
    for index in range(4):
        sums = (inner_sums, outer_sums)[index % 2]
        crossing[index].wait()
        met = sums[2 - 2 * (index // 2)][...] + inbox[index].astype(jnp.float32)
        outs[index][...] = met.astype(jnp.bfloat16)
    for i in (total - 2, total - 1):
        for side in range(2):
            back(i, side, sent)
    for b in range(batch):
        for step in range(1, 8):
            target, block = peer_of(step)
            pltpu.make_async_remote_copy(
                src_ref=going.at[0, 0],
                dst_ref=returned_ref.at[b, block],
                send_sem=send_sem.at[b, block],
                recv_sem=recv_sem.at[b, block],
                device_id=target,
                device_id_type=pl.DeviceIdType.MESH,
            ).wait_recv()


def layer_middle(arrived, inner, outer):
    batch, sources, _, slots, width = arrived.shape
    quarter = inner[0].shape
    anywhere = pl.BlockSpec(memory_space=pl.ANY)
    dma = pltpu.SemaphoreType.DMA
    results = pl.pallas_call(
        middle_kernel,
        out_shape=(
            jax.ShapeDtypeStruct(arrived.shape, jnp.bfloat16),
            *([jax.ShapeDtypeStruct(quarter, jnp.bfloat16)] * 4),
        ),
        in_specs=[anywhere] * 9,
        out_specs=[anywhere, *([VMEM] * 4)],
        scratch_shapes=[
            pltpu.VMEM((2, 2, 2, slots, width), jnp.bfloat16),
            pltpu.VMEM((2, 2, 2, slots, width), jnp.bfloat16),
            *([pltpu.VMEM(quarter, jnp.float32)] * 8),
            pltpu.VMEM((4, *quarter), jnp.bfloat16),
            pltpu.VMEM((4, *quarter), jnp.bfloat16),
            dma((2, 2)),
            dma((batch, sources)),
            dma((batch, sources)),
            dma((batch,)),
            dma((4,)),
            dma((4,)),
            dma((8,)),
            *([pltpu.VMEM(quarter, jnp.bfloat16)] * 8),
        ],
        compiler_params=pltpu.CompilerParams(
            collective_id=3, has_side_effects=True, vmem_limit_bytes=63 * 2**20
        ),
        name="layer_middle",
    )(arrived, *inner, *outer)
    return results[0], results[1:]


def bias_columns(diagonals, shards, bucket_count):
    lines = diagonals.shape[1]
    width = lines
    row = row_iota(lines, 1)
    distance = (row // (2 * LANES)) * LANES + LANES - 1 - row % (2 * LANES)
    table = bucket_table(lines // (2 * LANES) * LANES)
    bucket = jnp.minimum(distance, 16)
    for value in range(17, bucket_count):
        bucket = bucket + (distance >= int(np.argmax(table >= value))).astype(jnp.int32)
    lane = column_iota(1, width)
    place = lane % (width // shards)
    heads = 3
    hot = one_hot((bucket == place % bucket_count) & (place < heads * bucket_count))
    sums = sum(jnp.dot(part, hot, preferred_element_type=jnp.float32) for part in split(diagonals))
    head = lane // (width // shards) * heads + place // bucket_count
    return jnp.sum(jnp.where(row_iota(sums.shape[0], width) == head, sums, 0.0), 0, keepdims=True)


FOLD_SPLIT = 4


def tail_kernel(experts, capacity, bucket_count, lengths_ref, dealing_ref, *refs):
    x_ref, g_ref, routes_ref, refs = refs[0], refs[1], refs[2], refs[3:]
    weights, gain_ref, bias_ref, refs = refs[:5], refs[5], refs[6], refs[7:]
    normed_ref, q_ref, k_ref, v_ref, mix_ref, residual_ref, gates_ref, returned_ref = refs[:8]
    partials, refs = refs[8:12], refs[12:]
    result_ref, input_grad_ref, home_refs, outs, refs = (
        refs[0],
        refs[1],
        refs[2:4],
        refs[4:12],
        refs[12:],
    )
    out_rows, back_rows, branch, dq, dk, dv, router_grad, gain_grad, diag, refs = *refs[:9], refs[9:]
    grad_mix, grad_residual, scratch, refs = refs[0], refs[1], refs[2:6], refs[6:]
    grads, sums, refs = refs[:8], refs[8:16], refs[16:]
    inboxes, refs = [refs[8 * i : 8 * i + 8] for i in range(5)], refs[40:]
    fetched, landed, fold_send, fold_recv, move_send, move_recv, local_sem, own_sem = refs[:8]
    fetch_sem, *fetch_to = refs[8:]
    fetch_from = [mix_ref, q_ref, k_ref, v_ref, normed_ref, *weights[:3]]
    mix_ref, q_ref, k_ref, v_ref, normed_ref = fetch_to[:5]
    weights = [*fetch_to[5:], *weights[3:]]
    y, zh = lax.axis_index("y"), lax.axis_index("zh")
    at_home, away = zh == y, zh != y
    batch, tokens, width = x_ref.shape
    far, near = partials[:2], partials[2:]
    rows = far[0].shape[0] // CHUNKS
    cut_at = FOLD_SPLIT * LANES

    fetches = [
        pltpu.make_async_copy(source, target, fetch_sem.at[index])
        for index, (source, target) in enumerate(zip(fetch_from, fetch_to))
    ]

    def load(b):
        return [
            pltpu.make_async_copy(returned_ref.at[b, :, which], target, local_sem.at[which])
            for which, target in enumerate((out_rows, back_rows))
        ]

    def piece(ref, chunk):
        return ref.at[pl.ds(chunk * rows, rows)]

    for part in (*load(0), *fetches):
        part.start()
    greet(("core", "y", "x", "zl", "zh"))

    def own(which, chunk):
        return pltpu.make_async_copy(
            piece(near[which], chunk),
            (out_rows, back_rows)[which].at[chunk],
            own_sem.at[which, chunk],
        )

    def copy(which, chunk, kind, source, target, axis):
        return pltpu.make_async_remote_copy(
            src_ref=piece(source, chunk),
            dst_ref=piece(target, chunk),
            send_sem=move_send.at[which, chunk, kind],
            recv_sem=move_recv.at[which, chunk, kind],
            device_id=across(axis),
            device_id_type=pl.DeviceIdType.MESH,
        )

    def move(index):
        which, chunk = index // CHUNKS, index % CHUNKS
        copy(which, chunk, 0, far[which], fetched.at[which], "y").wait_recv()

        @pl.when(at_home)
        def _():
            copy(which, chunk, 1, fetched.at[which], landed.at[which], "zh").start()

        @pl.when(away)
        def _():
            copy(which, chunk, 1, near[which], landed.at[which], "zh").start()

    order = [(which, chunk) for which in range(2) for chunk in range(CHUNKS)]
    for which, chunk in order:
        copy(which, chunk, 0, far[which], fetched.at[which], "y").start()

    def columns(ref, b, first):
        return ref.at[b, :, :cut_at] if first else ref.at[b, :, cut_at:]

    operands = [(mix_ref.at[0], branch.at[0], mix_ref.at[1], branch.at[1])]
    for first in (True, False):
        for ref in (dq, dk, dv):
            operands.append(
                (
                    normed_ref.at[0],
                    columns(ref, 0, first),
                    normed_ref.at[1],
                    columns(ref, 1, first),
                )
            )
    operands.append(None)
    fold, fold_end = folder(operands, outs, grads, sums, inboxes, fold_send, fold_recv)
    early, late, small = (1, 2, 3), (4, 5, 6), 7

    def each(b, actions):
        for index, action in enumerate(actions):
            pl.when(b == index)(action)

    def combine(b, carry):
        for part in load(b):
            part.wait()
        combine_math(
            experts,
            capacity,
            g_ref.at[b],
            routes_ref.at[b],
            weights[3],
            weights[4],
            gain_ref,
            residual_ref.at[b],
            gates_ref.at[b],
            out_rows,
            back_rows,
            result_ref.at[b],
            branch.at[b],
            router_grad.at[b],
            gain_grad.at[b],
            grad_mix.at[b],
            grad_residual.at[b],
            lambda: each(b, [lambda: move(0), lambda: move(2)]),
        )

        def first():
            for part in load(1):
                part.start()
            move(1)

        def second():
            for which, chunk in order:
                own(which, chunk).start()
            move(3)

        each(b, [first, second])
        return carry

    lax.fori_loop(0, batch, combine, 0)
    for part in fetches:
        part.wait()
    fold(0, 0)

    actions = {
        0: [(fold, 0, 1), (move, 4)],
        3: [(fold, 0, 2), (move, 5)],
        6: [(move, 6)],
        7: [*((fold, i, 0) for i in early)],
        8: [(fold, 0, 3)],
        9: [*((fold, i, 1) for i in early)],
        11: [*((fold, i, 2) for i in early), (move, 7)],
    }

    def act(moment):
        for action, *values in actions[moment]:
            action(*values)

    def attend_back(item, carry):
        pair, b = item // 2, lax.rem(item, 2)
        attend_back_math(
            pair,
            lengths_ref[dealing_ref[b]],
            q_ref.at[b],
            k_ref.at[b],
            v_ref.at[b],
            grad_mix.at[b],
            bias_ref,
            dq.at[b],
            dk.at[b],
            dv.at[b],
            diag.at[b],
            *scratch,
        )
        for moment in actions:
            pl.when(item == moment)(functools.partial(act, moment))
        return carry

    lax.fori_loop(0, batch * (width // LANES), attend_back, 0)
    for i in late:
        fold(i, 0)
    for i in early:
        fold(i, 3)

    def finish(b, carry):
        finish_math(
            x_ref.at[b],
            *weights[:3],
            gain_ref,
            dq.at[b],
            dk.at[b],
            dv.at[b],
            grad_residual.at[b],
            gain_grad.at[b],
            input_grad_ref.at[b],
        )

        @pl.when(b == 0)
        def _():
            for i in late:
                fold(i, 1)

        return carry

    lax.fori_loop(0, batch, finish, 0)
    lines = [
        jnp.concatenate(
            [
                diag[0, head // 2, head % 2, offset : offset + 1, :]
                + diag[1, head // 2, head % 2, offset : offset + 1, :]
                for offset in range(diag.shape[3])
            ],
            1,
        )
        for head in range(2 * diag.shape[1])
    ]
    lines.append(jnp.zeros((16 - len(lines), width), jnp.float32))
    bias_line = bias_columns(jnp.concatenate(lines, 0), 4, bucket_count)
    gain_lines = gain_grad[0] + gain_grad[1]
    row = row_iota(LANES, width)
    stacked = jnp.where(
        row == 0,
        gain_lines[0:1, :],
        jnp.where(row == 1, gain_lines[1:2, :], jnp.where(row == 2, bias_line, 0.0)),
    )
    packed = jnp.concatenate([router_grad[0] + router_grad[1], stacked.T], 1)
    grads[small][...] = packed.astype(jnp.bfloat16).reshape(grads[small].shape)
    fold(small, 0)
    reached = {0: 4, **dict.fromkeys(early, 4), **dict.fromkeys(late, 2), small: 1}
    for k in range(1, FOLD_STEPS):
        for i in reached:
            if reached[i] == k:
                fold(i, k)
                reached[i] += 1
    fold_end()

    for which, chunk in order:
        own(which, chunk).wait()
        copy(which, chunk, 1, near[which], landed.at[which], "zh").wait()
        copy(which, chunk, 0, far[which], fetched.at[which], "y").wait_send()
        place = pl.ds(chunk * rows, rows)

        def settle(kept):
            total = kept.astype(jnp.float32) + landed[which, place].astype(jnp.float32)
            home_refs[which][place] = total.astype(jnp.bfloat16)

        pl.when(at_home)(lambda: settle((out_rows, back_rows)[which][chunk]))
        pl.when(away)(lambda: settle(fetched[which, place]))


def layer_tail(experts, capacity, bucket_count, lengths, x, g, routes, weights, gains, bias, saved, returned, partials):
    batch, tokens, width = x.shape
    blocks = tokens // LANES
    shape, dma = jax.ShapeDtypeStruct, pltpu.SemaphoreType.DMA
    anywhere = pl.BlockSpec(memory_space=pl.ANY)
    flat = shape(x.shape, jnp.bfloat16)
    quarter = partials[0].shape
    cut_at = FOLD_SPLIT * LANES
    widths = [width, *([cut_at] * 3), *([width - cut_at] * 3), 2 * LANES]
    sizes = [(width // 16, columns) for columns in widths]
    boxes = []
    for depth in range(5):
        for i, (part, columns) in enumerate(sizes):
            done = FOLD_ORDERS[i % len(FOLD_ORDERS)][:depth]
            lead = [2] * (3 - sum(axis != "zh" for axis in done))
            boxes.append(
                pltpu.VMEM(
                    (*lead, part, columns // 2 if "zh" in done else columns), jnp.bfloat16
                )
            )
    side = returned.shape[1:2] + returned.shape[3:]
    results = pl.pallas_call(
        functools.partial(tail_kernel, experts, capacity, bucket_count),
        out_shape=(
            flat,
            flat,
            *([shape(quarter, jnp.bfloat16)] * 2),
            *(shape((2, 2, *size), jnp.bfloat16) for size in sizes),
        ),
        in_specs=[
            SMEM,
            SMEM,
            *([VMEM] * 3),
            *([anywhere] * 3),
            *([VMEM] * 4),
            *([anywhere] * 5),
            *([VMEM] * 2),
            *([anywhere] * 5),
        ],
        out_specs=[VMEM] * 12,
        scratch_shapes=[
            pltpu.VMEM(side, jnp.bfloat16),
            pltpu.VMEM(side, jnp.bfloat16),
            *([pltpu.VMEM(x.shape, jnp.bfloat16)] * 4),
            pltpu.VMEM((batch, width, LANES), jnp.float32),
            pltpu.VMEM((batch, 2, width), jnp.float32),
            pltpu.VMEM((batch, *bias.shape), jnp.float32),
            pltpu.VMEM((batch, tokens, width), jnp.bfloat16),
            pltpu.VMEM((batch, tokens, width), jnp.float32),
            pltpu.VMEM((2, blocks, LANES, LANES), jnp.float32),
            pltpu.VMEM((tokens, LANES), jnp.float32),
            pltpu.VMEM((tokens, LANES), jnp.float32),
            pltpu.VMEM((2, blocks, LANES, LANES), jnp.float32),
            *(pltpu.VMEM((2, 2, 2, 2, *size), jnp.bfloat16) for size in sizes),
            *(pltpu.VMEM((2, 2, 2, *size), jnp.bfloat16) for size in sizes),
            *boxes,
            pltpu.VMEM((2, *quarter), jnp.bfloat16),
            pltpu.VMEM((2, *quarter), jnp.bfloat16),
            dma((8, FOLD_STEPS - 1)),
            dma((8, FOLD_STEPS - 1)),
            dma((2, CHUNKS, 2)),
            dma((2, CHUNKS, 2)),
            dma((2,)),
            dma((2, CHUNKS)),
            dma((8,)),
            *([pltpu.VMEM(x.shape, jnp.bfloat16)] * 5),
            *([pltpu.VMEM(weights[0].shape, jnp.bfloat16)] * 3),
        ],
        compiler_params=pltpu.CompilerParams(
            collective_id=2, has_side_effects=True, vmem_limit_bytes=63 * 2**20
        ),
        name="layer_tail",
    )(*lengths, x, g, routes, *weights, gains, bias, *saved, returned, *partials)
    output, *rest, packed = (
        out.reshape(-1, out.shape[-1]).astype(jnp.float32) for out in results[4:]
    )
    folded = [jnp.concatenate(pair, 1) for pair in zip(rest[:3], rest[3:])]
    folded += [output, packed]
    homes = [home.astype(jnp.float32) for home in results[2:4]]
    return results[0], results[1], folded, homes


class Grouped:
    swap_axes = "expert"

    def begin(self, sizes, lengths, x, g, routes, routes_t, inner, outer, parts, bias_shape):
        lengths = jnp.take(*lengths)
        wholes = [lax.all_gather(part, "shard", axis=0, tiled=True) for part in parts]
        misc = wholes[5].reshape(-1, *parts[5].shape).astype(jnp.float32)
        gains = jnp.sum(misc[:, -2:], 0)
        bias_rows = misc[:, :-2].reshape(bias_shape)
        inner, outer = (list(lax.all_gather(part, "shard", axis=0)) for part in (inner, outer))
        arrived, saved = [], []
        for index in range(x.shape[0]):
            sent, *kept = layer_forward(
                index,
                *sizes,
                lengths[index : index + 1],
                x,
                g,
                routes[index],
                routes_t[index],
                wholes[:4],
                wholes[4],
                gains,
                bias_rows,
            )
            saved.append(kept)
            arrived.append(self.swap(sent))
        saved = [jnp.stack(pair) for pair in zip(*saved)]
        return wholes, inner, outer, arrived, saved, gains, bias_rows

    def swap(self, blocks):
        experts = lax.axis_size("expert")
        count, _, slots, width = blocks.shape
        merged = blocks.swapaxes(0, 1).reshape(2, experts, -1, width).swapaxes(0, 1)
        merged = lax.all_to_all(merged, "expert", split_axis=0, concat_axis=0, tiled=True)
        return merged.swapaxes(0, 1).reshape(2, count, slots, width).swapaxes(0, 1)

    def finish(
        self,
        sizes,
        bucket_count,
        lengths,
        x,
        g,
        routes,
        wholes,
        gains,
        bias_rows,
        saved,
        arrived,
        inner,
        outer,
        likes,
    ):
        lengths = jnp.take(*lengths)
        returned, units = [], []
        for rows in arrived:
            going, *unit_pair = expert_pass(rows, inner, outer)
            units.append(unit_pair)
            returned.append(self.swap(going))
        returned = jnp.stack(returned)
        hiddens, pres = zip(*units)
        chunks = len(inner)
        passes = weight_pass(0, chunks, chunks, arrived, pres, hiddens)
        homes = [
            lax.psum_scatter(jnp.stack(grads), "shard", scatter_dimension=0).astype(jnp.float32)
            for grads in passes
        ]
        normed, queries, key_rows, value_rows, mixture, residual, gates = saved
        results, input_grads, grads, small = [], [], [], []
        for index in range(x.shape[0]):
            result, input_grad, branch, dq, dk, dv, *rest = layer_backward(
                index,
                *sizes,
                lengths[index : index + 1],
                x,
                g,
                routes,
                wholes[:4],
                wholes[4],
                gains,
                bias_rows,
                (queries, key_rows, value_rows, residual, gates),
                returned,
            )
            results.append(result)
            input_grads.append(input_grad)
            lefts = (normed[index],) * 3 + (mixture[index],)
            grads.append([tn_dot(*pair) for pair in zip(lefts, (dq, dk, dv, branch))])
            small.append(rest)
        router_grad, gain_grad, diagonals = (sum(parts) for parts in zip(*small))
        bias_grad = jnp.dot(
            diagonals.reshape(bias_rows.shape[0] * 2, -1),
            jnp.asarray(collect_hot(x.shape[1], bucket_count)),
            precision=HIGH,
        )
        small = (router_grad[:, : sizes[0]], gain_grad[0], gain_grad[1], bias_grad)
        shares = [
            lax.psum_scatter(
                sum(pair).astype(jnp.bfloat16), "shard", scatter_dimension=0, tiled=True
            ).astype(jnp.float32)
            for pair in (*zip(*grads), *((part,) for part in small))
        ]
        return jnp.stack(results), jnp.stack(input_grads), lax.psum(shares, "expert"), homes

    def shard_index(self):
        return lax.axis_index("shard")


class Halved:
    swap_axes = ("y", "zl", "x")

    def begin(self, sizes, lengths, x, g, routes, routes_t, inner, outer, parts, bias_shape):
        misc = jnp.pad(parts[5], ((0, 32 - parts[5].shape[0]), (0, 0)))
        return layer_head(
            *sizes, lengths, x, g, routes, routes_t, inner, outer, [*parts[:5], misc], bias_shape
        )

    def shard_index(self):
        return lax.axis_index("y") * 2 + lax.axis_index("core")

    def finish(
        self,
        sizes,
        bucket_count,
        lengths,
        x,
        g,
        routes,
        wholes,
        gains,
        bias_rows,
        saved,
        arrived,
        inner,
        outer,
        likes,
    ):
        returned, partials = layer_middle(arrived, inner, outer)
        result, input_grad, folded, homes = layer_tail(
            *sizes,
            bucket_count,
            lengths,
            x,
            g,
            routes,
            wholes[:5],
            gains,
            bias_rows,
            saved,
            returned,
            partials,
        )
        *large, packed = folded
        router, gain_one, gain_two, bias = likes
        small = [
            packed[:, : router.shape[1]],
            packed[:, LANES],
            packed[:, LANES + 1],
            packed[: bias.size, LANES + 2].reshape(bias.shape),
        ]
        return result, input_grad, [*large, *small], homes


def body(
    plan,
    tokens,
    cotangent,
    lengths,
    dealing,
    routes,
    query_weight,
    key_weight,
    value_weight,
    output_weight,
    router_weight,
    first_gain,
    second_gain,
    position_bias,
    inner_weight,
    outer_weight,
):
    batch, seq_len, model_width = tokens.shape
    experts = lax.axis_size(plan.swap_axes)
    capacity = 4 * seq_len // experts
    bucket_count = position_bias.shape[1]
    shard_rows = query_weight.shape[0]
    shards = model_width // shard_rows
    small_shard = (router_weight, first_gain, second_gain, position_bias)
    lane_shard = jnp.arange(model_width) // shard_rows
    bias_shard = jnp.dot(
        position_bias.astype(jnp.float32),
        jnp.asarray(spread_hot(seq_len, bucket_count)),
        precision=HIGH,
    ).astype(jnp.bfloat16)
    gain_shard = jnp.where(
        lane_shard == plan.shard_index(),
        jnp.tile(jnp.stack([first_gain, second_gain]), (1, shards)),
        0,
    )
    parts = [
        query_weight,
        key_weight,
        value_weight,
        output_weight,
        jnp.pad(router_weight, ((0, 0), (0, LANES - experts))),
        jnp.concatenate([bias_shard, gain_shard], 0),
    ]
    heads = shards * position_bias.shape[0]
    bias_shape = (heads // 2, 2, seq_len // LANES, 2 * LANES)
    sizes = (experts, capacity)
    wholes, inner_parts, outer_parts, arrived, saved, gains, bias_rows = plan.begin(
        sizes,
        (lengths, dealing),
        tokens,
        cotangent,
        routes,
        jnp.pad(routes.swapaxes(1, 2), ((0, 0), (0, 6), (0, 0))),
        inner_weight[0],
        outer_weight[0],
        parts,
        bias_shape,
    )
    results, input_grads, large_and_small, homes = plan.finish(
        sizes,
        bucket_count,
        (lengths, dealing),
        tokens,
        cotangent,
        routes,
        wholes,
        gains,
        bias_rows,
        saved,
        arrived,
        inner_parts,
        outer_parts,
        small_shard,
    )
    return (results, input_grads, *large_and_small, homes[0][None], homes[1][None])


def solution(mesh):
    experts, shards = mesh.shape["expert"], mesh.shape["shard"]
    if (experts, shards) == (8, 4):
        plan = Halved()
        mesh = jax.sharding.Mesh(
            mesh.devices.reshape(2, 2, 2, 2, 2), ("zh", "zl", "x", "y", "core")
        )
        expert_axes, shard_axes = ("zh", "zl", "x"), ("y", "core")
    else:
        plan = Grouped()
        expert_axes, shard_axes = ("expert",), ("shard",)
    both = (*expert_axes, *shard_axes)
    rows = P(both, None, None)
    weight = P(shard_axes, None)
    in_specs = (rows, rows, P(), P(both), rows, *([weight] * 5))
    in_specs += (P(shard_axes), P(shard_axes), weight)
    in_specs += (P(expert_axes, None, shard_axes), P(expert_axes, shard_axes, None))
    out_specs = (rows, rows, *([weight] * 5), P(shard_axes), P(shard_axes), weight)
    out_specs += (P(expert_axes, None, shard_axes), P(expert_axes, shard_axes, None))
    return jax.shard_map(
        functools.partial(body, plan),
        mesh=mesh,
        in_specs=in_specs,
        out_specs=out_specs,
        check_vma=False,
    )
```
